32 devices in a mesh: section: 2 (over y), dp: 4 (over x, core), mp: 4 (over z).
Axes of the slice: x: 2, y: 2, z: 4, core: 2. Of those that a mesh axis runs over, the one named last changes fastest.
Arguments:
- patches: bfloat16 [4096, 1280], P(('section', 'dp')), may hold values from -6 to 6
- patch_counts: int32 [16], P(('section', 'dp')), may hold values from 64 to 256, as said below
- dest_rows: int32 [1024], P(('section', 'dp')), may hold values from 0 to 4095, as said below
- qkv_weight: bfloat16 [1280, 3, 1280], P(None, None, 'mp'), may hold values from -1 to 1
- out_weight: bfloat16 [1280, 1280], P('mp'), may hold values from -0.15625 to 0.15625
- attn_gain: bfloat16 [1280], replicated, may hold values from 0.25 to 1.75
- merge_gain: bfloat16 [1280], replicated, may hold values from 0.25 to 1.75
- fc1_weight: bfloat16 [5120, 5120], P('mp', ('section', 'dp')), may hold values from -0.078125 to 0.078125
- fc1_bias: bfloat16 [5120], P(('section', 'dp')), may hold values from -3 to 3
- fc2_weight: bfloat16 [5120, 8192], P(('section', 'dp'), 'mp'), may hold values from -0.078125 to 0.078125
- fc2_bias: bfloat16 [8192], P('mp'), may hold values from -3 to 3
- text_embeds: bfloat16 [4096, 8192], P(('section', 'dp'), 'mp'), may hold values from -6 to 6
- section_hidden: bfloat16 [4096, 8192], P(('section', 'dp'), 'mp'), may hold values from -80 to 80
- llm_gain: bfloat16 [8192], P('mp'), may hold values from 0.25 to 1.75
Outputs:
- sequence_embeds: bfloat16 [4096, 8192], P(('section', 'dp'), 'mp')
- layer_inputs: bfloat16 [4096, 8192], P(('section', 'dp'), 'mp')
The draws below stay inside these ranges and needn't reach their ends.
Inputs may be any that keep to these rules, and one draw needn't show every extreme that they name: `patch_counts`: multiples of 4; a tile's patches fill the first slots of its block. `dest_rows`: all rows differ. Each group's merged slots form runs of 16 consecutive slots (aligned); a run goes to one sequence slice (row // 512, numbered in section-major order), different runs of a group to different slices. Rows of slots that are not live are never written.
All inputs are finite; a program needn't handle non-finite values.
Results may differ from the reference program's by a relative error of at most 0.0055.
Values may be sent and summed in bfloat16 or wider, within the bound.
A program may use at most 128 MiB of HBM per device.

```python
import math
import jax
import jax.numpy as jnp
from jax import lax

D_VIT = 1280
HEADS = 16
HEAD_DIM = 80
MERGE_HID = 5120
HID = 8192
BLOCK = 256
TILES_DEV = 2
SEQ_ROWS = 512
GROUPS = 8
P_DEV = 512
M_DEV = 128
CAP = 16
PATCHES = 4096
TILES = 16
MERGE_IN = 5120
RECV_ROWS = 4096
N_SECTION = 2
N_DP = 4


def draw_patch_counts(key, part):
    return (4 * jax.random.randint(key, (TILES,), CAP, BLOCK // 4 + 1)).astype(jnp.int32)


def draw_dest_rows(key, part):
    group_total = GROUPS
    run_total = M_DEV // CAP
    heavy = jax.random.randint(jax.random.fold_in(key, 1), (), 0, group_total).astype(jnp.int32)

    def run_order(order_key):
        others = (heavy + 1 + jax.random.permutation(order_key, group_total - 1).astype(jnp.int32)) % group_total
        return jnp.concatenate([heavy[None], others])[:run_total]
    targets = jax.vmap(run_order)(jax.random.split(jax.random.fold_in(key, 2), group_total))
    places = jax.vmap(lambda place_key: jax.random.permutation(place_key, SEQ_ROWS).astype(jnp.int32))(jax.random.split(jax.random.fold_in(key, 3), group_total))
    source = jnp.arange(group_total, dtype=jnp.int32)[:, None, None]
    lane = jnp.arange(CAP, dtype=jnp.int32)[None, None, :]
    receiver = jnp.broadcast_to(targets[:, :, None], (group_total, run_total, CAP))
    position = places[receiver, source * CAP + lane]
    return (receiver * SEQ_ROWS + position).reshape(-1).astype(jnp.int32)


def draw_qkv_weight(key, part):
    base = jax.random.normal(key, (D_VIT, 3, D_VIT), jnp.float32) * D_VIT ** (-0.5)
    base = jnp.clip(base, -0.15, 0.15)
    return base.astype(jnp.bfloat16)


def draw_section_hidden(key, part):
    noise = jax.random.normal(jax.random.fold_in(key, 1), (RECV_ROWS, HID), jnp.float32)
    column_scale = jnp.exp(jnp.linspace(0.0, math.log(10.0), HID))[None, :]
    row_scale = jnp.exp(jax.random.uniform(jax.random.fold_in(key, 2), (RECV_ROWS, 1), jnp.float32, 0.0, math.log(10.0)))
    return jnp.clip(0.1 * noise * column_scale * row_scale, -80.0, 80.0).astype(jnp.bfloat16)


def shard_levels(key, shape, pieces, low, high):
    loudness = 1.0
    for axis_at, blocks in pieces:
        draws = jax.random.uniform(jax.random.fold_in(jax.random.fold_in(key, 6), axis_at), (blocks,), jnp.float32, low / len(pieces), high / len(pieces))
        loudness = loudness * jnp.repeat(jnp.exp(draws), shape[axis_at] // blocks).reshape((-1,) + (1,) * (len(shape) - 1 - axis_at))
    return loudness


def gaussian(own_key, dims, scale, bound, shards=(), kind=jnp.bfloat16):
    array = scale * jax.random.normal(own_key, dims, jnp.float32)
    if shards:
        array = array * shard_levels(own_key, dims, shards, -0.22, 0.18)
    return jnp.clip(array, -bound, bound).astype(kind)


def setup_inputs(seed: int = 0) -> dict:
    streams_of = jax.random.split(jax.random.key(seed), 15)
    return {
        "patches": gaussian(streams_of[0], (PATCHES, D_VIT), 1.0, 6.0, ((0, 8),)),
        "patch_counts": draw_patch_counts(jax.random.fold_in(streams_of[14], 71), 0),
        "dest_rows": draw_dest_rows(jax.random.fold_in(streams_of[14], 71), 0),
        "qkv_weight": draw_qkv_weight(jax.random.fold_in(streams_of[14], 71), 0),
        "out_weight": gaussian(streams_of[4], (D_VIT, D_VIT), D_VIT ** -0.5, 0.15625, ((0, 4),)),
        "attn_gain": jnp.clip(1.0 + 0.15 * jax.random.normal(streams_of[5], (D_VIT,), jnp.float32), 0.25, 1.75).astype(jnp.bfloat16),
        "merge_gain": jnp.clip(1.0 + 0.15 * jax.random.normal(streams_of[6], (D_VIT,), jnp.float32), 0.25, 1.75).astype(jnp.bfloat16),
        "fc1_weight": gaussian(streams_of[7], (MERGE_IN, MERGE_HID), MERGE_IN ** -0.5, 0.078125, ((0, 4), (1, 8))),
        "fc1_bias": gaussian(streams_of[8], (MERGE_HID,), 0.5, 3.0, ((0, 8),)),
        "fc2_weight": gaussian(streams_of[9], (MERGE_HID, HID), MERGE_HID ** -0.5, 0.078125, ((0, 8), (1, 4))),
        "fc2_bias": gaussian(streams_of[10], (HID,), 0.5, 3.0, ((0, 4),)),
        "text_embeds": gaussian(streams_of[11], (RECV_ROWS, HID), 1.0, 6.0, ((0, 8), (1, 4))),
        "section_hidden": draw_section_hidden(jax.random.fold_in(streams_of[14], 71), 0),
        "llm_gain": jnp.clip(1.0 + 0.15 * jax.random.normal(streams_of[13], (HID,), jnp.float32), 0.25, 1.75).astype(jnp.bfloat16),
    }


vit_eps = 1e-06
llm_eps = 1e-06

def layer_norm(values, gain):
    centred = values.astype(jnp.float32)
    centred = centred - lax.optimization_barrier(jnp.mean(centred, axis=-1, keepdims=True))
    variance = lax.optimization_barrier(jnp.mean(centred * centred, axis=-1, keepdims=True))
    return centred * lax.rsqrt(variance + vit_eps) * gain.astype(jnp.float32)

def group_embed(group_rows, group_counts, qkv_weight, out_weight, attn_gain, merge_gain, fc1_weight, fc1_bias, fc2_weight, fc2_bias):
    normed_in = layer_norm(group_rows, attn_gain).astype(jnp.bfloat16)
    projections = jnp.dot(normed_in, qkv_weight.reshape(D_VIT, 3 * D_VIT), preferred_element_type=jnp.float32).astype(jnp.bfloat16)
    projections = projections.reshape(TILES_DEV, BLOCK, 3, HEADS, HEAD_DIM).astype(jnp.float32)
    query_part = projections[:, :, 0]
    key_part = projections[:, :, 1]
    value_part = projections[:, :, 2]
    scores = jnp.einsum('tqhd,tkhd->thqk', query_part, key_part) * HEAD_DIM ** (-0.5)
    key_live = jnp.arange(BLOCK, dtype=jnp.int32)[None, None, None, :] < group_counts[:, None, None, None]
    scores = jnp.where(key_live, scores, -1e+30)
    weights = jax.nn.softmax(scores, axis=-1).astype(jnp.bfloat16)
    attended = jnp.einsum('thqk,tkhd->tqhd', weights.astype(jnp.float32), value_part).astype(jnp.bfloat16)
    attended = attended.reshape(P_DEV, D_VIT)
    block_out = (group_rows.astype(jnp.float32) + jnp.dot(attended, out_weight, preferred_element_type=jnp.float32)).astype(jnp.bfloat16)
    merge_in = layer_norm(block_out, merge_gain).astype(jnp.bfloat16).reshape(M_DEV, MERGE_IN)
    hidden = jax.nn.gelu(jnp.dot(merge_in, fc1_weight, preferred_element_type=jnp.float32) + fc1_bias.astype(jnp.float32), approximate=False).astype(jnp.bfloat16)
    return (jnp.dot(hidden, fc2_weight, preferred_element_type=jnp.float32) + fc2_bias.astype(jnp.float32)).astype(jnp.bfloat16)

def reference(patches, patch_counts, dest_rows, qkv_weight, out_weight, attn_gain, merge_gain, fc1_weight, fc1_bias, fc2_weight, fc2_bias, text_embeds, section_hidden, llm_gain):
    group_total = N_SECTION * N_DP
    grouped = patches.reshape(group_total, P_DEV, D_VIT)
    grouped_counts = patch_counts.reshape(group_total, TILES_DEV)

    def one_group(pair):
        return group_embed(pair[0], pair[1], qkv_weight, out_weight, attn_gain, merge_gain, fc1_weight, fc1_bias, fc2_weight, fc2_bias)
    image_embeds = lax.map(one_group, (grouped, grouped_counts)).reshape(group_total * M_DEV, HID)
    slot_in_tile = jnp.arange(group_total * M_DEV, dtype=jnp.int32) % (BLOCK // 4)
    tile_counts = jnp.repeat(patch_counts, BLOCK // 4, total_repeat_length=group_total * M_DEV)
    live = slot_in_tile * 4 < tile_counts
    target_rows = jnp.where(live, dest_rows, group_total * SEQ_ROWS).astype(jnp.int32)
    sequence_embeds = text_embeds.at[target_rows].set(image_embeds, mode='drop')
    sectioned_seq = sequence_embeds.reshape(N_SECTION, N_DP * SEQ_ROWS, HID)
    sectioned_hidden = section_hidden.reshape(N_SECTION, N_DP * SEQ_ROWS, HID)
    entering = jnp.concatenate([sectioned_seq[:1], sectioned_hidden[:-1]], axis=0).reshape(group_total * SEQ_ROWS, HID)
    entering = entering.astype(jnp.float32)
    mean_square = lax.optimization_barrier(jnp.mean(entering * entering, axis=1, keepdims=True))
    layer_inputs = (entering * lax.rsqrt(mean_square + llm_eps) * llm_gain.astype(jnp.float32)).astype(jnp.bfloat16)
    return (sequence_embeds, layer_inputs)
```

```python
import functools
import math

import jax
import jax.numpy as jnp
from jax import lax
from jax.experimental import pallas as pl
from jax.experimental.pallas import tpu as pltpu
from jax.sharding import PartitionSpec as P

HEAD_DIM = 80
HID = 8192


vit_eps = 1e-06
llm_eps = 1e-06


def from_behind(value, axis, steps):
    count = lax.axis_size(axis)
    first, last = (max(0, -steps), min(count, count - steps))
    return lax.ppermute(value, axis, [(source, source + steps) for source in range(first, last)])


def layer_norm(values, gain):
    centred = values.astype(jnp.float32)
    centred = centred - jnp.mean(centred, axis=-1, keepdims=True)
    variance = jnp.mean(centred * centred, axis=-1, keepdims=True)
    return centred * lax.rsqrt(variance + vit_eps) * gain.astype(jnp.float32)


VMEM_LIMIT = 60 * 1024 * 1024
KERNEL_BYTES = 8 * 1024 * 1024


def vmem_call(kernel, out, scratch, sent_bytes, ident, *operands):
    return pl.pallas_call(
        kernel,
        out_shape=out,
        in_specs=[pl.BlockSpec(memory_space=pltpu.VMEM)] * len(operands),
        out_specs=pl.BlockSpec(memory_space=pltpu.VMEM),
        scratch_shapes=scratch,
        cost_estimate=pl.CostEstimate(
            flops=sent_bytes * 20000, bytes_accessed=sent_bytes * 2, transcendentals=0
        ),
        compiler_params=pltpu.CompilerParams(
            collective_id=ident, has_side_effects=True, vmem_limit_bytes=VMEM_LIMIT
        ),
    )(*operands)


def exchange_kernel(count, spread, x_ref, o_ref, send_sem, recv_sem, own_sem):
    me = lax.axis_index("mp")
    barrier = pltpu.get_barrier_semaphore()
    for step in range(1, count):
        peer = lax.rem(me + step, count)
        pl.semaphore_signal(
            barrier, inc=1, device_id={"mp": peer}, device_id_type=pl.DeviceIdType.MESH
        )
    pl.semaphore_wait(barrier, count - 1)
    copies = []
    for step in sorted(range(1, count), key=lambda s: -min(s, count - s)):
        peer = lax.rem(me + step, count)
        copy = pltpu.make_async_remote_copy(
            src_ref=x_ref.at[peer] if spread else x_ref,
            dst_ref=o_ref.at[me],
            send_sem=send_sem.at[step - 1],
            recv_sem=recv_sem.at[step - 1],
            device_id={"mp": peer},
            device_id_type=pl.DeviceIdType.MESH,
        )
        copy.start()
        copies.append(copy)
    own = pltpu.make_async_copy(x_ref.at[me] if spread else x_ref, o_ref.at[me], own_sem)
    own.start()
    own.wait()
    for copy in copies:
        copy.wait()


def relay_kernel(count, x_ref, o_ref, send_sem, recv_sem, own_sem):
    me = lax.axis_index("mp")
    barrier = pltpu.get_barrier_semaphore()
    for step in range(1, count):
        peer = lax.rem(me + step, count)
        pl.semaphore_signal(
            barrier, inc=1, device_id={"mp": peer}, device_id_type=pl.DeviceIdType.MESH
        )
    pl.semaphore_wait(barrier, count - 1)
    own = pltpu.make_async_copy(x_ref, o_ref.at[me], own_sem)
    own.start()

    def hop(way, step):
        owner = lax.rem(me - way * step + count, count)
        return pltpu.make_async_remote_copy(
            src_ref=o_ref.at[owner] if step else x_ref,
            dst_ref=o_ref.at[owner],
            send_sem=send_sem.at[(way + 1) // 2, step],
            recv_sem=recv_sem.at[(way + 1) // 2, step],
            device_id={"mp": lax.rem(me + way + count, count)},
            device_id_type=pl.DeviceIdType.MESH,
        )

    def holds(way, step):
        return me >= step if way > 0 else me + step < count

    def sends(way):
        return me < count - 1 if way > 0 else me > 0

    for step in range(count):
        for way in (1, -1):
            if step:

                @pl.when(holds(way, step))
                def _():
                    owner = lax.rem(me - way * step + count, count)
                    pltpu.make_async_remote_copy(
                        src_ref=x_ref,
                        dst_ref=o_ref.at[owner],
                        send_sem=send_sem.at[(way + 1) // 2, step - 1],
                        recv_sem=recv_sem.at[(way + 1) // 2, step - 1],
                        device_id={"mp": lax.rem(me - way + count, count)},
                        device_id_type=pl.DeviceIdType.MESH,
                    ).wait_recv()

            if step < count - 1:

                @pl.when(jnp.logical_and(holds(way, step), sends(way)))
                def _():
                    hop(way, step).start()

    own.wait()
    for step in range(count - 1):
        for way in (1, -1):

            @pl.when(jnp.logical_and(holds(way, step), sends(way)))
            def _():
                hop(way, step).wait_send()


def relay_mp(value, ident):
    count = lax.axis_size("mp")
    return vmem_call(
        functools.partial(relay_kernel, count),
        jax.ShapeDtypeStruct((count,) + value.shape, value.dtype),
        [
            pltpu.SemaphoreType.DMA((2, count - 1)),
            pltpu.SemaphoreType.DMA((2, count - 1)),
            pltpu.SemaphoreType.DMA,
        ],
        count * value.size * value.dtype.itemsize,
        ident,
        value,
    )


def exchange_mp(value, spread, ident):
    count = lax.axis_size("mp")
    shape = value.shape if spread else (count,) + value.shape
    size = math.prod(shape) * value.dtype.itemsize
    return vmem_call(
        functools.partial(exchange_kernel, count, spread),
        jax.ShapeDtypeStruct(shape, value.dtype),
        [
            pltpu.SemaphoreType.DMA((count - 1,)),
            pltpu.SemaphoreType.DMA((count - 1,)),
            pltpu.SemaphoreType.DMA,
        ],
        size,
        ident,
        value,
    )


def sum_scatter_mp(blocks, ident):
    return jnp.sum(exchange_mp(blocks, True, ident).astype(jnp.float32), axis=0)


def gather_mp(value):
    got = relay_mp(value, 2)
    return got.reshape((-1,) + value.shape[1:])


def total_mp(value):
    return jnp.sum(exchange_mp(value.reshape(-1, 128), False, 3), axis=0).reshape(-1)


def flip(index, bit):
    return index + bit * (1 - 2 * (index // bit % 2))


def group_bits():
    outer = [("dp", 1 << k) for k in range(1, lax.axis_size("dp").bit_length() - 1)]
    outer += [("section", 1 << k) for k in range(lax.axis_size("section").bit_length() - 1)]
    return outer, ("dp", 1)


def meets(axis, bit):
    return {axis: flip(lax.axis_index(axis), bit)}


def group_at(mask):
    spots = {axis: lax.axis_index(axis) for axis in ("section", "dp")}
    for axis, bit in mask:
        spots[axis] = flip(spots[axis], bit)
    return spots["section"] * lax.axis_size("dp") + spots["dp"]


def greet(bits):
    barrier = pltpu.get_barrier_semaphore()
    for axis, bit in bits:
        pl.semaphore_signal(
            barrier, inc=1, device_id=meets(axis, bit), device_id_type=pl.DeviceIdType.MESH
        )
    pl.semaphore_wait(barrier, len(bits))


def gather_kernel(x_ref, o_ref, send_sem, recv_sem, own_sem):
    outer, last = group_bits()
    greet(outer + [last])
    half = x_ref.shape[1] // 2
    sent, waiting = [], []
    slots = iter(range(send_sem.shape[0]))

    def pass_on(mask, stage, part, order):
        cols = pl.ds(part * half, half)
        spot = group_at(mask)
        source = o_ref.at[spot, :, cols] if mask else x_ref.at[:, cols]
        for later in range(stage, len(order)):
            slot = next(slots)
            copy = pltpu.make_async_remote_copy(
                src_ref=source,
                dst_ref=o_ref.at[spot, :, cols],
                send_sem=send_sem.at[slot],
                recv_sem=recv_sem.at[slot],
                device_id=meets(*order[later]),
                device_id_type=pl.DeviceIdType.MESH,
            )
            copy.start()
            sent.append(copy)
            waiting.append((later, copy, mask + [order[later]], part, order))

    pass_on([], 0, 0, outer + [last])
    pass_on([], 0, 1, outer[::-1] + [last])
    own = pltpu.make_async_copy(x_ref, o_ref.at[group_at([])], own_sem)
    own.start()
    while waiting:
        first = min(range(len(waiting)), key=lambda at: waiting[at][0])
        stage, copy, mask, part, order = waiting.pop(first)
        copy.wait_recv()
        pass_on(mask, stage + 1, part, order)
    for copy in sent:
        copy.wait_send()
    own.wait()


def gather_groups(value):
    count = lax.axis_size("section") * lax.axis_size("dp")
    size = count * value.size * value.dtype.itemsize
    if size > KERNEL_BYTES:
        return lax.all_gather(value, ("section", "dp"), axis=0, tiled=True)
    slots = 2 * (count - 1)
    got = vmem_call(
        gather_kernel,
        jax.ShapeDtypeStruct((count,) + value.shape, value.dtype),
        [
            pltpu.SemaphoreType.DMA((slots,)),
            pltpu.SemaphoreType.DMA((slots,)),
            pltpu.SemaphoreType.DMA,
        ],
        size,
        4,
        value,
    )
    return got.reshape(-1, value.shape[1])


def scatter_kernel(x_ref, o_ref, held, taken, send_sem, recv_sem):
    outer, first = group_bits()
    greet(outer + [first])
    rows = x_ref.shape[1]
    half = x_ref.shape[2] // 2
    chunk = 32
    orders = ([first] + outer, [first] + outer[::-1])
    slots = iter(range(send_sem.shape[0]))
    masks = [[]]
    for bit in outer:
        masks = masks + [mask + [bit] for mask in masks]
    place_of = {frozenset(mask): at for at, mask in enumerate(masks)}
    base = len(masks)
    live = {}

    def send(part, stage):
        cols = pl.ds(part * half, half)
        bit = orders[part][stage]
        kept = orders[part][stage + 1 :]
        copies = []
        for mask in [m for m in masks if set(m) <= set(kept)]:
            if stage == 0:
                source = x_ref.at[group_at(mask + [bit]), :, cols]
            else:
                source = held.at[place_of[frozenset(mask + [bit])], :, cols]
            landing = 2 * base - 2 ** (len(kept) + 1) + [
                m for m in masks if set(m) <= set(kept)
            ].index(mask)
            slot = next(slots)
            copy = pltpu.make_async_remote_copy(
                src_ref=source,
                dst_ref=taken.at[landing, :, cols],
                send_sem=send_sem.at[slot],
                recv_sem=recv_sem.at[slot],
                device_id=meets(*bit),
                device_id_type=pl.DeviceIdType.MESH,
            )
            copy.start()
            copies.append((copy, mask, landing))
        live[part, stage] = copies

    def add(part, stage):
        cols = pl.ds(part * half, half)
        final = stage + 1 == len(orders[part])
        following = None if final else orders[part][stage + 1]
        copies = live[part, stage]
        for copy, mask, landing in sorted(copies, key=lambda c: following not in c[1]):
            copy.wait_recv()
            at = place_of[frozenset(mask)]
            spot = group_at(mask)

            @pl.loop(0, rows // chunk)
            def _(step):
                span = pl.ds(step * chunk, chunk)
                mine = x_ref[spot, span, cols] if stage == 0 else held[at, span, cols]
                total = mine.astype(jnp.float32) + taken[landing, span, cols].astype(jnp.float32)
                if final:
                    o_ref[span, cols] = total
                else:
                    held[at, span, cols] = total.astype(held.dtype)

    send(0, 0)
    send(1, 0)
    for stage in range(len(orders[0])):
        for part in (0, 1):
            add(part, stage)
            if stage + 1 < len(orders[0]):
                send(part, stage + 1)
    for copies in live.values():
        for copy, _, _ in copies:
            copy.wait_send()


def sum_scatter_groups(value):
    count = lax.axis_size("section") * lax.axis_size("dp")
    size = value.size * value.dtype.itemsize
    if size > KERNEL_BYTES:
        return lax.psum_scatter(value, ("section", "dp"), scatter_dimension=0, tiled=True)
    rows, cols = value.shape[0] // count, value.shape[1]
    slots = 2 * (count - 1)
    return vmem_call(
        scatter_kernel,
        jax.ShapeDtypeStruct((rows, cols), jnp.float32),
        [
            pltpu.VMEM((count // 2, rows, cols), value.dtype),
            pltpu.VMEM((count - 1, rows, cols), value.dtype),
            pltpu.SemaphoreType.DMA((slots,)),
            pltpu.SemaphoreType.DMA((slots,)),
        ],
        size,
        5,
        value.reshape(count, rows, cols),
    )


def plain_per_device(
    patches,
    patch_counts,
    dest_rows,
    qkv_weight,
    out_weight,
    attn_gain,
    merge_gain,
    fc1_weight,
    fc1_bias,
    fc2_weight,
    fc2_bias,
    text_embeds,
    section_hidden,
    llm_gain,
):
    width = patches.shape[1]
    tile_total = patch_counts.shape[0]
    block_rows = patches.shape[0] // tile_total
    merged_rows = patches.shape[0] // 4
    local_cols = qkv_weight.shape[2]
    local_heads = local_cols // HEAD_DIM
    feature_cols = text_embeds.shape[1]
    seq_rows = text_embeds.shape[0]
    section_count = lax.axis_size("section")
    group_count = section_count * lax.axis_size("dp")
    run_cap = max(2, merged_rows // group_count)
    run_total = merged_rows // run_cap
    run_target = dest_rows.reshape(run_total, run_cap)[:, 0] // seq_rows
    takes = jnp.arange(group_count, dtype=jnp.int32)[:, None] == run_target[None, :]
    slot_in_tile = jnp.arange(merged_rows, dtype=jnp.int32) % (block_rows // 4)
    tile_counts = jnp.repeat(patch_counts, block_rows // 4, total_repeat_length=merged_rows)
    live = slot_in_tile * 4 < tile_counts
    place = jnp.where(live, dest_rows % seq_rows - seq_rows, 0).reshape(run_total, run_cap)
    send_place = jnp.sum(jnp.where(takes[:, :, None], place[None], 0), axis=1) + seq_rows
    got_place = lax.all_to_all(send_place, ("section", "dp"), split_axis=0, concat_axis=0, tiled=True)
    incoming = from_behind(section_hidden, "section", 1)
    normed_in = layer_norm(patches, attn_gain).astype(jnp.bfloat16)
    projections = jnp.dot(
        normed_in, qkv_weight.reshape(width, 3 * local_cols), preferred_element_type=jnp.float32
    ).astype(jnp.bfloat16)
    projections = projections.reshape(tile_total, block_rows, 3, local_heads, HEAD_DIM)
    query_part = projections[:, :, 0]
    key_part = projections[:, :, 1]
    value_part = projections[:, :, 2]
    scores = jnp.einsum(
        "tqhd,tkhd->thqk", query_part, key_part, preferred_element_type=jnp.float32
    ) * HEAD_DIM ** (-0.5)
    key_live = (
        jnp.arange(block_rows, dtype=jnp.int32)[None, None, None, :]
        < patch_counts[:, None, None, None]
    )
    scores = jnp.where(key_live, scores, -1e30)
    weights = jax.nn.softmax(scores, axis=-1).astype(jnp.bfloat16)
    attended = jnp.einsum(
        "thqk,tkhd->tqhd", weights, value_part, preferred_element_type=jnp.float32
    ).astype(jnp.bfloat16)
    attended = attended.reshape(patches.shape[0], local_cols)
    lane_source = jnp.arange(run_total, dtype=jnp.int32)[None, :] * run_cap
    run_source = jnp.sum(jnp.where(takes, lane_source, 0), axis=1)
    row_source = (
        run_source[:, None] + jnp.arange(run_cap, dtype=jnp.int32)[None, :]
    ).reshape(-1) * 4
    slots_at = jnp.arange(patches.shape[0], dtype=jnp.int32)
    patch_at = jnp.arange(4, dtype=jnp.int32)
    order = (
        (row_source[None, :] + patch_at[:, None]).reshape(-1)[:, None] == slots_at[None, :]
    ).astype(jnp.bfloat16)
    own_order = (
        (row_source + lax.axis_index("mp"))[:, None] == slots_at[None, :]
    ).astype(jnp.bfloat16)
    ordered = jnp.dot(order, attended, preferred_element_type=jnp.float32).astype(jnp.bfloat16)
    own_patch = jnp.dot(own_order, patches, preferred_element_type=jnp.float32)
    partial_proj = jnp.dot(ordered, out_weight, preferred_element_type=jnp.float32)
    own_proj = sum_scatter_mp(
        partial_proj.astype(jnp.bfloat16).reshape(4, group_count * run_cap, width), 0
    )
    block_out = (own_patch + own_proj).astype(jnp.bfloat16)
    merge_part = layer_norm(block_out, merge_gain).astype(jnp.bfloat16)
    slot_rows = group_count * run_cap
    gathered = gather_groups(merge_part)
    gathered = (
        gathered.reshape(group_count, group_count, run_cap, width)
        .transpose(1, 0, 2, 3)
        .reshape(group_count * slot_rows, width)
    )
    first_partial = jnp.dot(gathered, fc1_weight, preferred_element_type=jnp.float32)
    mp_count = lax.axis_size("mp")
    first_total = sum_scatter_mp(
        first_partial.astype(jnp.bfloat16).reshape(mp_count, -1, fc1_weight.shape[1]),
        1,
    )
    hidden_part = jax.nn.gelu(
        first_total + fc1_bias.astype(jnp.float32), approximate=False
    ).astype(jnp.bfloat16)
    hidden = gather_mp(hidden_part)
    second_partial = jnp.dot(hidden, fc2_weight, preferred_element_type=jnp.float32)
    embed_total = sum_scatter_groups(second_partial.astype(jnp.bfloat16)).astype(jnp.float32)
    image_embeds = (embed_total + fc2_bias.astype(jnp.float32)).astype(jnp.bfloat16)
    hits = got_place.reshape(1, -1) == jnp.arange(seq_rows, dtype=jnp.int32)[:, None]
    placed = jnp.dot(
        hits.astype(jnp.bfloat16), image_embeds, preferred_element_type=jnp.float32
    ).astype(jnp.bfloat16)
    sequence_embeds = jnp.where(jnp.any(hits, axis=1)[:, None], placed, text_embeds)
    entering = jnp.where(lax.axis_index("section") == 0, sequence_embeds, incoming).astype(
        jnp.float32
    )
    row_total = total_mp(jnp.sum(entering * entering, axis=1))
    layer_inputs = (
        entering * lax.rsqrt(row_total / HID + llm_eps)[:, None] * llm_gain.astype(jnp.float32)
    ).astype(jnp.bfloat16)
    return (sequence_embeds, layer_inputs)


LAG = 2
FC2_COLS = 512
HALF_ROOT = 0.5**0.5


def remote(src, dst, send_sem, recv_sem, device):
    return pltpu.make_async_remote_copy(
        src_ref=src,
        dst_ref=dst,
        send_sem=send_sem,
        recv_sem=recv_sem,
        device_id=device,
        device_id_type=pl.DeviceIdType.MESH,
    )


def group_device(group):
    per_section = lax.axis_size("dp")
    return {"section": group // per_section, "dp": lax.rem(group, per_section)}


def tell(device):
    pl.semaphore_signal(
        pltpu.get_barrier_semaphore(),
        inc=1,
        device_id=device,
        device_id_type=pl.DeviceIdType.MESH,
    )


def merger_kernel(
    x_ref,
    place_ref,
    sums_ref,
    w1_ref,
    b1_ref,
    w2_ref,
    b2_ref,
    img_ref,
    spot_ref,
    base_ref,
    total_ref,
    rows,
    part,
    before,
    after,
    right_out,
    left_out,
    hidden,
    give,
    take,
    keep,
    x_out,
    x_in,
    y_out,
    y_in,
    squares,
    spots,
    sums,
    base_out,
    base_in,
    totals,
    row_send,
    row_recv,
    pair_recv,
    right_send,
    right_recv,
    left_send,
    left_recv,
    give_send,
    give_recv,
    x_send,
    x_recv,
    y_send,
    y_recv,
    spot_send,
    spot_recv,
    sum_send,
    sum_recv,
    base_send,
    base_recv,
    total_send,
    total_recv,
):
    groups = lax.axis_size("section") * lax.axis_size("dp")
    sections = lax.axis_size("section")
    line = lax.axis_size("mp")
    me = lax.axis_index("mp")
    section = lax.axis_index("section")
    dp = lax.axis_index("dp")
    core = lax.rem(dp, 2)
    column = dp // 2
    wide = lax.axis_size("dp") // 2
    group = section * lax.axis_size("dp") + dp
    chips = groups // 2
    pair = {"dp": flip(dp, 1)}
    over_x = {"dp": flip(dp, 2)}
    over_y = {"section": flip(section, 1)}
    quarters = 4
    pieces = chips * quarters
    take_rows = rows.shape[2] // 2
    lag_right = me * LAG
    lag_left = (line - 1 - me) * LAG
    lag_total = (line - 1) * LAG

    for step in range(1, groups):
        tell(group_device(lax.rem(group + step, groups)))
    for step in range(1, line):
        tell({"mp": lax.rem(me + step, line)})
    pl.semaphore_wait(pltpu.get_barrier_semaphore(), groups + line - 2)

    def chip_of(quarter):
        there_x = lax.rem(quarter // 2 + column, 2)
        there_y = lax.rem(lax.rem(quarter, 2) + section, 2)
        return there_y * wide + there_x

    def group_of(quarter, at_core):
        return chip_of(quarter) * 2 + at_core

    def own_sends(chunk):
        return (
            remote(x_ref.at[chunk], rows.at[group, chunk], row_send.at[chunk, 0], row_recv.at[chunk, 1], over_y),
            remote(x_ref.at[chunk], rows.at[group, chunk], row_send.at[chunk, 1], row_recv.at[chunk, 2], over_x),
            remote(x_ref.at[chunk], rows.at[group, chunk], row_send.at[chunk, 2], pair_recv.at[chunk, 0], pair),
        )

    def forward_x(chunk):
        spot = rows.at[group_of(1, core), chunk]
        return remote(spot, spot, row_send.at[chunk, 3], row_recv.at[chunk, 3], over_x)

    def forward_pair(chunk, quarter):
        spot = rows.at[group_of(quarter, core), chunk]
        return remote(
            spot, spot, row_send.at[chunk, 3 + quarter], pair_recv.at[chunk, quarter], pair
        )

    for copy in own_sends(0):
        copy.start()

    place_copies = []
    for step in range(1, groups):
        peer = lax.rem(group + step, groups)
        copy = remote(
            place_ref.at[peer], spots.at[step], spot_send.at[step - 1], spot_recv.at[step - 1], group_device(peer)
        )
        copy.start()
        place_copies.append(copy)
    sum_copies = []
    for step in range(1, line):
        peer = lax.rem(me + step, line)
        copy = remote(sums_ref, sums.at[step], sum_send.at[step - 1], sum_recv.at[step - 1], {"mp": peer})
        copy.start()
        sum_copies.append(copy)
    spots[0] = place_ref[group]
    sums[0] = sums_ref[...]
    rows[group] = x_ref[...]

    def send_right(piece):
        return remote(
            right_out.at[piece], before.at[piece], right_send.at[piece], right_recv.at[piece], {"mp": me + 1}
        )

    def send_left(piece):
        return remote(
            left_out.at[piece], after.at[piece], left_send.at[piece], left_recv.at[piece], {"mp": me - 1}
        )

    def send_give(chunk):
        return remote(give.at[chunk], take.at[chunk], give_send.at[chunk], give_recv.at[chunk], pair)

    parts = x_send.shape[1]
    span = keep.shape[1] // parts

    def send_x(chunk, at):
        cut = pl.ds(at * span, span)
        return remote(
            x_out.at[chunk, cut], x_in.at[chunk, cut], x_send.at[chunk, at], x_recv.at[chunk, at], over_x
        )

    def send_y(at):
        cut = pl.ds(at * span, span)
        return remote(y_out.at[cut], y_in.at[cut], y_send.at[at], y_recv.at[at], over_y)

    def settle(chunk):
        send_give(chunk).wait_recv()
        mine = lax.rem(chunk, wide) == column

        @pl.when(mine)
        def _():
            @pl.loop(0, parts)
            def _(at):
                cut = pl.ds(at * span, span)
                keep[chunk, cut] = keep[chunk, cut] + take[chunk, cut].astype(jnp.float32)

        @pl.when(jnp.logical_not(mine))
        def _():
            @pl.loop(0, parts)
            def _(at):
                cut = pl.ds(at * span, span)
                x_out[chunk, cut] = (
                    keep[chunk, cut] + take[chunk, cut].astype(jnp.float32)
                ).astype(x_out.dtype)
                send_x(chunk, at).start()

    def stage(i, carry):
        @pl.when(i < pieces)
        def _():
            chunk = i // quarters
            quarter = lax.rem(i, quarters)

            @pl.when(quarter == 1)
            def _():
                remote(
                    x_ref.at[chunk], rows.at[group_of(1, core), chunk], row_send.at[chunk, 0], row_recv.at[chunk, 1], over_y
                ).wait_recv()
                forward_x(chunk).start()
                forward_pair(chunk, 1).start()

                @pl.when(chunk + 1 < chips)
                def _():
                    for copy in own_sends(chunk + 1):
                        copy.start()

            @pl.when(quarter > 1)
            def _():
                remote(
                    x_ref.at[chunk], rows.at[group_of(quarter, core), chunk], row_send.at[chunk, 1], row_recv.at[chunk, quarter], over_x
                ).wait_recv()
                forward_pair(chunk, quarter).start()

        at_dot = i - 1

        @pl.when(jnp.logical_and(at_dot >= 0, at_dot < pieces))
        def _():
            chunk = at_dot // quarters
            quarter = lax.rem(at_dot, quarters)
            spot = rows.at[group_of(quarter, 1 - core), chunk]
            remote(x_ref.at[chunk], spot, row_send.at[chunk, 2], pair_recv.at[chunk, quarter], pair).wait_recv()
            lhs = rows[pl.ds(chip_of(quarter) * 2, 2), chunk]
            part[at_dot] = jnp.dot(
                lhs.reshape(part.shape[1], lhs.shape[2]), w1_ref[...], preferred_element_type=jnp.float32
            )

        at_right = i - 1 - lag_right

        @pl.when(jnp.logical_and(me < line - 1, jnp.logical_and(at_right >= 0, at_right < pieces)))
        def _():
            @pl.when(me == 0)
            def _():
                right_out[at_right] = part[at_right].astype(right_out.dtype)

            @pl.when(me > 0)
            def _():
                send_right(at_right).wait_recv()
                right_out[at_right] = (
                    part[at_right] + before[at_right].astype(jnp.float32)
                ).astype(right_out.dtype)

            send_right(at_right).start()

        at_left = i - 1 - lag_left

        @pl.when(jnp.logical_and(me > 0, jnp.logical_and(at_left >= 0, at_left < pieces)))
        def _():
            @pl.when(me == line - 1)
            def _():
                left_out[at_left] = part[at_left].astype(left_out.dtype)

            @pl.when(me < line - 1)
            def _():
                send_left(at_left).wait_recv()
                left_out[at_left] = (
                    part[at_left] + after[at_left].astype(jnp.float32)
                ).astype(left_out.dtype)

            send_left(at_left).start()

        at_total = i - 1 - lag_total

        @pl.when(at_total >= 0)
        def _():
            chunk = at_total // quarters
            quarter = lax.rem(at_total, quarters)

            @pl.when(jnp.logical_and(quarter == 0, chunk > 0))
            def _():
                settle(chunk - 1)

            @pl.when(me == line - 1)
            def _():
                send_right(at_total).wait_recv()

            @pl.when(me == 0)
            def _():
                send_left(at_total).wait_recv()

            @pl.when(me > 0)
            def _():
                part[at_total] = part[at_total] + before[at_total].astype(jnp.float32)

            @pl.when(me < line - 1)
            def _():
                part[at_total] = part[at_total] + after[at_total].astype(jnp.float32)

            value = part[at_total] + b1_ref[...]
            value = 0.5 * value * (1.0 + lax.erf(value * HALF_ROOT))
            hidden[chunk, chip_of(quarter)] = value.astype(hidden.dtype).reshape(hidden.shape[2:])

            @pl.when(quarter == quarters - 1)
            def _():
                for_pair = hidden[chunk, :, :, 1 - core].reshape(-1, hidden.shape[5])
                for_me = hidden[chunk, :, :, core].reshape(-1, hidden.shape[5])
                count = for_me.shape[0]
                lhs = jnp.concatenate([for_pair, for_me], axis=0)

                @pl.loop(0, w2_ref.shape[1] // FC2_COLS)
                def _(at):
                    cols = pl.ds(pl.multiple_of(at * FC2_COLS, FC2_COLS), FC2_COLS)
                    result = jnp.dot(lhs, w2_ref[:, cols], preferred_element_type=jnp.float32)
                    give[chunk, :, cols] = result[:count].astype(give.dtype)
                    keep[chunk, :, cols] = result[count:]

                send_give(chunk).start()

        return carry

    lax.fori_loop(0, pieces + 1 + lag_total, stage, 0)
    settle(chips - 1)

    for copy in sum_copies:
        copy.wait_recv()
    sum_rows = base_out.shape[0]
    both = sums[0]
    for step in range(1, line):
        both = both + sums[step]
    base_out[...] = both[sum_rows:]
    base_ref[...] = both[:sum_rows]
    send_base = remote(base_out, base_in, base_send, base_recv, {"section": section + 1})

    @pl.when(section < sections - 1)
    def _():
        send_base.start()

    spot_sum = spots[0]
    for copy in place_copies:
        copy.wait_recv()
    for step in range(1, groups):
        spot_sum = spot_sum + spots[step]
    spot_ref[...] = spot_sum

    @pl.when(section > 0)
    def _():
        send_base.wait_recv()
        base_ref[...] = base_in[...]

    own_chunk = section * wide + column
    y_chunk = flip(section, 1) * wide + column

    @pl.loop(0, parts)
    def _(at):
        cut = pl.ds(at * span, span)
        send_x(y_chunk, at).wait_recv()
        y_out[cut] = (keep[y_chunk, cut] + x_in[y_chunk, cut].astype(jnp.float32)).astype(y_out.dtype)
        send_y(at).start()

    @pl.loop(0, parts)
    def _(at):
        cut = pl.ds(at * span, span)
        send_x(own_chunk, at).wait_recv()
        send_y(at).wait_recv()
        value = (
            keep[own_chunk, cut]
            + x_in[own_chunk, cut].astype(jnp.float32)
            + y_in[cut].astype(jnp.float32)
            + b2_ref[...]
        ).astype(img_ref.dtype)
        img_ref[cut] = value
        value = value.astype(jnp.float32)
        square = value * value
        width = squares.shape[1]
        folded = square[:, :width]
        for at_col in range(1, square.shape[1] // width):
            folded = folded + square[:, at_col * width : (at_col + 1) * width]
        squares[cut] = folded

    totals[0] = jnp.sum(squares[...].T, axis=0, keepdims=True)
    total_copies = []
    for step in range(1, line):
        copy = remote(
            totals.at[0], totals.at[step], total_send.at[step - 1], total_recv.at[step - 1], {"mp": lax.rem(me + step, line)}
        )
        copy.start()
        total_copies.append(copy)

    for chunk in range(chips):
        for copy in own_sends(chunk):
            copy.wait_send()
        forward_x(chunk).wait_send()
        for quarter in range(1, quarters):
            forward_pair(chunk, quarter).wait_send()
        send_give(chunk).wait_send()

        @pl.when(chunk % wide != column)
        def _():
            for at in range(parts):
                send_x(chunk, at).wait_send()

    for at in range(parts):
        send_y(at).wait_send()

    @pl.when(me < line - 1)
    def _():
        @pl.loop(0, pieces)
        def _(piece):
            send_right(piece).wait_send()

    @pl.when(me > 0)
    def _():
        @pl.loop(0, pieces)
        def _(piece):
            send_left(piece).wait_send()

    for copy in place_copies + sum_copies:
        copy.wait_send()

    @pl.when(section < sections - 1)
    def _():
        send_base.wait_send()

    row_total = totals[0]
    for step, copy in enumerate(total_copies):
        copy.wait()
        row_total = row_total + totals[step + 1]
    total_ref[...] = row_total


def merger(rows, places, sums, w1, b1, w2, b2):
    groups = lax.axis_size("section") * lax.axis_size("dp")
    line = lax.axis_size("mp")
    chips = groups // 2
    chunk_rows = rows.shape[0] // chips
    run = chunk_rows // 2
    width = rows.shape[1]
    units = w1.shape[1]
    features = w2.shape[1]
    pieces = chips * 4
    piece_rows = 2 * chunk_rows
    target_rows = groups * run
    parts = 4
    low = jnp.bfloat16
    dma = pltpu.SemaphoreType.DMA
    sum_rows = sums.shape[0] // 2
    return pl.pallas_call(
        merger_kernel,
        out_shape=(
            jax.ShapeDtypeStruct((target_rows, features), low),
            jax.ShapeDtypeStruct(places.shape[1:], jnp.int32),
            jax.ShapeDtypeStruct((sum_rows, sums.shape[1]), jnp.float32),
            jax.ShapeDtypeStruct((1, target_rows), jnp.float32),
        ),
        in_specs=[pl.BlockSpec(memory_space=pltpu.VMEM)] * 7,
        out_specs=[pl.BlockSpec(memory_space=pltpu.VMEM)] * 4,
        scratch_shapes=[
            pltpu.VMEM((groups, chips, chunk_rows, width), low),
            pltpu.VMEM((pieces, piece_rows, units), jnp.float32),
            pltpu.VMEM((pieces, piece_rows, units), low),
            pltpu.VMEM((pieces, piece_rows, units), low),
            pltpu.VMEM((pieces, piece_rows, units), low),
            pltpu.VMEM((pieces, piece_rows, units), low),
            pltpu.VMEM((chips, chips, 2, 2, run, units), low),
            pltpu.VMEM((chips, target_rows, features), low),
            pltpu.VMEM((chips, target_rows, features), low),
            pltpu.VMEM((chips, target_rows, features), jnp.float32),
            pltpu.VMEM((chips, target_rows, features), low),
            pltpu.VMEM((chips, target_rows, features), low),
            pltpu.VMEM((target_rows, features), low),
            pltpu.VMEM((target_rows, features), low),
            pltpu.VMEM((target_rows, 128), jnp.float32),
            pltpu.VMEM(places.shape, jnp.int32),
            pltpu.VMEM((line,) + sums.shape, jnp.float32),
            pltpu.VMEM((sum_rows, sums.shape[1]), jnp.float32),
            pltpu.VMEM((sum_rows, sums.shape[1]), jnp.float32),
            pltpu.VMEM((line, 1, target_rows), jnp.float32),
            dma((chips, 7)),
            dma((chips, 4)),
            dma((chips, 4)),
            dma((pieces,)),
            dma((pieces,)),
            dma((pieces,)),
            dma((pieces,)),
            dma((chips,)),
            dma((chips,)),
            dma((chips, parts)),
            dma((chips, parts)),
            dma((parts,)),
            dma((parts,)),
            dma((groups - 1,)),
            dma((groups - 1,)),
            dma((line - 1,)),
            dma((line - 1,)),
            dma,
            dma,
            dma((line - 1,)),
            dma((line - 1,)),
        ],
        cost_estimate=pl.CostEstimate(
            flops=10**11, bytes_accessed=10**7, transcendentals=0
        ),
        compiler_params=pltpu.CompilerParams(
            collective_id=6, has_side_effects=True, vmem_limit_bytes=VMEM_LIMIT
        ),
    )(rows.reshape(chips, chunk_rows, width), places, sums, w1, b1, w2, b2)


def placing_kernel(text_ref, incoming_ref, img_ref, spot_ref, total_ref, base_ref, gain_ref, seq_ref, layer_ref):
    height = text_ref.shape[0]
    at_row = pl.program_id(0) * height + lax.broadcasted_iota(jnp.int32, (height, spot_ref.shape[1]), 0)
    hits = spot_ref[...] == at_row
    hit = jnp.max(hits.astype(jnp.float32), axis=1, keepdims=True) > 0.0
    placed = jnp.dot(
        hits.astype(jnp.bfloat16), img_ref[...], preferred_element_type=jnp.float32
    ).astype(jnp.bfloat16)
    sequence = jnp.where(hit, placed, text_ref[...])
    seq_ref[...] = sequence
    gain = gain_ref[...].astype(jnp.float32)
    base = base_ref[...]

    @pl.when(lax.axis_index("section") == 0)
    def _():
        total = jnp.sum(jnp.where(hits, total_ref[...], 0.0), axis=1, keepdims=True)
        total = jnp.where(hit, total, base)
        scale = lax.rsqrt(total / HID + llm_eps)
        layer_ref[...] = (sequence.astype(jnp.float32) * scale * gain).astype(layer_ref.dtype)

    @pl.when(lax.axis_index("section") > 0)
    def _():
        scale = lax.rsqrt(base / HID + llm_eps)
        layer_ref[...] = (incoming_ref[...].astype(jnp.float32) * scale * gain).astype(layer_ref.dtype)


def placing(text, incoming, img, spot, total, base, gain):
    rows, features = text.shape
    height = rows // 8
    block = pl.BlockSpec((height, features), lambda i: (i, 0))

    def whole(value):
        return pl.BlockSpec(value.shape, lambda i: (0, 0))

    return pl.pallas_call(
        placing_kernel,
        grid=(rows // height,),
        out_shape=(jax.ShapeDtypeStruct(text.shape, text.dtype),) * 2,
        in_specs=[
            block,
            block,
            whole(img),
            whole(spot),
            whole(total),
            pl.BlockSpec((height, 1), lambda i: (i, 0)),
            whole(gain),
        ],
        out_specs=(block, block),
        cost_estimate=pl.CostEstimate(flops=10**9, bytes_accessed=10**7, transcendentals=0),
    )(text, incoming, img, spot, total, base, gain)


def per_device(*operands):
    (patches, patch_counts, dest_rows, qkv_weight, out_weight, attn_gain, merge_gain) = operands[:7]
    (fc1_weight, fc1_bias, fc2_weight, fc2_bias, text_embeds, section_hidden, llm_gain) = operands[7:]
    outer, _ = group_bits()
    group_count = lax.axis_size("section") * lax.axis_size("dp")
    merged_rows = patches.shape[0] // 4
    run_cap = merged_rows // group_count
    seq_rows = text_embeds.shape[0]
    held = group_count * merged_rows * patches.shape[1] * patches.dtype.itemsize
    if outer != [("dp", 2), ("section", 1)] or held > KERNEL_BYTES or run_cap % 16 or merged_rows % 128 or seq_rows % 128:
        return plain_per_device(*operands)
    width = patches.shape[1]
    tile_total = patch_counts.shape[0]
    block_rows = patches.shape[0] // tile_total
    local_cols = qkv_weight.shape[2]
    local_heads = local_cols // HEAD_DIM
    run_total = group_count
    incoming = from_behind(section_hidden, "section", 1)
    runs = dest_rows.reshape(run_total, run_cap)
    run_target = runs[:, 0] // seq_rows
    takes = jnp.arange(group_count, dtype=jnp.int32)[:, None] == run_target[None, :]
    tile_slots = block_rows // 4
    live = (
        jnp.arange(tile_slots, dtype=jnp.int32)[None, :] * 4 < patch_counts[:, None]
    ).reshape(run_total, run_cap)
    place = jnp.where(live, runs % seq_rows - seq_rows, 0)
    send_place = jnp.sum(jnp.where(takes[:, :, None], place[None], 0), axis=1) + seq_rows
    my_group = lax.axis_index("section") * lax.axis_size("dp") + lax.axis_index("dp")
    at_lane = jnp.arange(merged_rows, dtype=jnp.int32)
    places = jnp.where(
        (at_lane // run_cap == my_group)[None, :], jnp.tile(send_place, (1, group_count)), 0
    )[:, None, :]

    def square_sums(value):
        value = value.astype(jnp.float32)
        return jnp.sum(value * value, axis=1).reshape(-1, 128)

    sums = jnp.concatenate([square_sums(text_embeds), square_sums(section_hidden)], axis=0)

    normed_in = layer_norm(patches, attn_gain).astype(jnp.bfloat16)
    projections = jnp.dot(
        normed_in, qkv_weight.reshape(width, 3 * local_cols), preferred_element_type=jnp.float32
    ).astype(jnp.bfloat16)
    projections = projections.reshape(tile_total, block_rows, 3, local_heads, HEAD_DIM)
    query_part = projections[:, :, 0]
    key_part = projections[:, :, 1]
    value_part = projections[:, :, 2]
    scores = jnp.einsum(
        "tqhd,tkhd->thqk", query_part, key_part, preferred_element_type=jnp.float32
    ) * HEAD_DIM ** (-0.5)
    key_live = (
        jnp.arange(block_rows, dtype=jnp.int32)[None, None, None, :]
        < patch_counts[:, None, None, None]
    )
    scores = jnp.where(key_live, scores, -1e30)
    weights = jax.nn.softmax(scores, axis=-1).astype(jnp.bfloat16)
    attended = jnp.einsum(
        "thqk,tkhd->tqhd", weights, value_part, preferred_element_type=jnp.float32
    ).astype(jnp.bfloat16)
    attended = attended.reshape(patches.shape[0], local_cols)
    lane_source = jnp.arange(run_total, dtype=jnp.int32)[None, :] * run_cap
    run_source = jnp.sum(jnp.where(takes, lane_source, 0), axis=1)
    row_source = (
        run_source[:, None] + jnp.arange(run_cap, dtype=jnp.int32)[None, :]
    ).reshape(-1) * 4
    slots_at = jnp.arange(patches.shape[0], dtype=jnp.int32)
    patch_at = jnp.arange(4, dtype=jnp.int32)
    order = (
        (row_source[None, :] + patch_at[:, None]).reshape(-1)[:, None] == slots_at[None, :]
    ).astype(jnp.bfloat16)
    own_order = (
        (row_source + lax.axis_index("mp"))[:, None] == slots_at[None, :]
    ).astype(jnp.bfloat16)
    ordered = jnp.dot(order, attended, preferred_element_type=jnp.float32).astype(jnp.bfloat16)
    own_patch = jnp.dot(own_order, patches, preferred_element_type=jnp.float32)
    partial_proj = jnp.dot(ordered, out_weight, preferred_element_type=jnp.float32)
    own_proj = sum_scatter_mp(
        partial_proj.astype(jnp.bfloat16).reshape(4, merged_rows, width), 0
    )
    block_out = (own_patch + own_proj).astype(jnp.bfloat16)
    merge_part = layer_norm(block_out, merge_gain).astype(jnp.bfloat16)
    img, spot, base, total = merger(
        merge_part,
        places,
        sums,
        fc1_weight,
        fc1_bias.astype(jnp.float32)[None, :],
        fc2_weight,
        fc2_bias.astype(jnp.float32)[None, :],
    )
    return placing(
        text_embeds, incoming, img, spot, total, base.reshape(-1, 1), llm_gain[None, :]
    )


def solution(mesh):
    in_specs = (
        P(("section", "dp"), None),
        P(("section", "dp")),
        P(("section", "dp")),
        P(None, None, "mp"),
        P("mp", None),
        P(),
        P(),
        P("mp", ("section", "dp")),
        P(("section", "dp")),
        P(("section", "dp"), "mp"),
        P("mp"),
        P(("section", "dp"), "mp"),
        P(("section", "dp"), "mp"),
        P("mp"),
    )
    out_specs = (P(("section", "dp"), "mp"), P(("section", "dp"), "mp"))
    return jax.shard_map(
        per_device, mesh=mesh, in_specs=in_specs, out_specs=out_specs, check_vma=False
    )
```

```python
import functools
import math

import jax
import jax.numpy as jnp
from jax import lax
from jax.experimental import pallas as pl
from jax.experimental.pallas import tpu as pltpu
from jax.sharding import PartitionSpec as P

HEAD_DIM = 80
HID = 8192


vit_eps = 1e-06
llm_eps = 1e-06


def from_behind(value, axis, steps):
    count = lax.axis_size(axis)
    first, last = (max(0, -steps), min(count, count - steps))
    return lax.ppermute(value, axis, [(source, source + steps) for source in range(first, last)])


def layer_norm(values, gain):
    centred = values.astype(jnp.float32)
    centred = centred - jnp.mean(centred, axis=-1, keepdims=True)
    variance = jnp.mean(centred * centred, axis=-1, keepdims=True)
    return centred * lax.rsqrt(variance + vit_eps) * gain.astype(jnp.float32)


VMEM_LIMIT = 60 * 1024 * 1024
KERNEL_BYTES = 8 * 1024 * 1024


def vmem_call(kernel, out, scratch, sent_bytes, ident, *operands):
    return pl.pallas_call(
        kernel,
        out_shape=out,
        in_specs=[pl.BlockSpec(memory_space=pltpu.VMEM)] * len(operands),
        out_specs=pl.BlockSpec(memory_space=pltpu.VMEM),
        scratch_shapes=scratch,
        cost_estimate=pl.CostEstimate(
            flops=sent_bytes * 20000, bytes_accessed=sent_bytes * 2, transcendentals=0
        ),
        compiler_params=pltpu.CompilerParams(
            collective_id=ident, has_side_effects=True, vmem_limit_bytes=VMEM_LIMIT
        ),
    )(*operands)


def exchange_kernel(count, spread, x_ref, o_ref, send_sem, recv_sem, own_sem):
    me = lax.axis_index("mp")
    barrier = pltpu.get_barrier_semaphore()
    for step in range(1, count):
        peer = lax.rem(me + step, count)
        pl.semaphore_signal(
            barrier, inc=1, device_id={"mp": peer}, device_id_type=pl.DeviceIdType.MESH
        )
    pl.semaphore_wait(barrier, count - 1)
    copies = []
    for step in sorted(range(1, count), key=lambda s: -min(s, count - s)):
        peer = lax.rem(me + step, count)
        copy = pltpu.make_async_remote_copy(
            src_ref=x_ref.at[peer] if spread else x_ref,
            dst_ref=o_ref.at[me],
            send_sem=send_sem.at[step - 1],
            recv_sem=recv_sem.at[step - 1],
            device_id={"mp": peer},
            device_id_type=pl.DeviceIdType.MESH,
        )
        copy.start()
        copies.append(copy)
    own = pltpu.make_async_copy(x_ref.at[me] if spread else x_ref, o_ref.at[me], own_sem)
    own.start()
    own.wait()
    for copy in copies:
        copy.wait()


def relay_kernel(count, x_ref, o_ref, send_sem, recv_sem, own_sem):
    me = lax.axis_index("mp")
    barrier = pltpu.get_barrier_semaphore()
    for step in range(1, count):
        peer = lax.rem(me + step, count)
        pl.semaphore_signal(
            barrier, inc=1, device_id={"mp": peer}, device_id_type=pl.DeviceIdType.MESH
        )
    pl.semaphore_wait(barrier, count - 1)
    own = pltpu.make_async_copy(x_ref, o_ref.at[me], own_sem)
    own.start()

    def hop(way, step):
        owner = lax.rem(me - way * step + count, count)
        return pltpu.make_async_remote_copy(
            src_ref=o_ref.at[owner] if step else x_ref,
            dst_ref=o_ref.at[owner],
            send_sem=send_sem.at[(way + 1) // 2, step],
            recv_sem=recv_sem.at[(way + 1) // 2, step],
            device_id={"mp": lax.rem(me + way + count, count)},
            device_id_type=pl.DeviceIdType.MESH,
        )

    def holds(way, step):
        return me >= step if way > 0 else me + step < count

    def sends(way):
        return me < count - 1 if way > 0 else me > 0

    for step in range(count):
        for way in (1, -1):
            if step:

                @pl.when(holds(way, step))
                def _():
                    owner = lax.rem(me - way * step + count, count)
                    pltpu.make_async_remote_copy(
                        src_ref=x_ref,
                        dst_ref=o_ref.at[owner],
                        send_sem=send_sem.at[(way + 1) // 2, step - 1],
                        recv_sem=recv_sem.at[(way + 1) // 2, step - 1],
                        device_id={"mp": lax.rem(me - way + count, count)},
                        device_id_type=pl.DeviceIdType.MESH,
                    ).wait_recv()

            if step < count - 1:

                @pl.when(jnp.logical_and(holds(way, step), sends(way)))
                def _():
                    hop(way, step).start()

    own.wait()
    for step in range(count - 1):
        for way in (1, -1):

            @pl.when(jnp.logical_and(holds(way, step), sends(way)))
            def _():
                hop(way, step).wait_send()


def relay_mp(value, ident):
    count = lax.axis_size("mp")
    return vmem_call(
        functools.partial(relay_kernel, count),
        jax.ShapeDtypeStruct((count,) + value.shape, value.dtype),
        [
            pltpu.SemaphoreType.DMA((2, count - 1)),
            pltpu.SemaphoreType.DMA((2, count - 1)),
            pltpu.SemaphoreType.DMA,
        ],
        count * value.size * value.dtype.itemsize,
        ident,
        value,
    )


def exchange_mp(value, spread, ident):
    count = lax.axis_size("mp")
    shape = value.shape if spread else (count,) + value.shape
    size = math.prod(shape) * value.dtype.itemsize
    return vmem_call(
        functools.partial(exchange_kernel, count, spread),
        jax.ShapeDtypeStruct(shape, value.dtype),
        [
            pltpu.SemaphoreType.DMA((count - 1,)),
            pltpu.SemaphoreType.DMA((count - 1,)),
            pltpu.SemaphoreType.DMA,
        ],
        size,
        ident,
        value,
    )


def sum_scatter_mp(blocks, ident):
    return jnp.sum(exchange_mp(blocks, True, ident).astype(jnp.float32), axis=0)


def gather_mp(value):
    got = relay_mp(value, 2)
    return got.reshape((-1,) + value.shape[1:])


def total_mp(value):
    return jnp.sum(exchange_mp(value.reshape(-1, 128), False, 3), axis=0).reshape(-1)


def flip(index, bit):
    return index + bit * (1 - 2 * (index // bit % 2))


def group_bits():
    outer = [("dp", 1 << k) for k in range(1, lax.axis_size("dp").bit_length() - 1)]
    outer += [("section", 1 << k) for k in range(lax.axis_size("section").bit_length() - 1)]
    return outer, ("dp", 1)


def meets(axis, bit):
    return {axis: flip(lax.axis_index(axis), bit)}


def group_at(mask):
    spots = {axis: lax.axis_index(axis) for axis in ("section", "dp")}
    for axis, bit in mask:
        spots[axis] = flip(spots[axis], bit)
    return spots["section"] * lax.axis_size("dp") + spots["dp"]


def greet(bits):
    barrier = pltpu.get_barrier_semaphore()
    for axis, bit in bits:
        pl.semaphore_signal(
            barrier, inc=1, device_id=meets(axis, bit), device_id_type=pl.DeviceIdType.MESH
        )
    pl.semaphore_wait(barrier, len(bits))


def gather_kernel(x_ref, o_ref, send_sem, recv_sem, own_sem):
    outer, last = group_bits()
    greet(outer + [last])
    half = x_ref.shape[1] // 2
    sent, waiting = [], []
    slots = iter(range(send_sem.shape[0]))

    def pass_on(mask, stage, part, order):
        cols = pl.ds(part * half, half)
        spot = group_at(mask)
        source = o_ref.at[spot, :, cols] if mask else x_ref.at[:, cols]
        for later in range(stage, len(order)):
            slot = next(slots)
            copy = pltpu.make_async_remote_copy(
                src_ref=source,
                dst_ref=o_ref.at[spot, :, cols],
                send_sem=send_sem.at[slot],
                recv_sem=recv_sem.at[slot],
                device_id=meets(*order[later]),
                device_id_type=pl.DeviceIdType.MESH,
            )
            copy.start()
            sent.append(copy)
            waiting.append((later, copy, mask + [order[later]], part, order))

    pass_on([], 0, 0, outer + [last])
    pass_on([], 0, 1, outer[::-1] + [last])
    own = pltpu.make_async_copy(x_ref, o_ref.at[group_at([])], own_sem)
    own.start()
    while waiting:
        first = min(range(len(waiting)), key=lambda at: waiting[at][0])
        stage, copy, mask, part, order = waiting.pop(first)
        copy.wait_recv()
        pass_on(mask, stage + 1, part, order)
    for copy in sent:
        copy.wait_send()
    own.wait()


def gather_groups(value):
    count = lax.axis_size("section") * lax.axis_size("dp")
    size = count * value.size * value.dtype.itemsize
    if size > KERNEL_BYTES:
        return lax.all_gather(value, ("section", "dp"), axis=0, tiled=True)
    slots = 2 * (count - 1)
    got = vmem_call(
        gather_kernel,
        jax.ShapeDtypeStruct((count,) + value.shape, value.dtype),
        [
            pltpu.SemaphoreType.DMA((slots,)),
            pltpu.SemaphoreType.DMA((slots,)),
            pltpu.SemaphoreType.DMA,
        ],
        size,
        4,
        value,
    )
    return got.reshape(-1, value.shape[1])


def scatter_kernel(x_ref, o_ref, held, taken, send_sem, recv_sem):
    outer, first = group_bits()
    greet(outer + [first])
    rows = x_ref.shape[1]
    half = x_ref.shape[2] // 2
    chunk = 32
    orders = ([first] + outer, [first] + outer[::-1])
    slots = iter(range(send_sem.shape[0]))
    masks = [[]]
    for bit in outer:
        masks = masks + [mask + [bit] for mask in masks]
    place_of = {frozenset(mask): at for at, mask in enumerate(masks)}
    base = len(masks)
    live = {}

    def send(part, stage):
        cols = pl.ds(part * half, half)
        bit = orders[part][stage]
        kept = orders[part][stage + 1 :]
        copies = []
        for mask in [m for m in masks if set(m) <= set(kept)]:
            if stage == 0:
                source = x_ref.at[group_at(mask + [bit]), :, cols]
            else:
                source = held.at[place_of[frozenset(mask + [bit])], :, cols]
            landing = 2 * base - 2 ** (len(kept) + 1) + [
                m for m in masks if set(m) <= set(kept)
            ].index(mask)
            slot = next(slots)
            copy = pltpu.make_async_remote_copy(
                src_ref=source,
                dst_ref=taken.at[landing, :, cols],
                send_sem=send_sem.at[slot],
                recv_sem=recv_sem.at[slot],
                device_id=meets(*bit),
                device_id_type=pl.DeviceIdType.MESH,
            )
            copy.start()
            copies.append((copy, mask, landing))
        live[part, stage] = copies

    def add(part, stage):
        cols = pl.ds(part * half, half)
        final = stage + 1 == len(orders[part])
        following = None if final else orders[part][stage + 1]
        copies = live[part, stage]
        for copy, mask, landing in sorted(copies, key=lambda c: following not in c[1]):
            copy.wait_recv()
            at = place_of[frozenset(mask)]
            spot = group_at(mask)

            @pl.loop(0, rows // chunk)
            def _(step):
                span = pl.ds(step * chunk, chunk)
                mine = x_ref[spot, span, cols] if stage == 0 else held[at, span, cols]
                total = mine.astype(jnp.float32) + taken[landing, span, cols].astype(jnp.float32)
                if final:
                    o_ref[span, cols] = total
                else:
                    held[at, span, cols] = total.astype(held.dtype)

    send(0, 0)
    send(1, 0)
    for stage in range(len(orders[0])):
        for part in (0, 1):
            add(part, stage)
            if stage + 1 < len(orders[0]):
                send(part, stage + 1)
    for copies in live.values():
        for copy, _, _ in copies:
            copy.wait_send()


def sum_scatter_groups(value):
    count = lax.axis_size("section") * lax.axis_size("dp")
    size = value.size * value.dtype.itemsize
    if size > KERNEL_BYTES:
        return lax.psum_scatter(value, ("section", "dp"), scatter_dimension=0, tiled=True)
    rows, cols = value.shape[0] // count, value.shape[1]
    slots = 2 * (count - 1)
    return vmem_call(
        scatter_kernel,
        jax.ShapeDtypeStruct((rows, cols), jnp.float32),
        [
            pltpu.VMEM((count // 2, rows, cols), value.dtype),
            pltpu.VMEM((count - 1, rows, cols), value.dtype),
            pltpu.SemaphoreType.DMA((slots,)),
            pltpu.SemaphoreType.DMA((slots,)),
        ],
        size,
        5,
        value.reshape(count, rows, cols),
    )


def plain_per_device(
    patches,
    patch_counts,
    dest_rows,
    qkv_weight,
    out_weight,
    attn_gain,
    merge_gain,
    fc1_weight,
    fc1_bias,
    fc2_weight,
    fc2_bias,
    text_embeds,
    section_hidden,
    llm_gain,
):
    width = patches.shape[1]
    tile_total = patch_counts.shape[0]
    block_rows = patches.shape[0] // tile_total
    merged_rows = patches.shape[0] // 4
    local_cols = qkv_weight.shape[2]
    local_heads = local_cols // HEAD_DIM
    feature_cols = text_embeds.shape[1]
    seq_rows = text_embeds.shape[0]
    section_count = lax.axis_size("section")
    group_count = section_count * lax.axis_size("dp")
    run_cap = max(2, merged_rows // group_count)
    run_total = merged_rows // run_cap
    run_target = dest_rows.reshape(run_total, run_cap)[:, 0] // seq_rows
    takes = jnp.arange(group_count, dtype=jnp.int32)[:, None] == run_target[None, :]
    slot_in_tile = jnp.arange(merged_rows, dtype=jnp.int32) % (block_rows // 4)
    tile_counts = jnp.repeat(patch_counts, block_rows // 4, total_repeat_length=merged_rows)
    live = slot_in_tile * 4 < tile_counts
    place = jnp.where(live, dest_rows % seq_rows - seq_rows, 0).reshape(run_total, run_cap)
    send_place = jnp.sum(jnp.where(takes[:, :, None], place[None], 0), axis=1) + seq_rows
    got_place = lax.all_to_all(send_place, ("section", "dp"), split_axis=0, concat_axis=0, tiled=True)
    incoming = from_behind(section_hidden, "section", 1)
    normed_in = layer_norm(patches, attn_gain).astype(jnp.bfloat16)
    projections = jnp.dot(
        normed_in, qkv_weight.reshape(width, 3 * local_cols), preferred_element_type=jnp.float32
    ).astype(jnp.bfloat16)
    projections = projections.reshape(tile_total, block_rows, 3, local_heads, HEAD_DIM)
    query_part = projections[:, :, 0]
    key_part = projections[:, :, 1]
    value_part = projections[:, :, 2]
    scores = jnp.einsum(
        "tqhd,tkhd->thqk", query_part, key_part, preferred_element_type=jnp.float32
    ) * HEAD_DIM ** (-0.5)
    key_live = (
        jnp.arange(block_rows, dtype=jnp.int32)[None, None, None, :]
        < patch_counts[:, None, None, None]
    )
    scores = jnp.where(key_live, scores, -1e30)
    weights = jax.nn.softmax(scores, axis=-1).astype(jnp.bfloat16)
    attended = jnp.einsum(
        "thqk,tkhd->tqhd", weights, value_part, preferred_element_type=jnp.float32
    ).astype(jnp.bfloat16)
    attended = attended.reshape(patches.shape[0], local_cols)
    lane_source = jnp.arange(run_total, dtype=jnp.int32)[None, :] * run_cap
    run_source = jnp.sum(jnp.where(takes, lane_source, 0), axis=1)
    row_source = (
        run_source[:, None] + jnp.arange(run_cap, dtype=jnp.int32)[None, :]
    ).reshape(-1) * 4
    slots_at = jnp.arange(patches.shape[0], dtype=jnp.int32)
    patch_at = jnp.arange(4, dtype=jnp.int32)
    order = (
        (row_source[None, :] + patch_at[:, None]).reshape(-1)[:, None] == slots_at[None, :]
    ).astype(jnp.bfloat16)
    own_order = (
        (row_source + lax.axis_index("mp"))[:, None] == slots_at[None, :]
    ).astype(jnp.bfloat16)
    ordered = jnp.dot(order, attended, preferred_element_type=jnp.float32).astype(jnp.bfloat16)
    own_patch = jnp.dot(own_order, patches, preferred_element_type=jnp.float32)
    partial_proj = jnp.dot(ordered, out_weight, preferred_element_type=jnp.float32)
    own_proj = sum_scatter_mp(
        partial_proj.astype(jnp.bfloat16).reshape(4, group_count * run_cap, width), 0
    )
    block_out = (own_patch + own_proj).astype(jnp.bfloat16)
    merge_part = layer_norm(block_out, merge_gain).astype(jnp.bfloat16)
    slot_rows = group_count * run_cap
    gathered = gather_groups(merge_part)
    gathered = (
        gathered.reshape(group_count, group_count, run_cap, width)
        .transpose(1, 0, 2, 3)
        .reshape(group_count * slot_rows, width)
    )
    first_partial = jnp.dot(gathered, fc1_weight, preferred_element_type=jnp.float32)
    mp_count = lax.axis_size("mp")
    first_total = sum_scatter_mp(
        first_partial.astype(jnp.bfloat16).reshape(mp_count, -1, fc1_weight.shape[1]),
        1,
    )
    hidden_part = jax.nn.gelu(
        first_total + fc1_bias.astype(jnp.float32), approximate=False
    ).astype(jnp.bfloat16)
    hidden = gather_mp(hidden_part)
    second_partial = jnp.dot(hidden, fc2_weight, preferred_element_type=jnp.float32)
    embed_total = sum_scatter_groups(second_partial.astype(jnp.bfloat16)).astype(jnp.float32)
    image_embeds = (embed_total + fc2_bias.astype(jnp.float32)).astype(jnp.bfloat16)
    hits = got_place.reshape(1, -1) == jnp.arange(seq_rows, dtype=jnp.int32)[:, None]
    placed = jnp.dot(
        hits.astype(jnp.bfloat16), image_embeds, preferred_element_type=jnp.float32
    ).astype(jnp.bfloat16)
    sequence_embeds = jnp.where(jnp.any(hits, axis=1)[:, None], placed, text_embeds)
    entering = jnp.where(lax.axis_index("section") == 0, sequence_embeds, incoming).astype(
        jnp.float32
    )
    row_total = total_mp(jnp.sum(entering * entering, axis=1))
    layer_inputs = (
        entering * lax.rsqrt(row_total / HID + llm_eps)[:, None] * llm_gain.astype(jnp.float32)
    ).astype(jnp.bfloat16)
    return (sequence_embeds, layer_inputs)


LAG = 3
FC2_COLS = 512
HALF_ROOT = 0.5**0.5


def remote(src, dst, send_sem, recv_sem, device):
    return pltpu.make_async_remote_copy(
        src_ref=src,
        dst_ref=dst,
        send_sem=send_sem,
        recv_sem=recv_sem,
        device_id=device,
        device_id_type=pl.DeviceIdType.MESH,
    )


def group_device(group):
    per_section = lax.axis_size("dp")
    return {"section": group // per_section, "dp": lax.rem(group, per_section)}


def tell(device):
    pl.semaphore_signal(
        pltpu.get_barrier_semaphore(),
        inc=1,
        device_id=device,
        device_id_type=pl.DeviceIdType.MESH,
    )


def merger_kernel(
    patches_ref,
    counts_ref,
    key_ref,
    qkv_ref,
    wo_ref,
    attn_gain_ref,
    merge_gain_ref,
    place_ref,
    sums_ref,
    w1_hbm,
    b1_ref,
    w2_hbm,
    b2_ref,
    img_ref,
    spot_ref,
    base_ref,
    total_ref,
    query,
    key,
    value_part,
    attended,
    ordered,
    arrived,
    wo_all,
    x_ref,
    w1_ref,
    w2_ref,
    weight_sem,
    wo_send,
    wo_recv,
    wo_out,
    wo_plane,
    wo_pair,
    a_send,
    a_recv,
    rows,
    part,
    before,
    after,
    right_out,
    left_out,
    hidden,
    give,
    take,
    keep,
    x_out,
    x_in,
    y_out,
    y_in,
    squares,
    spots,
    sums,
    base_out,
    base_in,
    totals,
    row_send,
    row_recv,
    pair_recv,
    right_send,
    right_recv,
    left_send,
    left_recv,
    give_send,
    give_recv,
    x_send,
    x_recv,
    y_send,
    y_recv,
    spot_send,
    spot_recv,
    sum_send,
    sum_recv,
    base_send,
    base_recv,
    total_send,
    total_recv,
):
    groups = lax.axis_size("section") * lax.axis_size("dp")
    sections = lax.axis_size("section")
    line = lax.axis_size("mp")
    me = lax.axis_index("mp")
    section = lax.axis_index("section")
    dp = lax.axis_index("dp")
    core = lax.rem(dp, 2)
    column = dp // 2
    wide = lax.axis_size("dp") // 2
    group = section * lax.axis_size("dp") + dp
    chips = groups // 2
    pair = {"dp": flip(dp, 1)}
    over_x = {"dp": flip(dp, 2)}
    over_y = {"section": flip(section, 1)}
    quarters = 4
    pieces = chips * quarters
    take_rows = rows.shape[2] // 2
    lag_right = me * LAG
    lag_left = (line - 1 - me) * LAG
    lag_total = (line - 1) * LAG

    for step in range(1, groups):
        tell(group_device(lax.rem(group + step, groups)))
    for step in range(1, line):
        tell({"mp": lax.rem(me + step, line)})
    pl.semaphore_wait(pltpu.get_barrier_semaphore(), groups + line - 2)

    def chip_of(quarter):
        there_x = lax.rem(quarter // 2 + column, 2)
        there_y = lax.rem(lax.rem(quarter, 2) + section, 2)
        return there_y * wide + there_x

    def group_of(quarter, at_core):
        return chip_of(quarter) * 2 + at_core

    def own_sends(chunk):
        return (
            remote(x_ref.at[chunk], rows.at[group, chunk], row_send.at[chunk, 0], row_recv.at[chunk, 1], over_y),
            remote(x_ref.at[chunk], rows.at[group, chunk], row_send.at[chunk, 1], row_recv.at[chunk, 2], over_x),
            remote(x_ref.at[chunk], rows.at[group, chunk], row_send.at[chunk, 2], pair_recv.at[chunk, 0], pair),
        )

    def forward_x(chunk):
        spot = rows.at[group_of(1, core), chunk]
        return remote(spot, spot, row_send.at[chunk, 3], row_recv.at[chunk, 3], over_x)

    def forward_pair(chunk, quarter):
        spot = rows.at[group_of(quarter, core), chunk]
        return remote(
            spot, spot, row_send.at[chunk, 3 + quarter], pair_recv.at[chunk, quarter], pair
        )

    fetches = [
        pltpu.make_async_copy(w1_hbm, w1_ref, weight_sem.at[0]),
        pltpu.make_async_copy(w2_hbm, w2_ref, weight_sem.at[1]),
    ]
    for fetch in fetches:
        fetch.start()

    def wo_slice(ref, holder):
        high = wo_ref.shape[0] // lax.axis_size("dp")
        broad = wo_ref.shape[1] // sections
        top = pl.multiple_of(lax.rem(holder, lax.axis_size("dp")) * high, high)
        left = pl.multiple_of(holder // lax.axis_size("dp") * broad, broad)
        return ref.at[pl.ds(top, high), pl.ds(left, broad)]

    def wo_line(step):
        return remote(
            wo_slice(wo_ref, group),
            wo_slice(wo_all.at[me], group),
            wo_send.at[step - 1],
            wo_recv.at[step - 1],
            {"mp": lax.rem(me + step, line)},
        )

    def wo_hop(step, quarter, at, sem, device):
        block = wo_slice(wo_all.at[lax.rem(me - step + line, line)], group_of(quarter, core))
        return remote(block, block, wo_out.at[step - 1, at], sem, device)

    def wo_starts(step):
        return (
            wo_hop(step, 0, 0, wo_plane.at[step - 1, 1], over_y),
            wo_hop(step, 0, 1, wo_plane.at[step - 1, 2], over_x),
            wo_hop(step, 0, 2, wo_pair.at[step - 1, 0], pair),
        )

    def wo_forward_x(step):
        return wo_hop(step, 1, 3, wo_plane.at[step - 1, 3], over_x)

    def wo_forward_pair(step, quarter):
        return wo_hop(step, quarter, 3 + quarter, wo_pair.at[step - 1, quarter], pair)

    def wo_landed(step, quarter):
        return wo_hop(step, quarter, 0, wo_plane.at[step - 1, quarter], over_x)

    def wo_paired(step, quarter):
        block = wo_slice(wo_all.at[lax.rem(me - step + line, line)], group_of(quarter, 1 - core))
        return remote(block, block, wo_out.at[step - 1, 0], wo_pair.at[step - 1, quarter], pair)

    steps = range(1, line)
    for step in steps:
        wo_line(step).start()

    place_copies = []
    for step in range(1, groups):
        peer = lax.rem(group + step, groups)
        copy = remote(
            place_ref.at[peer], spots.at[step], spot_send.at[step - 1], spot_recv.at[step - 1], group_device(peer)
        )
        copy.start()
        place_copies.append(copy)
    sum_copies = []
    for step in range(1, line):
        peer = lax.rem(me + step, line)
        copy = remote(sums_ref, sums.at[step], sum_send.at[step - 1], sum_recv.at[step - 1], {"mp": peer})
        copy.start()
        sum_copies.append(copy)
    spots[0] = place_ref[group]
    sums[0] = sums_ref[...]

    tall = min(patches_ref.shape[0], 128)

    @pl.loop(0, patches_ref.shape[0] // tall)
    def _(at):
        cut = pl.ds(at * tall, tall)
        normed = layer_norm(patches_ref[cut], attn_gain_ref[...]).astype(jnp.bfloat16)
        for which, ref in enumerate((query, key, value_part)):
            ref[cut] = lax.dot_general(
                normed, qkv_ref[which], (((1,), (1,)), ((), ())), preferred_element_type=jnp.float32
            ).astype(ref.dtype)

    for step in steps:
        wo_line(step).wait_recv()
        for copy in wo_starts(step):
            copy.start()
    wo_all[me] = wo_ref[...]

    tiles = counts_ref.shape[0]
    block = query.shape[0] // tiles
    lane = lax.broadcasted_iota(jnp.int32, (1, query.shape[1]), 1)
    at_key = lax.broadcasted_iota(jnp.int32, (block, block), 1)

    def attend(tile):
        cut = pl.ds(tile * block, block)
        tile_query, tile_key, tile_value = query[cut], key[cut], value_part[cut]
        live = at_key < counts_ref[tile]
        result = jnp.zeros((block, query.shape[1]), jnp.float32)
        for head in range(query.shape[1] // HEAD_DIM):
            own = jnp.logical_and(lane >= head * HEAD_DIM, lane < (head + 1) * HEAD_DIM)
            own = own.astype(jnp.float32).astype(jnp.bfloat16)
            scores = lax.dot_general(
                tile_query * own, tile_key, (((1,), (1,)), ((), ())), preferred_element_type=jnp.float32
            )
            scores = jnp.where(live, scores * HEAD_DIM**-0.5, -1e30)
            power = jnp.exp(scores - jnp.max(scores, axis=1, keepdims=True))
            weights = (power / jnp.sum(power, axis=1, keepdims=True)).astype(jnp.bfloat16)
            result = result + jnp.dot(weights, tile_value * own, preferred_element_type=jnp.float32)
        attended[cut] = result.astype(attended.dtype)

    for tile in range(tiles):
        attend(tile)
        for step in steps:
            if tile == 0:
                wo_landed(step, 1).wait_recv()
                wo_forward_x(step).start()
                wo_forward_pair(step, 1).start()
            elif tile == 1:
                wo_landed(step, 2).wait_recv()
                wo_forward_pair(step, 2).start()

    place_of = lax.broadcasted_iota(jnp.int32, (attended.shape[0], attended.shape[0]), 0)
    order = (key_ref[...] == place_of).astype(jnp.float32).astype(jnp.bfloat16)
    ordered[...] = (
        jnp.dot(order, attended[...], preferred_element_type=jnp.float32)
        .astype(ordered.dtype)
        .reshape(ordered.shape)
    )

    def exchange(step):
        peer = lax.rem(me + step, line)
        return remote(ordered.at[peer], arrived.at[me], a_send.at[step - 1], a_recv.at[step - 1], {"mp": peer})

    for step in steps:
        exchange(step).start()
    arrived[me] = ordered[me]
    slots = ordered.shape[1]
    own_place = me * slots + lax.broadcasted_iota(jnp.int32, (slots, attended.shape[0]), 0)
    own_order = (key_ref[...] == own_place).astype(jnp.float32).astype(jnp.bfloat16)
    block_out = jnp.dot(own_order, patches_ref[...], preferred_element_type=jnp.float32)
    for step in steps:
        wo_landed(step, 3).wait_recv()
        wo_forward_pair(step, 3).start()
    for step in steps:
        for quarter in range(quarters):
            wo_paired(step, quarter).wait_recv()
    for step in steps:
        exchange(step).wait_recv()
    for source in range(line):
        block_out = block_out + jnp.dot(
            arrived[source], wo_all[source], preferred_element_type=jnp.float32
        )
    block_out = block_out.astype(jnp.bfloat16)
    x_ref[...] = (
        layer_norm(block_out, merge_gain_ref[...]).astype(x_ref.dtype).reshape(x_ref.shape)
    )
    for copy in own_sends(0):
        copy.start()
    rows[group] = x_ref[...]
    for fetch in fetches:
        fetch.wait()

    def send_right(piece):
        return remote(
            right_out.at[piece], before.at[piece], right_send.at[piece], right_recv.at[piece], {"mp": me + 1}
        )

    def send_left(piece):
        return remote(
            left_out.at[piece], after.at[piece], left_send.at[piece], left_recv.at[piece], {"mp": me - 1}
        )

    def send_give(chunk):
        return remote(give.at[chunk], take.at[chunk], give_send.at[chunk], give_recv.at[chunk], pair)

    parts = x_send.shape[1]
    span = keep.shape[1] // parts

    def send_x(chunk, at):
        cut = pl.ds(at * span, span)
        return remote(
            x_out.at[chunk, cut], x_in.at[chunk, cut], x_send.at[chunk, at], x_recv.at[chunk, at], over_x
        )

    def send_y(at):
        cut = pl.ds(at * span, span)
        return remote(y_out.at[cut], y_in.at[cut], y_send.at[at], y_recv.at[at], over_y)

    def settle(chunk):
        send_give(chunk).wait_recv()
        mine = lax.rem(chunk, wide) == column

        @pl.when(mine)
        def _():
            @pl.loop(0, parts)
            def _(at):
                cut = pl.ds(at * span, span)
                keep[chunk, cut] = keep[chunk, cut] + take[chunk, cut].astype(jnp.float32)

        @pl.when(jnp.logical_not(mine))
        def _():
            @pl.loop(0, parts)
            def _(at):
                cut = pl.ds(at * span, span)
                x_out[chunk, cut] = (
                    keep[chunk, cut] + take[chunk, cut].astype(jnp.float32)
                ).astype(x_out.dtype)
                send_x(chunk, at).start()

    def stage(i, carry):
        @pl.when(i < pieces)
        def _():
            chunk = i // quarters
            quarter = lax.rem(i, quarters)

            @pl.when(quarter == 1)
            def _():
                remote(
                    x_ref.at[chunk], rows.at[group_of(1, core), chunk], row_send.at[chunk, 0], row_recv.at[chunk, 1], over_y
                ).wait_recv()
                forward_x(chunk).start()
                forward_pair(chunk, 1).start()

                @pl.when(chunk + 1 < chips)
                def _():
                    for copy in own_sends(chunk + 1):
                        copy.start()

            @pl.when(quarter > 1)
            def _():
                remote(
                    x_ref.at[chunk], rows.at[group_of(quarter, core), chunk], row_send.at[chunk, 1], row_recv.at[chunk, quarter], over_x
                ).wait_recv()
                forward_pair(chunk, quarter).start()

        at_dot = i - 1

        @pl.when(jnp.logical_and(at_dot >= 0, at_dot < pieces))
        def _():
            chunk = at_dot // quarters
            quarter = lax.rem(at_dot, quarters)
            spot = rows.at[group_of(quarter, 1 - core), chunk]
            remote(x_ref.at[chunk], spot, row_send.at[chunk, 2], pair_recv.at[chunk, quarter], pair).wait_recv()
            lhs = rows[pl.ds(chip_of(quarter) * 2, 2), chunk]
            part[at_dot] = jnp.dot(
                lhs.reshape(part.shape[1], lhs.shape[2]), w1_ref[...], preferred_element_type=jnp.float32
            )

        at_right = i - 1 - lag_right

        @pl.when(jnp.logical_and(me < line - 1, jnp.logical_and(at_right >= 0, at_right < pieces)))
        def _():
            @pl.when(me == 0)
            def _():
                right_out[at_right] = part[at_right].astype(right_out.dtype)

            @pl.when(me > 0)
            def _():
                send_right(at_right).wait_recv()
                right_out[at_right] = (
                    part[at_right] + before[at_right].astype(jnp.float32)
                ).astype(right_out.dtype)

            send_right(at_right).start()

        at_left = i - 1 - lag_left

        @pl.when(jnp.logical_and(me > 0, jnp.logical_and(at_left >= 0, at_left < pieces)))
        def _():
            @pl.when(me == line - 1)
            def _():
                left_out[at_left] = part[at_left].astype(left_out.dtype)

            @pl.when(me < line - 1)
            def _():
                send_left(at_left).wait_recv()
                left_out[at_left] = (
                    part[at_left] + after[at_left].astype(jnp.float32)
                ).astype(left_out.dtype)

            send_left(at_left).start()

        at_total = i - 1 - lag_total

        @pl.when(at_total >= 0)
        def _():
            chunk = at_total // quarters
            quarter = lax.rem(at_total, quarters)

            @pl.when(jnp.logical_and(quarter == 0, chunk > 0))
            def _():
                settle(chunk - 1)

            @pl.when(me == line - 1)
            def _():
                send_right(at_total).wait_recv()

            @pl.when(me == 0)
            def _():
                send_left(at_total).wait_recv()

            @pl.when(me > 0)
            def _():
                part[at_total] = part[at_total] + before[at_total].astype(jnp.float32)

            @pl.when(me < line - 1)
            def _():
                part[at_total] = part[at_total] + after[at_total].astype(jnp.float32)

            value = part[at_total] + b1_ref[...]
            value = 0.5 * value * (1.0 + lax.erf(value * HALF_ROOT))
            hidden[chunk, chip_of(quarter)] = value.astype(hidden.dtype).reshape(hidden.shape[2:])

            @pl.when(quarter == quarters - 1)
            def _():
                for_pair = hidden[chunk, :, :, 1 - core].reshape(-1, hidden.shape[5])
                for_me = hidden[chunk, :, :, core].reshape(-1, hidden.shape[5])
                count = for_me.shape[0]
                lhs = jnp.concatenate([for_pair, for_me], axis=0)

                @pl.loop(0, w2_ref.shape[1] // FC2_COLS)
                def _(at):
                    cols = pl.ds(pl.multiple_of(at * FC2_COLS, FC2_COLS), FC2_COLS)
                    result = jnp.dot(lhs, w2_ref[:, cols], preferred_element_type=jnp.float32)
                    give[chunk, :, cols] = result[:count].astype(give.dtype)
                    keep[chunk, :, cols] = result[count:]

                send_give(chunk).start()

        return carry

    lax.fori_loop(0, pieces + 1 + lag_total, stage, 0)
    settle(chips - 1)

    for copy in sum_copies:
        copy.wait_recv()
    sum_rows = base_out.shape[0]
    both = sums[0]
    for step in range(1, line):
        both = both + sums[step]
    base_out[...] = both[sum_rows:]
    base_ref[...] = both[:sum_rows]
    send_base = remote(base_out, base_in, base_send, base_recv, {"section": section + 1})

    @pl.when(section < sections - 1)
    def _():
        send_base.start()

    spot_sum = spots[0]
    for copy in place_copies:
        copy.wait_recv()
    for step in range(1, groups):
        spot_sum = spot_sum + spots[step]
    spot_ref[...] = spot_sum

    @pl.when(section > 0)
    def _():
        send_base.wait_recv()
        base_ref[...] = base_in[...]

    own_chunk = section * wide + column
    y_chunk = flip(section, 1) * wide + column

    @pl.loop(0, parts)
    def _(at):
        cut = pl.ds(at * span, span)
        send_x(y_chunk, at).wait_recv()
        y_out[cut] = (keep[y_chunk, cut] + x_in[y_chunk, cut].astype(jnp.float32)).astype(y_out.dtype)
        send_y(at).start()

    @pl.loop(0, parts)
    def _(at):
        cut = pl.ds(at * span, span)
        send_x(own_chunk, at).wait_recv()
        send_y(at).wait_recv()
        value = (
            keep[own_chunk, cut]
            + x_in[own_chunk, cut].astype(jnp.float32)
            + y_in[cut].astype(jnp.float32)
            + b2_ref[...]
        ).astype(img_ref.dtype)
        img_ref[cut] = value
        value = value.astype(jnp.float32)
        square = value * value
        width = squares.shape[1]
        folded = square[:, :width]
        for at_col in range(1, square.shape[1] // width):
            folded = folded + square[:, at_col * width : (at_col + 1) * width]
        squares[cut] = folded

    totals[0] = jnp.sum(squares[...].T, axis=0, keepdims=True)
    total_copies = []
    for step in range(1, line):
        copy = remote(
            totals.at[0], totals.at[step], total_send.at[step - 1], total_recv.at[step - 1], {"mp": lax.rem(me + step, line)}
        )
        copy.start()
        total_copies.append(copy)

    for step in steps:
        wo_line(step).wait_send()
        for copy in wo_starts(step) + (wo_forward_x(step),):
            copy.wait_send()
        for quarter in range(1, quarters):
            wo_forward_pair(step, quarter).wait_send()
        exchange(step).wait_send()

    for chunk in range(chips):
        for copy in own_sends(chunk):
            copy.wait_send()
        forward_x(chunk).wait_send()
        for quarter in range(1, quarters):
            forward_pair(chunk, quarter).wait_send()
        send_give(chunk).wait_send()

        @pl.when(chunk % wide != column)
        def _():
            for at in range(parts):
                send_x(chunk, at).wait_send()

    for at in range(parts):
        send_y(at).wait_send()

    @pl.when(me < line - 1)
    def _():
        @pl.loop(0, pieces)
        def _(piece):
            send_right(piece).wait_send()

    @pl.when(me > 0)
    def _():
        @pl.loop(0, pieces)
        def _(piece):
            send_left(piece).wait_send()

    for copy in place_copies + sum_copies:
        copy.wait_send()

    @pl.when(section < sections - 1)
    def _():
        send_base.wait_send()

    row_total = totals[0]
    for step, copy in enumerate(total_copies):
        copy.wait()
        row_total = row_total + totals[step + 1]
    total_ref[...] = row_total


def merger(patches, counts, keys, qkv, wo, attn_gain, merge_gain, places, sums, w1, b1, w2, b2):
    groups = lax.axis_size("section") * lax.axis_size("dp")
    line = lax.axis_size("mp")
    chips = groups // 2
    patch_rows, width = patches.shape
    slot_rows = patch_rows // 4
    chunk_rows = slot_rows // chips
    run = chunk_rows // 2
    local_cols = qkv.shape[1]
    units = w1.shape[1]
    features = w2.shape[1]
    pieces = chips * 4
    piece_rows = 2 * chunk_rows
    target_rows = groups * run
    parts = 4
    low = jnp.bfloat16
    dma = pltpu.SemaphoreType.DMA
    sum_rows = sums.shape[0] // 2
    return pl.pallas_call(
        merger_kernel,
        out_shape=(
            jax.ShapeDtypeStruct((target_rows, features), low),
            jax.ShapeDtypeStruct(places.shape[1:], jnp.int32),
            jax.ShapeDtypeStruct((sum_rows, sums.shape[1]), jnp.float32),
            jax.ShapeDtypeStruct((1, target_rows), jnp.float32),
        ),
        in_specs=[
            pl.BlockSpec(memory_space={1: pltpu.SMEM, 9: pl.ANY, 11: pl.ANY}.get(at, pltpu.VMEM))
            for at in range(13)
        ],
        out_specs=[pl.BlockSpec(memory_space=pltpu.VMEM)] * 4,
        scratch_shapes=[
            pltpu.VMEM((patch_rows, local_cols), low),
            pltpu.VMEM((patch_rows, local_cols), low),
            pltpu.VMEM((patch_rows, local_cols), low),
            pltpu.VMEM((patch_rows, local_cols), low),
            pltpu.VMEM((4, slot_rows, local_cols), low),
            pltpu.VMEM((line, slot_rows, local_cols), low),
            pltpu.VMEM((line,) + wo.shape, low),
            pltpu.VMEM((chips, chunk_rows, width), low),
            pltpu.VMEM(w1.shape, low),
            pltpu.VMEM(w2.shape, low),
            dma((2,)),
            dma((line - 1,)),
            dma((line - 1,)),
            dma((line - 1, 7)),
            dma((line - 1, 4)),
            dma((line - 1, 4)),
            dma((line - 1,)),
            dma((line - 1,)),
            pltpu.VMEM((groups, chips, chunk_rows, width), low),
            pltpu.VMEM((pieces, piece_rows, units), jnp.float32),
            pltpu.VMEM((pieces, piece_rows, units), low),
            pltpu.VMEM((pieces, piece_rows, units), low),
            pltpu.VMEM((pieces, piece_rows, units), low),
            pltpu.VMEM((pieces, piece_rows, units), low),
            pltpu.VMEM((chips, chips, 2, 2, run, units), low),
            pltpu.VMEM((chips, target_rows, features), low),
            pltpu.VMEM((chips, target_rows, features), low),
            pltpu.VMEM((chips, target_rows, features), jnp.float32),
            pltpu.VMEM((chips, target_rows, features), low),
            pltpu.VMEM((chips, target_rows, features), low),
            pltpu.VMEM((target_rows, features), low),
            pltpu.VMEM((target_rows, features), low),
            pltpu.VMEM((target_rows, 128), jnp.float32),
            pltpu.VMEM(places.shape, jnp.int32),
            pltpu.VMEM((line,) + sums.shape, jnp.float32),
            pltpu.VMEM((sum_rows, sums.shape[1]), jnp.float32),
            pltpu.VMEM((sum_rows, sums.shape[1]), jnp.float32),
            pltpu.VMEM((line, 1, target_rows), jnp.float32),
            dma((chips, 7)),
            dma((chips, 4)),
            dma((chips, 4)),
            dma((pieces,)),
            dma((pieces,)),
            dma((pieces,)),
            dma((pieces,)),
            dma((chips,)),
            dma((chips,)),
            dma((chips, parts)),
            dma((chips, parts)),
            dma((parts,)),
            dma((parts,)),
            dma((groups - 1,)),
            dma((groups - 1,)),
            dma((line - 1,)),
            dma((line - 1,)),
            dma,
            dma,
            dma((line - 1,)),
            dma((line - 1,)),
        ],
        cost_estimate=pl.CostEstimate(
            flops=10**11, bytes_accessed=10**7, transcendentals=0
        ),
        compiler_params=pltpu.CompilerParams(
            collective_id=6, has_side_effects=True, vmem_limit_bytes=VMEM_LIMIT
        ),
    )(patches, counts, keys, qkv, wo, attn_gain, merge_gain, places, sums, w1, b1, w2, b2)


def placing_kernel(text_ref, incoming_ref, img_ref, spot_ref, total_ref, base_ref, gain_ref, seq_ref, layer_ref):
    height = text_ref.shape[0]
    at_row = pl.program_id(0) * height + lax.broadcasted_iota(jnp.int32, (height, spot_ref.shape[1]), 0)
    hits = spot_ref[...] == at_row
    hit = jnp.max(hits.astype(jnp.float32), axis=1, keepdims=True) > 0.0
    placed = jnp.dot(
        hits.astype(jnp.bfloat16), img_ref[...], preferred_element_type=jnp.float32
    ).astype(jnp.bfloat16)
    sequence = jnp.where(hit, placed, text_ref[...])
    seq_ref[...] = sequence
    gain = gain_ref[...].astype(jnp.float32)
    base = base_ref[...]

    @pl.when(lax.axis_index("section") == 0)
    def _():
        total = jnp.sum(jnp.where(hits, total_ref[...], 0.0), axis=1, keepdims=True)
        total = jnp.where(hit, total, base)
        scale = lax.rsqrt(total / HID + llm_eps)
        layer_ref[...] = (sequence.astype(jnp.float32) * scale * gain).astype(layer_ref.dtype)

    @pl.when(lax.axis_index("section") > 0)
    def _():
        scale = lax.rsqrt(base / HID + llm_eps)
        layer_ref[...] = (incoming_ref[...].astype(jnp.float32) * scale * gain).astype(layer_ref.dtype)


def placing(text, incoming, img, spot, total, base, gain):
    rows, features = text.shape
    height = rows // 8
    block = pl.BlockSpec((height, features), lambda i: (i, 0))

    def whole(value):
        return pl.BlockSpec(value.shape, lambda i: (0, 0))

    return pl.pallas_call(
        placing_kernel,
        grid=(rows // height,),
        out_shape=(jax.ShapeDtypeStruct(text.shape, text.dtype),) * 2,
        in_specs=[
            block,
            block,
            whole(img),
            whole(spot),
            whole(total),
            pl.BlockSpec((height, 1), lambda i: (i, 0)),
            whole(gain),
        ],
        out_specs=(block, block),
        cost_estimate=pl.CostEstimate(flops=10**9, bytes_accessed=10**7, transcendentals=0),
    )(text, incoming, img, spot, total, base, gain)


def per_device(*operands):
    (patches, patch_counts, dest_rows, qkv_weight, out_weight, attn_gain, merge_gain) = operands[:7]
    (fc1_weight, fc1_bias, fc2_weight, fc2_bias, text_embeds, section_hidden, llm_gain) = operands[7:]
    outer, _ = group_bits()
    group_count = lax.axis_size("section") * lax.axis_size("dp")
    merged_rows = patches.shape[0] // 4
    run_cap = merged_rows // group_count
    seq_rows = text_embeds.shape[0]
    held = group_count * merged_rows * patches.shape[1] * patches.dtype.itemsize
    if lax.axis_size("mp") != 4 or outer != [("dp", 2), ("section", 1)] or held > KERNEL_BYTES or run_cap % 16 or merged_rows % 128 or seq_rows % 128:
        return plain_per_device(*operands)
    tile_total = patch_counts.shape[0]
    block_rows = patches.shape[0] // tile_total
    run_total = group_count
    incoming = from_behind(section_hidden, "section", 1)
    runs = dest_rows.reshape(run_total, run_cap)
    run_target = runs[:, 0] // seq_rows
    takes = jnp.arange(group_count, dtype=jnp.int32)[:, None] == run_target[None, :]
    tile_slots = block_rows // 4
    live = (
        jnp.arange(tile_slots, dtype=jnp.int32)[None, :] * 4 < patch_counts[:, None]
    ).reshape(run_total, run_cap)
    place = jnp.where(live, runs % seq_rows - seq_rows, 0)
    send_place = jnp.sum(jnp.where(takes[:, :, None], place[None], 0), axis=1) + seq_rows
    my_group = lax.axis_index("section") * lax.axis_size("dp") + lax.axis_index("dp")
    at_lane = jnp.arange(merged_rows, dtype=jnp.int32)
    places = jnp.where(
        (at_lane // run_cap == my_group)[None, :], jnp.tile(send_place, (1, group_count)), 0
    )[:, None, :]

    def square_sums(value):
        value = value.astype(jnp.float32)
        return jnp.sum(value * value, axis=1).reshape(-1, 128)

    sums = jnp.concatenate([square_sums(text_embeds), square_sums(section_hidden)], axis=0)

    slot_key = (
        run_target[:, None] * run_cap + jnp.arange(run_cap, dtype=jnp.int32)[None, :]
    ).reshape(-1)
    keys = (slot_key[:, None] + jnp.arange(4, dtype=jnp.int32)[None, :] * merged_rows).reshape(1, -1)
    img, spot, base, total = merger(
        patches,
        patch_counts,
        keys,
        qkv_weight.transpose(1, 2, 0),
        out_weight,
        attn_gain[None, :],
        merge_gain[None, :],
        places,
        sums,
        fc1_weight,
        fc1_bias.astype(jnp.float32)[None, :],
        fc2_weight,
        fc2_bias.astype(jnp.float32)[None, :],
    )
    return placing(
        text_embeds, incoming, img, spot, total, base.reshape(-1, 1), llm_gain[None, :]
    )


def solution(mesh):
    in_specs = (
        P(("section", "dp"), None),
        P(("section", "dp")),
        P(("section", "dp")),
        P(None, None, "mp"),
        P("mp", None),
        P(),
        P(),
        P("mp", ("section", "dp")),
        P(("section", "dp")),
        P(("section", "dp"), "mp"),
        P("mp"),
        P(("section", "dp"), "mp"),
        P(("section", "dp"), "mp"),
        P("mp"),
    )
    out_specs = (P(("section", "dp"), "mp"), P(("section", "dp"), "mp"))
    return jax.shard_map(
        per_device, mesh=mesh, in_specs=in_specs, out_specs=out_specs, check_vma=False
    )
```

```python
import functools
import math

import jax
import jax.numpy as jnp
from jax import lax
from jax.experimental import pallas as pl
from jax.experimental.pallas import tpu as pltpu
from jax.sharding import PartitionSpec as P

HEAD_DIM = 80
HID = 8192


vit_eps = 1e-06
llm_eps = 1e-06


def from_behind(value, axis, steps):
    count = lax.axis_size(axis)
    first, last = (max(0, -steps), min(count, count - steps))
    return lax.ppermute(value, axis, [(source, source + steps) for source in range(first, last)])


def layer_norm(values, gain):
    centred = values.astype(jnp.float32)
    centred = centred - jnp.mean(centred, axis=-1, keepdims=True)
    variance = jnp.mean(centred * centred, axis=-1, keepdims=True)
    return centred * lax.rsqrt(variance + vit_eps) * gain.astype(jnp.float32)


VMEM_LIMIT = 60 * 1024 * 1024
KERNEL_BYTES = 8 * 1024 * 1024


def vmem_call(kernel, out, scratch, sent_bytes, ident, *operands):
    return pl.pallas_call(
        kernel,
        out_shape=out,
        in_specs=[pl.BlockSpec(memory_space=pltpu.VMEM)] * len(operands),
        out_specs=pl.BlockSpec(memory_space=pltpu.VMEM),
        scratch_shapes=scratch,
        cost_estimate=pl.CostEstimate(
            flops=sent_bytes * 20000, bytes_accessed=sent_bytes * 2, transcendentals=0
        ),
        compiler_params=pltpu.CompilerParams(
            collective_id=ident, has_side_effects=True, vmem_limit_bytes=VMEM_LIMIT
        ),
    )(*operands)


def exchange_kernel(count, spread, x_ref, o_ref, send_sem, recv_sem, own_sem):
    me = lax.axis_index("mp")
    barrier = pltpu.get_barrier_semaphore()
    for step in range(1, count):
        peer = lax.rem(me + step, count)
        pl.semaphore_signal(
            barrier, inc=1, device_id={"mp": peer}, device_id_type=pl.DeviceIdType.MESH
        )
    pl.semaphore_wait(barrier, count - 1)
    copies = []
    for step in sorted(range(1, count), key=lambda s: -min(s, count - s)):
        peer = lax.rem(me + step, count)
        copy = pltpu.make_async_remote_copy(
            src_ref=x_ref.at[peer] if spread else x_ref,
            dst_ref=o_ref.at[me],
            send_sem=send_sem.at[step - 1],
            recv_sem=recv_sem.at[step - 1],
            device_id={"mp": peer},
            device_id_type=pl.DeviceIdType.MESH,
        )
        copy.start()
        copies.append(copy)
    own = pltpu.make_async_copy(x_ref.at[me] if spread else x_ref, o_ref.at[me], own_sem)
    own.start()
    own.wait()
    for copy in copies:
        copy.wait()


def relay_kernel(count, x_ref, o_ref, send_sem, recv_sem, own_sem):
    me = lax.axis_index("mp")
    barrier = pltpu.get_barrier_semaphore()
    for step in range(1, count):
        peer = lax.rem(me + step, count)
        pl.semaphore_signal(
            barrier, inc=1, device_id={"mp": peer}, device_id_type=pl.DeviceIdType.MESH
        )
    pl.semaphore_wait(barrier, count - 1)
    own = pltpu.make_async_copy(x_ref, o_ref.at[me], own_sem)
    own.start()

    def hop(way, step):
        owner = lax.rem(me - way * step + count, count)
        return pltpu.make_async_remote_copy(
            src_ref=o_ref.at[owner] if step else x_ref,
            dst_ref=o_ref.at[owner],
            send_sem=send_sem.at[(way + 1) // 2, step],
            recv_sem=recv_sem.at[(way + 1) // 2, step],
            device_id={"mp": lax.rem(me + way + count, count)},
            device_id_type=pl.DeviceIdType.MESH,
        )

    def holds(way, step):
        return me >= step if way > 0 else me + step < count

    def sends(way):
        return me < count - 1 if way > 0 else me > 0

    for step in range(count):
        for way in (1, -1):
            if step:

                @pl.when(holds(way, step))
                def _():
                    owner = lax.rem(me - way * step + count, count)
                    pltpu.make_async_remote_copy(
                        src_ref=x_ref,
                        dst_ref=o_ref.at[owner],
                        send_sem=send_sem.at[(way + 1) // 2, step - 1],
                        recv_sem=recv_sem.at[(way + 1) // 2, step - 1],
                        device_id={"mp": lax.rem(me - way + count, count)},
                        device_id_type=pl.DeviceIdType.MESH,
                    ).wait_recv()

            if step < count - 1:

                @pl.when(jnp.logical_and(holds(way, step), sends(way)))
                def _():
                    hop(way, step).start()

    own.wait()
    for step in range(count - 1):
        for way in (1, -1):

            @pl.when(jnp.logical_and(holds(way, step), sends(way)))
            def _():
                hop(way, step).wait_send()


def relay_mp(value, ident):
    count = lax.axis_size("mp")
    return vmem_call(
        functools.partial(relay_kernel, count),
        jax.ShapeDtypeStruct((count,) + value.shape, value.dtype),
        [
            pltpu.SemaphoreType.DMA((2, count - 1)),
            pltpu.SemaphoreType.DMA((2, count - 1)),
            pltpu.SemaphoreType.DMA,
        ],
        count * value.size * value.dtype.itemsize,
        ident,
        value,
    )


def exchange_mp(value, spread, ident):
    count = lax.axis_size("mp")
    shape = value.shape if spread else (count,) + value.shape
    size = math.prod(shape) * value.dtype.itemsize
    return vmem_call(
        functools.partial(exchange_kernel, count, spread),
        jax.ShapeDtypeStruct(shape, value.dtype),
        [
            pltpu.SemaphoreType.DMA((count - 1,)),
            pltpu.SemaphoreType.DMA((count - 1,)),
            pltpu.SemaphoreType.DMA,
        ],
        size,
        ident,
        value,
    )


def sum_scatter_mp(blocks, ident):
    return jnp.sum(exchange_mp(blocks, True, ident).astype(jnp.float32), axis=0)


def gather_mp(value):
    got = relay_mp(value, 2)
    return got.reshape((-1,) + value.shape[1:])


def total_mp(value):
    return jnp.sum(exchange_mp(value.reshape(-1, 128), False, 3), axis=0).reshape(-1)


def flip(index, bit):
    return index + bit * (1 - 2 * (index // bit % 2))


def group_bits():
    outer = [("dp", 1 << k) for k in range(1, lax.axis_size("dp").bit_length() - 1)]
    outer += [("section", 1 << k) for k in range(lax.axis_size("section").bit_length() - 1)]
    return outer, ("dp", 1)


def meets(axis, bit):
    return {axis: flip(lax.axis_index(axis), bit)}


def group_at(mask):
    spots = {axis: lax.axis_index(axis) for axis in ("section", "dp")}
    for axis, bit in mask:
        spots[axis] = flip(spots[axis], bit)
    return spots["section"] * lax.axis_size("dp") + spots["dp"]


def greet(bits):
    barrier = pltpu.get_barrier_semaphore()
    for axis, bit in bits:
        pl.semaphore_signal(
            barrier, inc=1, device_id=meets(axis, bit), device_id_type=pl.DeviceIdType.MESH
        )
    pl.semaphore_wait(barrier, len(bits))


def gather_kernel(x_ref, o_ref, send_sem, recv_sem, own_sem):
    outer, last = group_bits()
    greet(outer + [last])
    half = x_ref.shape[1] // 2
    sent, waiting = [], []
    slots = iter(range(send_sem.shape[0]))

    def pass_on(mask, stage, part, order):
        cols = pl.ds(part * half, half)
        spot = group_at(mask)
        source = o_ref.at[spot, :, cols] if mask else x_ref.at[:, cols]
        for later in range(stage, len(order)):
            slot = next(slots)
            copy = pltpu.make_async_remote_copy(
                src_ref=source,
                dst_ref=o_ref.at[spot, :, cols],
                send_sem=send_sem.at[slot],
                recv_sem=recv_sem.at[slot],
                device_id=meets(*order[later]),
                device_id_type=pl.DeviceIdType.MESH,
            )
            copy.start()
            sent.append(copy)
            waiting.append((later, copy, mask + [order[later]], part, order))

    pass_on([], 0, 0, outer + [last])
    pass_on([], 0, 1, outer[::-1] + [last])
    own = pltpu.make_async_copy(x_ref, o_ref.at[group_at([])], own_sem)
    own.start()
    while waiting:
        first = min(range(len(waiting)), key=lambda at: waiting[at][0])
        stage, copy, mask, part, order = waiting.pop(first)
        copy.wait_recv()
        pass_on(mask, stage + 1, part, order)
    for copy in sent:
        copy.wait_send()
    own.wait()


def gather_groups(value):
    count = lax.axis_size("section") * lax.axis_size("dp")
    size = count * value.size * value.dtype.itemsize
    if size > KERNEL_BYTES:
        return lax.all_gather(value, ("section", "dp"), axis=0, tiled=True)
    slots = 2 * (count - 1)
    got = vmem_call(
        gather_kernel,
        jax.ShapeDtypeStruct((count,) + value.shape, value.dtype),
        [
            pltpu.SemaphoreType.DMA((slots,)),
            pltpu.SemaphoreType.DMA((slots,)),
            pltpu.SemaphoreType.DMA,
        ],
        size,
        4,
        value,
    )
    return got.reshape(-1, value.shape[1])


def scatter_kernel(x_ref, o_ref, held, taken, send_sem, recv_sem):
    outer, first = group_bits()
    greet(outer + [first])
    rows = x_ref.shape[1]
    half = x_ref.shape[2] // 2
    chunk = 32
    orders = ([first] + outer, [first] + outer[::-1])
    slots = iter(range(send_sem.shape[0]))
    masks = [[]]
    for bit in outer:
        masks = masks + [mask + [bit] for mask in masks]
    place_of = {frozenset(mask): at for at, mask in enumerate(masks)}
    base = len(masks)
    live = {}

    def send(part, stage):
        cols = pl.ds(part * half, half)
        bit = orders[part][stage]
        kept = orders[part][stage + 1 :]
        copies = []
        for mask in [m for m in masks if set(m) <= set(kept)]:
            if stage == 0:
                source = x_ref.at[group_at(mask + [bit]), :, cols]
            else:
                source = held.at[place_of[frozenset(mask + [bit])], :, cols]
            landing = 2 * base - 2 ** (len(kept) + 1) + [
                m for m in masks if set(m) <= set(kept)
            ].index(mask)
            slot = next(slots)
            copy = pltpu.make_async_remote_copy(
                src_ref=source,
                dst_ref=taken.at[landing, :, cols],
                send_sem=send_sem.at[slot],
                recv_sem=recv_sem.at[slot],
                device_id=meets(*bit),
                device_id_type=pl.DeviceIdType.MESH,
            )
            copy.start()
            copies.append((copy, mask, landing))
        live[part, stage] = copies

    def add(part, stage):
        cols = pl.ds(part * half, half)
        final = stage + 1 == len(orders[part])
        following = None if final else orders[part][stage + 1]
        copies = live[part, stage]
        for copy, mask, landing in sorted(copies, key=lambda c: following not in c[1]):
            copy.wait_recv()
            at = place_of[frozenset(mask)]
            spot = group_at(mask)

            @pl.loop(0, rows // chunk)
            def _(step):
                span = pl.ds(step * chunk, chunk)
                mine = x_ref[spot, span, cols] if stage == 0 else held[at, span, cols]
                total = mine.astype(jnp.float32) + taken[landing, span, cols].astype(jnp.float32)
                if final:
                    o_ref[span, cols] = total
                else:
                    held[at, span, cols] = total.astype(held.dtype)

    send(0, 0)
    send(1, 0)
    for stage in range(len(orders[0])):
        for part in (0, 1):
            add(part, stage)
            if stage + 1 < len(orders[0]):
                send(part, stage + 1)
    for copies in live.values():
        for copy, _, _ in copies:
            copy.wait_send()


def sum_scatter_groups(value):
    count = lax.axis_size("section") * lax.axis_size("dp")
    size = value.size * value.dtype.itemsize
    if size > KERNEL_BYTES:
        return lax.psum_scatter(value, ("section", "dp"), scatter_dimension=0, tiled=True)
    rows, cols = value.shape[0] // count, value.shape[1]
    slots = 2 * (count - 1)
    return vmem_call(
        scatter_kernel,
        jax.ShapeDtypeStruct((rows, cols), jnp.float32),
        [
            pltpu.VMEM((count // 2, rows, cols), value.dtype),
            pltpu.VMEM((count - 1, rows, cols), value.dtype),
            pltpu.SemaphoreType.DMA((slots,)),
            pltpu.SemaphoreType.DMA((slots,)),
        ],
        size,
        5,
        value.reshape(count, rows, cols),
    )


def plain_per_device(
    patches,
    patch_counts,
    dest_rows,
    qkv_weight,
    out_weight,
    attn_gain,
    merge_gain,
    fc1_weight,
    fc1_bias,
    fc2_weight,
    fc2_bias,
    text_embeds,
    section_hidden,
    llm_gain,
):
    width = patches.shape[1]
    tile_total = patch_counts.shape[0]
    block_rows = patches.shape[0] // tile_total
    merged_rows = patches.shape[0] // 4
    local_cols = qkv_weight.shape[2]
    local_heads = local_cols // HEAD_DIM
    feature_cols = text_embeds.shape[1]
    seq_rows = text_embeds.shape[0]
    section_count = lax.axis_size("section")
    group_count = section_count * lax.axis_size("dp")
    run_cap = max(2, merged_rows // group_count)
    run_total = merged_rows // run_cap
    run_target = dest_rows.reshape(run_total, run_cap)[:, 0] // seq_rows
    takes = jnp.arange(group_count, dtype=jnp.int32)[:, None] == run_target[None, :]
    slot_in_tile = jnp.arange(merged_rows, dtype=jnp.int32) % (block_rows // 4)
    tile_counts = jnp.repeat(patch_counts, block_rows // 4, total_repeat_length=merged_rows)
    live = slot_in_tile * 4 < tile_counts
    place = jnp.where(live, dest_rows % seq_rows - seq_rows, 0).reshape(run_total, run_cap)
    send_place = jnp.sum(jnp.where(takes[:, :, None], place[None], 0), axis=1) + seq_rows
    got_place = lax.all_to_all(send_place, ("section", "dp"), split_axis=0, concat_axis=0, tiled=True)
    incoming = from_behind(section_hidden, "section", 1)
    normed_in = layer_norm(patches, attn_gain).astype(jnp.bfloat16)
    projections = jnp.dot(
        normed_in, qkv_weight.reshape(width, 3 * local_cols), preferred_element_type=jnp.float32
    ).astype(jnp.bfloat16)
    projections = projections.reshape(tile_total, block_rows, 3, local_heads, HEAD_DIM)
    query_part = projections[:, :, 0]
    key_part = projections[:, :, 1]
    value_part = projections[:, :, 2]
    scores = jnp.einsum(
        "tqhd,tkhd->thqk", query_part, key_part, preferred_element_type=jnp.float32
    ) * HEAD_DIM ** (-0.5)
    key_live = (
        jnp.arange(block_rows, dtype=jnp.int32)[None, None, None, :]
        < patch_counts[:, None, None, None]
    )
    scores = jnp.where(key_live, scores, -1e30)
    weights = jax.nn.softmax(scores, axis=-1).astype(jnp.bfloat16)
    attended = jnp.einsum(
        "thqk,tkhd->tqhd", weights, value_part, preferred_element_type=jnp.float32
    ).astype(jnp.bfloat16)
    attended = attended.reshape(patches.shape[0], local_cols)
    lane_source = jnp.arange(run_total, dtype=jnp.int32)[None, :] * run_cap
    run_source = jnp.sum(jnp.where(takes, lane_source, 0), axis=1)
    row_source = (
        run_source[:, None] + jnp.arange(run_cap, dtype=jnp.int32)[None, :]
    ).reshape(-1) * 4
    slots_at = jnp.arange(patches.shape[0], dtype=jnp.int32)
    patch_at = jnp.arange(4, dtype=jnp.int32)
    order = (
        (row_source[None, :] + patch_at[:, None]).reshape(-1)[:, None] == slots_at[None, :]
    ).astype(jnp.bfloat16)
    own_order = (
        (row_source + lax.axis_index("mp"))[:, None] == slots_at[None, :]
    ).astype(jnp.bfloat16)
    ordered = jnp.dot(order, attended, preferred_element_type=jnp.float32).astype(jnp.bfloat16)
    own_patch = jnp.dot(own_order, patches, preferred_element_type=jnp.float32)
    partial_proj = jnp.dot(ordered, out_weight, preferred_element_type=jnp.float32)
    own_proj = sum_scatter_mp(
        partial_proj.astype(jnp.bfloat16).reshape(4, group_count * run_cap, width), 0
    )
    block_out = (own_patch + own_proj).astype(jnp.bfloat16)
    merge_part = layer_norm(block_out, merge_gain).astype(jnp.bfloat16)
    slot_rows = group_count * run_cap
    gathered = gather_groups(merge_part)
    gathered = (
        gathered.reshape(group_count, group_count, run_cap, width)
        .transpose(1, 0, 2, 3)
        .reshape(group_count * slot_rows, width)
    )
    first_partial = jnp.dot(gathered, fc1_weight, preferred_element_type=jnp.float32)
    mp_count = lax.axis_size("mp")
    first_total = sum_scatter_mp(
        first_partial.astype(jnp.bfloat16).reshape(mp_count, -1, fc1_weight.shape[1]),
        1,
    )
    hidden_part = jax.nn.gelu(
        first_total + fc1_bias.astype(jnp.float32), approximate=False
    ).astype(jnp.bfloat16)
    hidden = gather_mp(hidden_part)
    second_partial = jnp.dot(hidden, fc2_weight, preferred_element_type=jnp.float32)
    embed_total = sum_scatter_groups(second_partial.astype(jnp.bfloat16)).astype(jnp.float32)
    image_embeds = (embed_total + fc2_bias.astype(jnp.float32)).astype(jnp.bfloat16)
    hits = got_place.reshape(1, -1) == jnp.arange(seq_rows, dtype=jnp.int32)[:, None]
    placed = jnp.dot(
        hits.astype(jnp.bfloat16), image_embeds, preferred_element_type=jnp.float32
    ).astype(jnp.bfloat16)
    sequence_embeds = jnp.where(jnp.any(hits, axis=1)[:, None], placed, text_embeds)
    entering = jnp.where(lax.axis_index("section") == 0, sequence_embeds, incoming).astype(
        jnp.float32
    )
    row_total = total_mp(jnp.sum(entering * entering, axis=1))
    layer_inputs = (
        entering * lax.rsqrt(row_total / HID + llm_eps)[:, None] * llm_gain.astype(jnp.float32)
    ).astype(jnp.bfloat16)
    return (sequence_embeds, layer_inputs)


LAG = 3
FC2_COLS = 512
HALF_ROOT = 0.5**0.5


def remote(src, dst, send_sem, recv_sem, device):
    return pltpu.make_async_remote_copy(
        src_ref=src,
        dst_ref=dst,
        send_sem=send_sem,
        recv_sem=recv_sem,
        device_id=device,
        device_id_type=pl.DeviceIdType.MESH,
    )


def group_device(group):
    per_section = lax.axis_size("dp")
    return {"section": group // per_section, "dp": lax.rem(group, per_section)}


def tell(device):
    pl.semaphore_signal(
        pltpu.get_barrier_semaphore(),
        inc=1,
        device_id=device,
        device_id_type=pl.DeviceIdType.MESH,
    )


def merger_kernel(
    patches_ref,
    counts_ref,
    dest_ref,
    qkv_ref,
    wo_ref,
    attn_gain_ref,
    merge_gain_ref,
    w1_hbm,
    b1_ref,
    w2_hbm,
    b2_ref,
    text_hbm,
    carry_hbm,
    img_ref,
    spot_ref,
    base_ref,
    total_ref,
    incoming_hbm,
    text_ref,
    carry_ref,
    text_squares,
    carry_squares,
    carry_sem,
    carry_send,
    carry_recv,
    normed,
    place_ref,
    sums_ref,
    query,
    key,
    value_part,
    attended,
    ordered,
    arrived,
    wo_all,
    x_ref,
    w1_ref,
    w2_ref,
    weight_sem,
    wo_send,
    wo_recv,
    wo_out,
    wo_plane,
    wo_pair,
    a_send,
    a_recv,
    rows,
    part,
    before,
    after,
    right_out,
    left_out,
    hidden,
    give,
    take,
    keep,
    x_out,
    x_in,
    y_out,
    y_in,
    squares,
    spots,
    sums,
    base_out,
    base_in,
    totals,
    row_send,
    row_recv,
    pair_recv,
    right_send,
    right_recv,
    left_send,
    left_recv,
    give_send,
    give_recv,
    x_send,
    x_recv,
    y_send,
    y_recv,
    spot_send,
    spot_recv,
    sum_send,
    sum_recv,
    base_send,
    base_recv,
    total_send,
    total_recv,
):
    groups = lax.axis_size("section") * lax.axis_size("dp")
    sections = lax.axis_size("section")
    line = lax.axis_size("mp")
    me = lax.axis_index("mp")
    section = lax.axis_index("section")
    dp = lax.axis_index("dp")
    core = lax.rem(dp, 2)
    column = dp // 2
    wide = lax.axis_size("dp") // 2
    group = section * lax.axis_size("dp") + dp
    chips = groups // 2
    pair = {"dp": flip(dp, 1)}
    over_x = {"dp": flip(dp, 2)}
    over_y = {"section": flip(section, 1)}
    quarters = 4
    pieces = chips * quarters
    take_rows = rows.shape[2] // 2
    lag_right = me * LAG
    lag_left = (line - 1 - me) * LAG
    lag_total = (line - 1) * LAG

    for step in range(1, groups):
        tell(group_device(lax.rem(group + step, groups)))
    for step in range(1, line):
        tell({"mp": lax.rem(me + step, line)})
    pl.semaphore_wait(pltpu.get_barrier_semaphore(), groups + line - 2)

    def chip_of(quarter):
        there_x = lax.rem(quarter // 2 + column, 2)
        there_y = lax.rem(lax.rem(quarter, 2) + section, 2)
        return there_y * wide + there_x

    def group_of(quarter, at_core):
        return chip_of(quarter) * 2 + at_core

    def own_sends(chunk):
        return (
            remote(x_ref.at[chunk], rows.at[group, chunk], row_send.at[chunk, 0], row_recv.at[chunk, 1], over_y),
            remote(x_ref.at[chunk], rows.at[group, chunk], row_send.at[chunk, 1], row_recv.at[chunk, 2], over_x),
            remote(x_ref.at[chunk], rows.at[group, chunk], row_send.at[chunk, 2], pair_recv.at[chunk, 0], pair),
        )

    def forward_x(chunk):
        spot = rows.at[group_of(1, core), chunk]
        return remote(spot, spot, row_send.at[chunk, 3], row_recv.at[chunk, 3], over_x)

    def forward_pair(chunk, quarter):
        spot = rows.at[group_of(quarter, core), chunk]
        return remote(
            spot, spot, row_send.at[chunk, 3 + quarter], pair_recv.at[chunk, quarter], pair
        )

    fetches = [
        pltpu.make_async_copy(w1_hbm, w1_ref, weight_sem.at[0]),
        pltpu.make_async_copy(w2_hbm, w2_ref, weight_sem.at[1]),
    ]
    for fetch in fetches:
        fetch.start()
    leads = section < sections - 1
    bands = carry_send.shape[0]
    band_rows = carry_hbm.shape[0] // bands
    text_fetch = pltpu.make_async_copy(text_hbm, text_ref, carry_sem.at[0])
    carry_fetch = pltpu.make_async_copy(carry_hbm, carry_ref, carry_sem.at[1])

    @pl.when(leads)
    def _():
        text_fetch.start()
        carry_fetch.start()

    def send_band(at):
        cut = pl.ds(pl.multiple_of(at * band_rows, band_rows), band_rows)
        return remote(
            carry_hbm.at[cut], incoming_hbm.at[cut], carry_send.at[at], carry_recv.at[at], {"section": section + 1}
        )

    def send_bands(first, last):
        @pl.when(leads)
        def _():
            for at in range(first, last):
                send_band(at).start()

    early = bands // 8

    def wo_slice(ref, holder):
        high = wo_ref.shape[0] // lax.axis_size("dp")
        broad = wo_ref.shape[1] // sections
        top = pl.multiple_of(lax.rem(holder, lax.axis_size("dp")) * high, high)
        left = pl.multiple_of(holder // lax.axis_size("dp") * broad, broad)
        return ref.at[pl.ds(top, high), pl.ds(left, broad)]

    def wo_line(step):
        return remote(
            wo_slice(wo_ref, group),
            wo_slice(wo_all.at[me], group),
            wo_send.at[step - 1],
            wo_recv.at[step - 1],
            {"mp": lax.rem(me + step, line)},
        )

    def wo_hop(step, quarter, at, sem, device):
        block = wo_slice(wo_all.at[lax.rem(me - step + line, line)], group_of(quarter, core))
        return remote(block, block, wo_out.at[step - 1, at], sem, device)

    def wo_starts(step):
        return (
            wo_hop(step, 0, 0, wo_plane.at[step - 1, 1], over_y),
            wo_hop(step, 0, 1, wo_plane.at[step - 1, 2], over_x),
            wo_hop(step, 0, 2, wo_pair.at[step - 1, 0], pair),
        )

    def wo_forward_x(step):
        return wo_hop(step, 1, 3, wo_plane.at[step - 1, 3], over_x)

    def wo_forward_pair(step, quarter):
        return wo_hop(step, quarter, 3 + quarter, wo_pair.at[step - 1, quarter], pair)

    def wo_landed(step, quarter):
        return wo_hop(step, quarter, 0, wo_plane.at[step - 1, quarter], over_x)

    def wo_paired(step, quarter):
        block = wo_slice(wo_all.at[lax.rem(me - step + line, line)], group_of(quarter, 1 - core))
        return remote(block, block, wo_out.at[step - 1, 0], wo_pair.at[step - 1, quarter], pair)

    steps = range(1, line)
    for step in steps:
        wo_line(step).start()

    send_bands(0, early)
    slots = ordered.shape[1]
    run = slots // groups
    dest = dest_ref[...].reshape(1, slots)
    slot = lax.broadcasted_iota(jnp.int32, (1, slots), 1)
    tiles = counts_ref.shape[0]
    slice_rows = carry_hbm.shape[0]
    target = dest // slice_rows
    slot_place = slot
    for stride in [1 << bit for bit in range(run.bit_length() - 1, slots.bit_length())][::-1]:
        slot_place = jnp.where(slot_place >= stride, slot_place - stride, slot_place)
    slot_target = target * run + slot_place
    filled = jnp.zeros((1, slots), jnp.int32)
    for tile in range(tiles):
        start = tile * (slots // tiles)
        within = jnp.logical_and(slot >= start, slot - start < slots // tiles)
        filled = jnp.where(jnp.logical_and(within, (slot - start) * 4 < counts_ref[tile]), 1, filled)
    spot = jnp.where(filled > 0, dest - target * slice_rows, slice_rows)
    high = (spot // 16).astype(jnp.float32)
    low = (spot - spot // 16 * 16).astype(jnp.float32)
    to_group = lax.broadcasted_iota(jnp.int32, (groups, slots), 0) == target
    at_source = lax.broadcasted_iota(jnp.int32, (slots, slots), 1)
    moved = (at_source == group * run + slot_place.reshape(slots, 1)).astype(jnp.float32).astype(jnp.bfloat16)

    def moved_to(value):
        picked = jnp.where(to_group, value, 0.0).astype(jnp.bfloat16)
        return jnp.dot(picked, moved, preferred_element_type=jnp.float32)

    place_rows = (moved_to(high) * 16.0 + moved_to(low)).astype(jnp.int32)
    place_ref[...] = place_rows.reshape(place_ref.shape)
    place_copies = []
    for step in range(1, groups):
        peer = lax.rem(group + step, groups)
        copy = remote(
            place_ref.at[peer], spots.at[step], spot_send.at[step - 1], spot_recv.at[step - 1], group_device(peer)
        )
        copy.start()
        place_copies.append(copy)
    spots[0] = place_ref[group]

    tall = min(patches_ref.shape[0], 128)

    @pl.loop(0, patches_ref.shape[0] // tall)
    def _(at):
        cut = pl.ds(at * tall, tall)
        normed[cut] = layer_norm(
            patches_ref[cut], attn_gain_ref[...].reshape(1, -1)
        ).astype(normed.dtype)

    for which, ref in enumerate((query, key, value_part)):
        ref[...] = lax.dot_general(
            normed[...], qkv_ref[which], (((1,), (1,)), ((), ())), preferred_element_type=jnp.float32
        ).astype(ref.dtype)

    for step in steps:
        wo_line(step).wait_recv()
        for copy in wo_starts(step):
            copy.start()
    send_bands(early, 2 * early)
    wo_all[me] = wo_ref[...]

    block = query.shape[0] // tiles
    lane = lax.broadcasted_iota(jnp.int32, (1, query.shape[1]), 1)
    at_key = lax.broadcasted_iota(jnp.int32, (block, block), 1)

    def attend(tile):
        cut = pl.ds(tile * block, block)
        tile_query, tile_key, tile_value = query[cut], key[cut], value_part[cut]
        live = at_key < counts_ref[tile]
        result = jnp.zeros((block, query.shape[1]), jnp.float32)
        for head in range(query.shape[1] // HEAD_DIM):
            own = jnp.logical_and(lane >= head * HEAD_DIM, lane < (head + 1) * HEAD_DIM)
            own = own.astype(jnp.float32).astype(jnp.bfloat16)
            scores = lax.dot_general(
                tile_query * own, tile_key, (((1,), (1,)), ((), ())), preferred_element_type=jnp.float32
            )
            scores = jnp.where(live, scores * HEAD_DIM**-0.5, -1e30)
            power = jnp.exp(scores - jnp.max(scores, axis=1, keepdims=True))
            weights = (power / jnp.sum(power, axis=1, keepdims=True)).astype(jnp.bfloat16)
            result = result + jnp.dot(weights, tile_value * own, preferred_element_type=jnp.float32)
        attended[cut] = result.astype(attended.dtype)

    for tile in range(tiles):
        attend(tile)
        for step in steps:
            if tile == 0:
                wo_landed(step, 1).wait_recv()
                wo_forward_x(step).start()
                wo_forward_pair(step, 1).start()
            elif tile == 1:
                wo_landed(step, 2).wait_recv()
                wo_forward_pair(step, 2).start()
        if tile < 2:
            send_bands((2 + tile) * early, (3 + tile) * early)

    whole = attended.shape[0]
    at_row = lax.broadcasted_iota(jnp.int32, (slots, whole), 0)
    at_patch = lax.broadcasted_iota(jnp.int32, (slots, whole), 1)
    order = (
        lax.broadcasted_iota(jnp.int32, (slots, slots), 0) == slot_target
    ).astype(jnp.float32).astype(jnp.bfloat16)

    def picked(patch, source):
        pick = (at_patch == at_row * line + patch).astype(jnp.float32).astype(jnp.bfloat16)
        rows_of = jnp.dot(pick, source, preferred_element_type=jnp.float32).astype(jnp.bfloat16)
        return jnp.dot(order, rows_of, preferred_element_type=jnp.float32)

    for patch in range(line):
        ordered[patch] = picked(patch, attended[...]).astype(ordered.dtype)

    def exchange(step):
        peer = lax.rem(me + step, line)
        return remote(ordered.at[peer], arrived.at[me], a_send.at[step - 1], a_recv.at[step - 1], {"mp": peer})

    for step in steps:
        exchange(step).start()
    arrived[me] = ordered[me]
    block_out = picked(me, patches_ref[...])
    for step in steps:
        wo_landed(step, 3).wait_recv()
        wo_forward_pair(step, 3).start()
    for step in steps:
        for quarter in range(quarters):
            wo_paired(step, quarter).wait_recv()
    for step in steps:
        exchange(step).wait_recv()
    for source in range(line):
        block_out = block_out + jnp.dot(
            arrived[source], wo_all[source], preferred_element_type=jnp.float32
        )
    block_out = block_out.astype(jnp.bfloat16)
    x_ref[...] = (
        layer_norm(block_out, merge_gain_ref[...].reshape(1, -1)).astype(x_ref.dtype).reshape(x_ref.shape)
    )
    for copy in own_sends(0):
        copy.start()
    rows[group] = x_ref[...]
    for fetch in fetches:
        fetch.wait()

    def send_right(piece):
        return remote(
            right_out.at[piece], before.at[piece], right_send.at[piece], right_recv.at[piece], {"mp": me + 1}
        )

    def send_left(piece):
        return remote(
            left_out.at[piece], after.at[piece], left_send.at[piece], left_recv.at[piece], {"mp": me - 1}
        )

    def send_give(chunk):
        return remote(give.at[chunk], take.at[chunk], give_send.at[chunk], give_recv.at[chunk], pair)

    parts = x_send.shape[1]
    span = keep.shape[1] // parts

    def send_x(chunk, at):
        cut = pl.ds(at * span, span)
        return remote(
            x_out.at[chunk, cut], x_in.at[chunk, cut], x_send.at[chunk, at], x_recv.at[chunk, at], over_x
        )

    def send_y(at):
        cut = pl.ds(at * span, span)
        return remote(y_out.at[cut], y_in.at[cut], y_send.at[at], y_recv.at[at], over_y)

    def settle(chunk):
        send_give(chunk).wait_recv()
        mine = lax.rem(chunk, wide) == column

        @pl.when(mine)
        def _():
            @pl.loop(0, parts)
            def _(at):
                cut = pl.ds(at * span, span)
                keep[chunk, cut] = keep[chunk, cut] + take[chunk, cut].astype(jnp.float32)

        @pl.when(jnp.logical_not(mine))
        def _():
            @pl.loop(0, parts)
            def _(at):
                cut = pl.ds(at * span, span)
                x_out[chunk, cut] = (
                    keep[chunk, cut] + take[chunk, cut].astype(jnp.float32)
                ).astype(x_out.dtype)
                send_x(chunk, at).start()

    sum_rows = base_out.shape[0]

    def folded(value):
        value = value.astype(jnp.float32)
        square = value * value
        width = squares.shape[1]
        total = square[:, :width]
        for at_col in range(1, square.shape[1] // width):
            total = total + square[:, at_col * width : (at_col + 1) * width]
        return total

    def exchange_sums(step):
        return remote(
            sums_ref, sums.at[step], sum_send.at[step - 1], sum_recv.at[step - 1], {"mp": lax.rem(me + step, line)}
        )

    send_base = remote(base_out, base_in, base_send, base_recv, {"section": section + 1})
    share = text_ref.shape[0] // pieces

    def stage(i, carry):
        @pl.when(jnp.logical_and(leads, i < pieces))
        def _():
            @pl.loop(0, (bands - 4 * early) // pieces)
            def _(at):
                send_band(4 * early + i * ((bands - 4 * early) // pieces) + at).start()

            @pl.when(i == 0)
            def _():
                text_fetch.wait()
                carry_fetch.wait()

            cut = pl.ds(pl.multiple_of(i * share, share), share)
            text_squares[cut] = folded(text_ref[cut])
            carry_squares[cut] = folded(carry_ref[cut])

        @pl.when(jnp.logical_and(leads, i == pieces))
        def _():
            for which, ref in enumerate((text_squares, carry_squares)):
                for at in range(sum_rows):
                    cut = pl.ds(at * 128, 128)
                    at_sum = which * sum_rows + at
                    sums_ref[at_sum : at_sum + 1] = jnp.sum(ref[cut].T, axis=0, keepdims=True)
            for step in steps:
                exchange_sums(step).start()

        @pl.when(jnp.logical_and(leads, i == pieces + 4))
        def _():
            both = sums_ref[...]
            for step in steps:
                exchange_sums(step).wait()
                both = both + sums[step]
            base_out[...] = both[sum_rows:]
            base_ref[...] = both[:sum_rows]
            send_base.start()

        @pl.when(i < pieces)
        def _():
            chunk = i // quarters
            quarter = lax.rem(i, quarters)

            @pl.when(quarter == 1)
            def _():
                remote(
                    x_ref.at[chunk], rows.at[group_of(1, core), chunk], row_send.at[chunk, 0], row_recv.at[chunk, 1], over_y
                ).wait_recv()
                forward_x(chunk).start()
                forward_pair(chunk, 1).start()

                @pl.when(chunk + 1 < chips)
                def _():
                    for copy in own_sends(chunk + 1):
                        copy.start()

            @pl.when(quarter > 1)
            def _():
                remote(
                    x_ref.at[chunk], rows.at[group_of(quarter, core), chunk], row_send.at[chunk, 1], row_recv.at[chunk, quarter], over_x
                ).wait_recv()
                forward_pair(chunk, quarter).start()

        at_dot = i - 1

        @pl.when(jnp.logical_and(at_dot >= 0, at_dot < pieces))
        def _():
            chunk = at_dot // quarters
            quarter = lax.rem(at_dot, quarters)
            spot = rows.at[group_of(quarter, 1 - core), chunk]
            remote(x_ref.at[chunk], spot, row_send.at[chunk, 2], pair_recv.at[chunk, quarter], pair).wait_recv()
            lhs = rows[pl.ds(chip_of(quarter) * 2, 2), chunk]
            part[at_dot] = jnp.dot(
                lhs.reshape(part.shape[1], lhs.shape[2]), w1_ref[...], preferred_element_type=jnp.float32
            )

        at_right = i - 1 - lag_right

        @pl.when(jnp.logical_and(me < line - 1, jnp.logical_and(at_right >= 0, at_right < pieces)))
        def _():
            @pl.when(me == 0)
            def _():
                right_out[at_right] = part[at_right].astype(right_out.dtype)

            @pl.when(me > 0)
            def _():
                send_right(at_right).wait_recv()
                right_out[at_right] = (
                    part[at_right] + before[at_right].astype(jnp.float32)
                ).astype(right_out.dtype)

            send_right(at_right).start()

        at_left = i - 1 - lag_left

        @pl.when(jnp.logical_and(me > 0, jnp.logical_and(at_left >= 0, at_left < pieces)))
        def _():
            @pl.when(me == line - 1)
            def _():
                left_out[at_left] = part[at_left].astype(left_out.dtype)

            @pl.when(me < line - 1)
            def _():
                send_left(at_left).wait_recv()
                left_out[at_left] = (
                    part[at_left] + after[at_left].astype(jnp.float32)
                ).astype(left_out.dtype)

            send_left(at_left).start()

        at_total = i - 1 - lag_total

        @pl.when(at_total >= 0)
        def _():
            chunk = at_total // quarters
            quarter = lax.rem(at_total, quarters)

            @pl.when(jnp.logical_and(quarter == 0, chunk > 0))
            def _():
                settle(chunk - 1)

            @pl.when(me == line - 1)
            def _():
                send_right(at_total).wait_recv()

            @pl.when(me == 0)
            def _():
                send_left(at_total).wait_recv()

            @pl.when(me > 0)
            def _():
                part[at_total] = part[at_total] + before[at_total].astype(jnp.float32)

            @pl.when(me < line - 1)
            def _():
                part[at_total] = part[at_total] + after[at_total].astype(jnp.float32)

            value = part[at_total] + b1_ref[...].reshape(1, -1).astype(jnp.float32)
            value = 0.5 * value * (1.0 + lax.erf(value * HALF_ROOT))
            hidden[chunk, chip_of(quarter)] = value.astype(hidden.dtype).reshape(hidden.shape[2:])

            @pl.when(quarter == quarters - 1)
            def _():
                for_pair = hidden[chunk, :, :, 1 - core].reshape(-1, hidden.shape[5])
                for_me = hidden[chunk, :, :, core].reshape(-1, hidden.shape[5])
                count = for_me.shape[0]
                lhs = jnp.concatenate([for_pair, for_me], axis=0)

                @pl.loop(0, w2_ref.shape[1] // FC2_COLS)
                def _(at):
                    cols = pl.ds(pl.multiple_of(at * FC2_COLS, FC2_COLS), FC2_COLS)
                    result = jnp.dot(lhs, w2_ref[:, cols], preferred_element_type=jnp.float32)
                    give[chunk, :, cols] = result[:count].astype(give.dtype)
                    keep[chunk, :, cols] = result[count:]

                send_give(chunk).start()

        return carry

    lax.fori_loop(0, pieces + 1 + lag_total, stage, 0)
    settle(chips - 1)

    spot_sum = spots[0]
    for copy in place_copies:
        copy.wait_recv()
    for step in range(1, groups):
        spot_sum = spot_sum + spots[step]
    spot_ref[...] = spot_sum

    @pl.when(section > 0)
    def _():
        send_base.wait_recv()
        base_ref[...] = base_in[...]

        @pl.loop(0, bands)
        def _(at):
            remote(
                carry_hbm.at[pl.ds(0, band_rows)], incoming_hbm.at[pl.ds(0, band_rows)], carry_send.at[at], carry_recv.at[at], over_y
            ).wait_recv()

    own_chunk = section * wide + column
    y_chunk = flip(section, 1) * wide + column

    @pl.loop(0, parts)
    def _(at):
        cut = pl.ds(at * span, span)
        send_x(y_chunk, at).wait_recv()
        y_out[cut] = (keep[y_chunk, cut] + x_in[y_chunk, cut].astype(jnp.float32)).astype(y_out.dtype)
        send_y(at).start()

    @pl.loop(0, parts)
    def _(at):
        cut = pl.ds(at * span, span)
        send_x(own_chunk, at).wait_recv()
        send_y(at).wait_recv()
        value = (
            keep[own_chunk, cut]
            + x_in[own_chunk, cut].astype(jnp.float32)
            + y_in[cut].astype(jnp.float32)
            + b2_ref[...].reshape(1, -1).astype(jnp.float32)
        ).astype(img_ref.dtype)
        img_ref[cut] = value
        squares[cut] = folded(value)

    totals[0] = jnp.sum(squares[...].T, axis=0, keepdims=True)
    total_copies = []
    for step in range(1, line):
        copy = remote(
            totals.at[0], totals.at[step], total_send.at[step - 1], total_recv.at[step - 1], {"mp": lax.rem(me + step, line)}
        )
        copy.start()
        total_copies.append(copy)

    for step in steps:
        wo_line(step).wait_send()
        for copy in wo_starts(step) + (wo_forward_x(step),):
            copy.wait_send()
        for quarter in range(1, quarters):
            wo_forward_pair(step, quarter).wait_send()
        exchange(step).wait_send()

    for chunk in range(chips):
        for copy in own_sends(chunk):
            copy.wait_send()
        forward_x(chunk).wait_send()
        for quarter in range(1, quarters):
            forward_pair(chunk, quarter).wait_send()
        send_give(chunk).wait_send()

        @pl.when(chunk % wide != column)
        def _():
            for at in range(parts):
                send_x(chunk, at).wait_send()

    for at in range(parts):
        send_y(at).wait_send()

    @pl.when(me < line - 1)
    def _():
        @pl.loop(0, pieces)
        def _(piece):
            send_right(piece).wait_send()

    @pl.when(me > 0)
    def _():
        @pl.loop(0, pieces)
        def _(piece):
            send_left(piece).wait_send()

    for copy in place_copies:
        copy.wait_send()

    @pl.when(leads)
    def _():
        send_base.wait_send()

        @pl.loop(0, bands)
        def _(at):
            send_band(at).wait_send()

    row_total = totals[0]
    for step, copy in enumerate(total_copies):
        copy.wait()
        row_total = row_total + totals[step + 1]
    total_ref[...] = row_total


def merger(patches, counts, dest, qkv, wo, attn_gain, merge_gain, w1, b1, w2, b2, text, carry):
    groups = lax.axis_size("section") * lax.axis_size("dp")
    line = lax.axis_size("mp")
    chips = groups // 2
    patch_rows, width = patches.shape
    slot_rows = patch_rows // 4
    chunk_rows = slot_rows // chips
    run = chunk_rows // 2
    local_cols = qkv.shape[1]
    units = w1.shape[1]
    features = w2.shape[1]
    pieces = chips * 4
    piece_rows = 2 * chunk_rows
    target_rows = groups * run
    parts = 4
    low = jnp.bfloat16
    dma = pltpu.SemaphoreType.DMA
    sum_rows = text.shape[0] // 128
    bands = text.shape[0] // 16
    return pl.pallas_call(
        merger_kernel,
        out_shape=(
            jax.ShapeDtypeStruct((target_rows, features), low),
            jax.ShapeDtypeStruct((1, slot_rows), jnp.int32),
            jax.ShapeDtypeStruct((sum_rows, 128), jnp.float32),
            jax.ShapeDtypeStruct((1, target_rows), jnp.float32),
            jax.ShapeDtypeStruct(carry.shape, carry.dtype),
        ),
        in_specs=[
            pl.BlockSpec(memory_space={1: pltpu.SMEM, 7: pl.ANY, 9: pl.ANY, 11: pl.ANY, 12: pl.ANY}.get(at, pltpu.VMEM))
            for at in range(13)
        ],
        out_specs=[pl.BlockSpec(memory_space=pltpu.VMEM)] * 4 + [pl.BlockSpec(memory_space=pl.ANY)],
        scratch_shapes=[
            pltpu.VMEM(text.shape, low),
            pltpu.VMEM(text.shape, low),
            pltpu.VMEM((text.shape[0], 128), jnp.float32),
            pltpu.VMEM((text.shape[0], 128), jnp.float32),
            dma((2,)),
            dma((bands,)),
            dma((bands,)),
            pltpu.VMEM(patches.shape, low),
            pltpu.VMEM((groups, 1, slot_rows), jnp.int32),
            pltpu.VMEM((2 * sum_rows, 128), jnp.float32),
            pltpu.VMEM((patch_rows, local_cols), low),
            pltpu.VMEM((patch_rows, local_cols), low),
            pltpu.VMEM((patch_rows, local_cols), low),
            pltpu.VMEM((patch_rows, local_cols), low),
            pltpu.VMEM((4, slot_rows, local_cols), low),
            pltpu.VMEM((line, slot_rows, local_cols), low),
            pltpu.VMEM((line,) + wo.shape, low),
            pltpu.VMEM((chips, chunk_rows, width), low),
            pltpu.VMEM(w1.shape, low),
            pltpu.VMEM(w2.shape, low),
            dma((2,)),
            dma((line - 1,)),
            dma((line - 1,)),
            dma((line - 1, 7)),
            dma((line - 1, 4)),
            dma((line - 1, 4)),
            dma((line - 1,)),
            dma((line - 1,)),
            pltpu.VMEM((groups, chips, chunk_rows, width), low),
            pltpu.VMEM((pieces, piece_rows, units), jnp.float32),
            pltpu.VMEM((pieces, piece_rows, units), low),
            pltpu.VMEM((pieces, piece_rows, units), low),
            pltpu.VMEM((pieces, piece_rows, units), low),
            pltpu.VMEM((pieces, piece_rows, units), low),
            pltpu.VMEM((chips, chips, 2, 2, run, units), low),
            pltpu.VMEM((chips, target_rows, features), low),
            pltpu.VMEM((chips, target_rows, features), low),
            pltpu.VMEM((chips, target_rows, features), jnp.float32),
            pltpu.VMEM((chips, target_rows, features), low),
            pltpu.VMEM((chips, target_rows, features), low),
            pltpu.VMEM((target_rows, features), low),
            pltpu.VMEM((target_rows, features), low),
            pltpu.VMEM((target_rows, 128), jnp.float32),
            pltpu.VMEM((groups, 1, slot_rows), jnp.int32),
            pltpu.VMEM((line, 2 * sum_rows, 128), jnp.float32),
            pltpu.VMEM((sum_rows, 128), jnp.float32),
            pltpu.VMEM((sum_rows, 128), jnp.float32),
            pltpu.VMEM((line, 1, target_rows), jnp.float32),
            dma((chips, 7)),
            dma((chips, 4)),
            dma((chips, 4)),
            dma((pieces,)),
            dma((pieces,)),
            dma((pieces,)),
            dma((pieces,)),
            dma((chips,)),
            dma((chips,)),
            dma((chips, parts)),
            dma((chips, parts)),
            dma((parts,)),
            dma((parts,)),
            dma((groups - 1,)),
            dma((groups - 1,)),
            dma((line - 1,)),
            dma((line - 1,)),
            dma,
            dma,
            dma((line - 1,)),
            dma((line - 1,)),
        ],
        cost_estimate=pl.CostEstimate(
            flops=10**11, bytes_accessed=10**7, transcendentals=0
        ),
        compiler_params=pltpu.CompilerParams(
            collective_id=6, has_side_effects=True, vmem_limit_bytes=VMEM_LIMIT
        ),
    )(patches, counts, dest, qkv, wo, attn_gain, merge_gain, w1, b1, w2, b2, text, carry)


def placing_kernel(
    text_hbm,
    incoming_hbm,
    img_ref,
    spot_ref,
    total_ref,
    base_ref,
    gain_ref,
    seq_hbm,
    layer_hbm,
    text,
    incoming,
    seq,
    layer,
    load_sem,
    store_sem,
):
    cuts = base_ref.shape[0]
    height = text.shape[0] // cuts
    first = lax.axis_index("section") == 0
    gain = gain_ref[...].reshape(1, -1).astype(jnp.float32)

    def move(which, at):
        cut = pl.ds(at * height, height)
        source, target, sem = (
            (text_hbm, text, load_sem.at[0, at]),
            (incoming_hbm, incoming, load_sem.at[1, at]),
            (seq, seq_hbm, store_sem.at[0, at]),
            (layer, layer_hbm, store_sem.at[1, at]),
        )[which]
        return pltpu.make_async_copy(source.at[cut], target.at[cut], sem)

    for at in range(cuts):
        move(0, at).start()

        @pl.when(jnp.logical_not(first))
        def _():
            move(1, at).start()

    width = base_ref.shape[1]
    diagonal = lax.broadcasted_iota(jnp.int32, (height, width), 0) == lax.broadcasted_iota(
        jnp.int32, (height, width), 1
    )
    for at in range(cuts):
        cut = pl.ds(at * height, height)
        at_row = at * height + lax.broadcasted_iota(jnp.int32, (height, spot_ref.shape[1]), 0)
        hits = spot_ref[...] == at_row
        hit = jnp.max(hits.astype(jnp.float32), axis=1, keepdims=True) > 0.0
        placed = jnp.dot(
            hits.astype(jnp.float32).astype(jnp.bfloat16), img_ref[...], preferred_element_type=jnp.float32
        ).astype(jnp.bfloat16)
        base = jnp.sum(jnp.where(diagonal, base_ref[at : at + 1], 0.0), axis=1, keepdims=True)
        move(0, at).wait()
        seq[cut] = jnp.where(hit, placed, text[cut])
        move(2, at).start()

        @pl.when(first)
        def _():
            total = jnp.sum(jnp.where(hits, total_ref[...], 0.0), axis=1, keepdims=True)
            total = jnp.where(hit, total, base)
            scale = lax.rsqrt(total / HID + llm_eps)
            layer[cut] = (seq[cut].astype(jnp.float32) * scale * gain).astype(layer.dtype)

        @pl.when(jnp.logical_not(first))
        def _():
            move(1, at).wait()
            scale = lax.rsqrt(base / HID + llm_eps)
            layer[cut] = (incoming[cut].astype(jnp.float32) * scale * gain).astype(layer.dtype)

        move(3, at).start()

    for at in range(cuts):
        move(2, at).wait()
        move(3, at).wait()


def placing(text, incoming, img, spot, total, base, gain):
    cuts = base.shape[0]
    return pl.pallas_call(
        placing_kernel,
        out_shape=(jax.ShapeDtypeStruct(text.shape, text.dtype),) * 2,
        in_specs=[pl.BlockSpec(memory_space=pl.ANY)] * 2 + [pl.BlockSpec(memory_space=pltpu.VMEM)] * 5,
        out_specs=[pl.BlockSpec(memory_space=pl.ANY)] * 2,
        scratch_shapes=[pltpu.VMEM(text.shape, text.dtype)] * 4
        + [pltpu.SemaphoreType.DMA((2, cuts)), pltpu.SemaphoreType.DMA((2, cuts))],
        cost_estimate=pl.CostEstimate(flops=10**9, bytes_accessed=10**7, transcendentals=0),
        compiler_params=pltpu.CompilerParams(vmem_limit_bytes=VMEM_LIMIT),
    )(text, incoming, img, spot, total, base, gain)


def per_device(*operands):
    (patches, patch_counts, dest_rows, qkv_weight, out_weight, attn_gain, merge_gain) = operands[:7]
    (fc1_weight, fc1_bias, fc2_weight, fc2_bias, text_embeds, section_hidden, llm_gain) = operands[7:]
    outer, _ = group_bits()
    group_count = lax.axis_size("section") * lax.axis_size("dp")
    merged_rows = patches.shape[0] // 4
    run_cap = merged_rows // group_count
    seq_rows = text_embeds.shape[0]
    held = group_count * merged_rows * patches.shape[1] * patches.dtype.itemsize
    if lax.axis_size("mp") != 4 or outer != [("dp", 2), ("section", 1)] or held > KERNEL_BYTES or run_cap % 16 or merged_rows % 128 or seq_rows % 128:
        return plain_per_device(*operands)
    img, spot, base, total, incoming = merger(
        patches,
        patch_counts,
        dest_rows,
        qkv_weight.transpose(1, 2, 0),
        out_weight,
        attn_gain,
        merge_gain,
        fc1_weight,
        fc1_bias,
        fc2_weight,
        fc2_bias,
        text_embeds,
        section_hidden,
    )
    return placing(text_embeds, incoming, img, spot, total, base, llm_gain)


def solution(mesh):
    in_specs = (
        P(("section", "dp"), None),
        P(("section", "dp")),
        P(("section", "dp")),
        P(None, None, "mp"),
        P("mp", None),
        P(),
        P(),
        P("mp", ("section", "dp")),
        P(("section", "dp")),
        P(("section", "dp"), "mp"),
        P("mp"),
        P(("section", "dp"), "mp"),
        P(("section", "dp"), "mp"),
        P("mp"),
    )
    out_specs = (P(("section", "dp"), "mp"), P(("section", "dp"), "mp"))
    return jax.shard_map(
        per_device, mesh=mesh, in_specs=in_specs, out_specs=out_specs, check_vma=False
    )
```

```python
import functools
import math

import jax
import jax.numpy as jnp
from jax import lax
from jax.experimental import pallas as pl
from jax.experimental.pallas import tpu as pltpu
from jax.sharding import PartitionSpec as P

HEAD_DIM = 80
HID = 8192


vit_eps = 1e-06
llm_eps = 1e-06


def from_behind(value, axis, steps):
    count = lax.axis_size(axis)
    first, last = (max(0, -steps), min(count, count - steps))
    return lax.ppermute(value, axis, [(source, source + steps) for source in range(first, last)])


def layer_norm(values, gain):
    centred = values.astype(jnp.float32)
    centred = centred - jnp.mean(centred, axis=-1, keepdims=True)
    variance = jnp.mean(centred * centred, axis=-1, keepdims=True)
    return centred * lax.rsqrt(variance + vit_eps) * gain.astype(jnp.float32)


VMEM_LIMIT = 60 * 1024 * 1024
KERNEL_BYTES = 8 * 1024 * 1024


def vmem_call(kernel, out, scratch, sent_bytes, ident, *operands):
    return pl.pallas_call(
        kernel,
        out_shape=out,
        in_specs=[pl.BlockSpec(memory_space=pltpu.VMEM)] * len(operands),
        out_specs=pl.BlockSpec(memory_space=pltpu.VMEM),
        scratch_shapes=scratch,
        cost_estimate=pl.CostEstimate(
            flops=sent_bytes * 20000, bytes_accessed=sent_bytes * 2, transcendentals=0
        ),
        compiler_params=pltpu.CompilerParams(
            collective_id=ident, has_side_effects=True, vmem_limit_bytes=VMEM_LIMIT
        ),
    )(*operands)


def exchange_kernel(count, spread, x_ref, o_ref, send_sem, recv_sem, own_sem):
    me = lax.axis_index("mp")
    barrier = pltpu.get_barrier_semaphore()
    for step in range(1, count):
        peer = lax.rem(me + step, count)
        pl.semaphore_signal(
            barrier, inc=1, device_id={"mp": peer}, device_id_type=pl.DeviceIdType.MESH
        )
    pl.semaphore_wait(barrier, count - 1)
    copies = []
    for step in sorted(range(1, count), key=lambda s: -min(s, count - s)):
        peer = lax.rem(me + step, count)
        copy = pltpu.make_async_remote_copy(
            src_ref=x_ref.at[peer] if spread else x_ref,
            dst_ref=o_ref.at[me],
            send_sem=send_sem.at[step - 1],
            recv_sem=recv_sem.at[step - 1],
            device_id={"mp": peer},
            device_id_type=pl.DeviceIdType.MESH,
        )
        copy.start()
        copies.append(copy)
    own = pltpu.make_async_copy(x_ref.at[me] if spread else x_ref, o_ref.at[me], own_sem)
    own.start()
    own.wait()
    for copy in copies:
        copy.wait()


def relay_kernel(count, x_ref, o_ref, send_sem, recv_sem, own_sem):
    me = lax.axis_index("mp")
    barrier = pltpu.get_barrier_semaphore()
    for step in range(1, count):
        peer = lax.rem(me + step, count)
        pl.semaphore_signal(
            barrier, inc=1, device_id={"mp": peer}, device_id_type=pl.DeviceIdType.MESH
        )
    pl.semaphore_wait(barrier, count - 1)
    own = pltpu.make_async_copy(x_ref, o_ref.at[me], own_sem)
    own.start()

    def hop(way, step):
        owner = lax.rem(me - way * step + count, count)
        return pltpu.make_async_remote_copy(
            src_ref=o_ref.at[owner] if step else x_ref,
            dst_ref=o_ref.at[owner],
            send_sem=send_sem.at[(way + 1) // 2, step],
            recv_sem=recv_sem.at[(way + 1) // 2, step],
            device_id={"mp": lax.rem(me + way + count, count)},
            device_id_type=pl.DeviceIdType.MESH,
        )

    def holds(way, step):
        return me >= step if way > 0 else me + step < count

    def sends(way):
        return me < count - 1 if way > 0 else me > 0

    for step in range(count):
        for way in (1, -1):
            if step:

                @pl.when(holds(way, step))
                def _():
                    owner = lax.rem(me - way * step + count, count)
                    pltpu.make_async_remote_copy(
                        src_ref=x_ref,
                        dst_ref=o_ref.at[owner],
                        send_sem=send_sem.at[(way + 1) // 2, step - 1],
                        recv_sem=recv_sem.at[(way + 1) // 2, step - 1],
                        device_id={"mp": lax.rem(me - way + count, count)},
                        device_id_type=pl.DeviceIdType.MESH,
                    ).wait_recv()

            if step < count - 1:

                @pl.when(jnp.logical_and(holds(way, step), sends(way)))
                def _():
                    hop(way, step).start()

    own.wait()
    for step in range(count - 1):
        for way in (1, -1):

            @pl.when(jnp.logical_and(holds(way, step), sends(way)))
            def _():
                hop(way, step).wait_send()


def relay_mp(value, ident):
    count = lax.axis_size("mp")
    return vmem_call(
        functools.partial(relay_kernel, count),
        jax.ShapeDtypeStruct((count,) + value.shape, value.dtype),
        [
            pltpu.SemaphoreType.DMA((2, count - 1)),
            pltpu.SemaphoreType.DMA((2, count - 1)),
            pltpu.SemaphoreType.DMA,
        ],
        count * value.size * value.dtype.itemsize,
        ident,
        value,
    )


def exchange_mp(value, spread, ident):
    count = lax.axis_size("mp")
    shape = value.shape if spread else (count,) + value.shape
    size = math.prod(shape) * value.dtype.itemsize
    return vmem_call(
        functools.partial(exchange_kernel, count, spread),
        jax.ShapeDtypeStruct(shape, value.dtype),
        [
            pltpu.SemaphoreType.DMA((count - 1,)),
            pltpu.SemaphoreType.DMA((count - 1,)),
            pltpu.SemaphoreType.DMA,
        ],
        size,
        ident,
        value,
    )


def sum_scatter_mp(blocks, ident):
    return jnp.sum(exchange_mp(blocks, True, ident).astype(jnp.float32), axis=0)


def gather_mp(value):
    got = relay_mp(value, 2)
    return got.reshape((-1,) + value.shape[1:])


def total_mp(value):
    return jnp.sum(exchange_mp(value.reshape(-1, 128), False, 3), axis=0).reshape(-1)


def flip(index, bit):
    return index + bit * (1 - 2 * (index // bit % 2))


def group_bits():
    outer = [("dp", 1 << k) for k in range(1, lax.axis_size("dp").bit_length() - 1)]
    outer += [("section", 1 << k) for k in range(lax.axis_size("section").bit_length() - 1)]
    return outer, ("dp", 1)


def meets(axis, bit):
    return {axis: flip(lax.axis_index(axis), bit)}


def group_at(mask):
    spots = {axis: lax.axis_index(axis) for axis in ("section", "dp")}
    for axis, bit in mask:
        spots[axis] = flip(spots[axis], bit)
    return spots["section"] * lax.axis_size("dp") + spots["dp"]


def greet(bits):
    barrier = pltpu.get_barrier_semaphore()
    for axis, bit in bits:
        pl.semaphore_signal(
            barrier, inc=1, device_id=meets(axis, bit), device_id_type=pl.DeviceIdType.MESH
        )
    pl.semaphore_wait(barrier, len(bits))


def gather_kernel(x_ref, o_ref, send_sem, recv_sem, own_sem):
    outer, last = group_bits()
    greet(outer + [last])
    half = x_ref.shape[1] // 2
    sent, waiting = [], []
    slots = iter(range(send_sem.shape[0]))

    def pass_on(mask, stage, part, order):
        cols = pl.ds(part * half, half)
        spot = group_at(mask)
        source = o_ref.at[spot, :, cols] if mask else x_ref.at[:, cols]
        for later in range(stage, len(order)):
            slot = next(slots)
            copy = pltpu.make_async_remote_copy(
                src_ref=source,
                dst_ref=o_ref.at[spot, :, cols],
                send_sem=send_sem.at[slot],
                recv_sem=recv_sem.at[slot],
                device_id=meets(*order[later]),
                device_id_type=pl.DeviceIdType.MESH,
            )
            copy.start()
            sent.append(copy)
            waiting.append((later, copy, mask + [order[later]], part, order))

    pass_on([], 0, 0, outer + [last])
    pass_on([], 0, 1, outer[::-1] + [last])
    own = pltpu.make_async_copy(x_ref, o_ref.at[group_at([])], own_sem)
    own.start()
    while waiting:
        first = min(range(len(waiting)), key=lambda at: waiting[at][0])
        stage, copy, mask, part, order = waiting.pop(first)
        copy.wait_recv()
        pass_on(mask, stage + 1, part, order)
    for copy in sent:
        copy.wait_send()
    own.wait()


def gather_groups(value):
    count = lax.axis_size("section") * lax.axis_size("dp")
    size = count * value.size * value.dtype.itemsize
    if size > KERNEL_BYTES:
        return lax.all_gather(value, ("section", "dp"), axis=0, tiled=True)
    slots = 2 * (count - 1)
    got = vmem_call(
        gather_kernel,
        jax.ShapeDtypeStruct((count,) + value.shape, value.dtype),
        [
            pltpu.SemaphoreType.DMA((slots,)),
            pltpu.SemaphoreType.DMA((slots,)),
            pltpu.SemaphoreType.DMA,
        ],
        size,
        4,
        value,
    )
    return got.reshape(-1, value.shape[1])


def scatter_kernel(x_ref, o_ref, held, taken, send_sem, recv_sem):
    outer, first = group_bits()
    greet(outer + [first])
    rows = x_ref.shape[1]
    half = x_ref.shape[2] // 2
    chunk = 32
    orders = ([first] + outer, [first] + outer[::-1])
    slots = iter(range(send_sem.shape[0]))
    masks = [[]]
    for bit in outer:
        masks = masks + [mask + [bit] for mask in masks]
    place_of = {frozenset(mask): at for at, mask in enumerate(masks)}
    base = len(masks)
    live = {}

    def send(part, stage):
        cols = pl.ds(part * half, half)
        bit = orders[part][stage]
        kept = orders[part][stage + 1 :]
        copies = []
        for mask in [m for m in masks if set(m) <= set(kept)]:
            if stage == 0:
                source = x_ref.at[group_at(mask + [bit]), :, cols]
            else:
                source = held.at[place_of[frozenset(mask + [bit])], :, cols]
            landing = 2 * base - 2 ** (len(kept) + 1) + [
                m for m in masks if set(m) <= set(kept)
            ].index(mask)
            slot = next(slots)
            copy = pltpu.make_async_remote_copy(
                src_ref=source,
                dst_ref=taken.at[landing, :, cols],
                send_sem=send_sem.at[slot],
                recv_sem=recv_sem.at[slot],
                device_id=meets(*bit),
                device_id_type=pl.DeviceIdType.MESH,
            )
            copy.start()
            copies.append((copy, mask, landing))
        live[part, stage] = copies

    def add(part, stage):
        cols = pl.ds(part * half, half)
        final = stage + 1 == len(orders[part])
        following = None if final else orders[part][stage + 1]
        copies = live[part, stage]
        for copy, mask, landing in sorted(copies, key=lambda c: following not in c[1]):
            copy.wait_recv()
            at = place_of[frozenset(mask)]
            spot = group_at(mask)

            @pl.loop(0, rows // chunk)
            def _(step):
                span = pl.ds(step * chunk, chunk)
                mine = x_ref[spot, span, cols] if stage == 0 else held[at, span, cols]
                total = mine.astype(jnp.float32) + taken[landing, span, cols].astype(jnp.float32)
                if final:
                    o_ref[span, cols] = total
                else:
                    held[at, span, cols] = total.astype(held.dtype)

    send(0, 0)
    send(1, 0)
    for stage in range(len(orders[0])):
        for part in (0, 1):
            add(part, stage)
            if stage + 1 < len(orders[0]):
                send(part, stage + 1)
    for copies in live.values():
        for copy, _, _ in copies:
            copy.wait_send()


def sum_scatter_groups(value):
    count = lax.axis_size("section") * lax.axis_size("dp")
    size = value.size * value.dtype.itemsize
    if size > KERNEL_BYTES:
        return lax.psum_scatter(value, ("section", "dp"), scatter_dimension=0, tiled=True)
    rows, cols = value.shape[0] // count, value.shape[1]
    slots = 2 * (count - 1)
    return vmem_call(
        scatter_kernel,
        jax.ShapeDtypeStruct((rows, cols), jnp.float32),
        [
            pltpu.VMEM((count // 2, rows, cols), value.dtype),
            pltpu.VMEM((count - 1, rows, cols), value.dtype),
            pltpu.SemaphoreType.DMA((slots,)),
            pltpu.SemaphoreType.DMA((slots,)),
        ],
        size,
        5,
        value.reshape(count, rows, cols),
    )


def plain_per_device(
    patches,
    patch_counts,
    dest_rows,
    qkv_weight,
    out_weight,
    attn_gain,
    merge_gain,
    fc1_weight,
    fc1_bias,
    fc2_weight,
    fc2_bias,
    text_embeds,
    section_hidden,
    llm_gain,
):
    width = patches.shape[1]
    tile_total = patch_counts.shape[0]
    block_rows = patches.shape[0] // tile_total
    merged_rows = patches.shape[0] // 4
    local_cols = qkv_weight.shape[2]
    local_heads = local_cols // HEAD_DIM
    feature_cols = text_embeds.shape[1]
    seq_rows = text_embeds.shape[0]
    section_count = lax.axis_size("section")
    group_count = section_count * lax.axis_size("dp")
    run_cap = max(2, merged_rows // group_count)
    run_total = merged_rows // run_cap
    run_target = dest_rows.reshape(run_total, run_cap)[:, 0] // seq_rows
    takes = jnp.arange(group_count, dtype=jnp.int32)[:, None] == run_target[None, :]
    slot_in_tile = jnp.arange(merged_rows, dtype=jnp.int32) % (block_rows // 4)
    tile_counts = jnp.repeat(patch_counts, block_rows // 4, total_repeat_length=merged_rows)
    live = slot_in_tile * 4 < tile_counts
    place = jnp.where(live, dest_rows % seq_rows - seq_rows, 0).reshape(run_total, run_cap)
    send_place = jnp.sum(jnp.where(takes[:, :, None], place[None], 0), axis=1) + seq_rows
    got_place = lax.all_to_all(send_place, ("section", "dp"), split_axis=0, concat_axis=0, tiled=True)
    incoming = from_behind(section_hidden, "section", 1)
    normed_in = layer_norm(patches, attn_gain).astype(jnp.bfloat16)
    projections = jnp.dot(
        normed_in, qkv_weight.reshape(width, 3 * local_cols), preferred_element_type=jnp.float32
    ).astype(jnp.bfloat16)
    projections = projections.reshape(tile_total, block_rows, 3, local_heads, HEAD_DIM)
    query_part = projections[:, :, 0]
    key_part = projections[:, :, 1]
    value_part = projections[:, :, 2]
    scores = jnp.einsum(
        "tqhd,tkhd->thqk", query_part, key_part, preferred_element_type=jnp.float32
    ) * HEAD_DIM ** (-0.5)
    key_live = (
        jnp.arange(block_rows, dtype=jnp.int32)[None, None, None, :]
        < patch_counts[:, None, None, None]
    )
    scores = jnp.where(key_live, scores, -1e30)
    weights = jax.nn.softmax(scores, axis=-1).astype(jnp.bfloat16)
    attended = jnp.einsum(
        "thqk,tkhd->tqhd", weights, value_part, preferred_element_type=jnp.float32
    ).astype(jnp.bfloat16)
    attended = attended.reshape(patches.shape[0], local_cols)
    lane_source = jnp.arange(run_total, dtype=jnp.int32)[None, :] * run_cap
    run_source = jnp.sum(jnp.where(takes, lane_source, 0), axis=1)
    row_source = (
        run_source[:, None] + jnp.arange(run_cap, dtype=jnp.int32)[None, :]
    ).reshape(-1) * 4
    slots_at = jnp.arange(patches.shape[0], dtype=jnp.int32)
    patch_at = jnp.arange(4, dtype=jnp.int32)
    order = (
        (row_source[None, :] + patch_at[:, None]).reshape(-1)[:, None] == slots_at[None, :]
    ).astype(jnp.bfloat16)
    own_order = (
        (row_source + lax.axis_index("mp"))[:, None] == slots_at[None, :]
    ).astype(jnp.bfloat16)
    ordered = jnp.dot(order, attended, preferred_element_type=jnp.float32).astype(jnp.bfloat16)
    own_patch = jnp.dot(own_order, patches, preferred_element_type=jnp.float32)
    partial_proj = jnp.dot(ordered, out_weight, preferred_element_type=jnp.float32)
    own_proj = sum_scatter_mp(
        partial_proj.astype(jnp.bfloat16).reshape(4, group_count * run_cap, width), 0
    )
    block_out = (own_patch + own_proj).astype(jnp.bfloat16)
    merge_part = layer_norm(block_out, merge_gain).astype(jnp.bfloat16)
    slot_rows = group_count * run_cap
    gathered = gather_groups(merge_part)
    gathered = (
        gathered.reshape(group_count, group_count, run_cap, width)
        .transpose(1, 0, 2, 3)
        .reshape(group_count * slot_rows, width)
    )
    first_partial = jnp.dot(gathered, fc1_weight, preferred_element_type=jnp.float32)
    mp_count = lax.axis_size("mp")
    first_total = sum_scatter_mp(
        first_partial.astype(jnp.bfloat16).reshape(mp_count, -1, fc1_weight.shape[1]),
        1,
    )
    hidden_part = jax.nn.gelu(
        first_total + fc1_bias.astype(jnp.float32), approximate=False
    ).astype(jnp.bfloat16)
    hidden = gather_mp(hidden_part)
    second_partial = jnp.dot(hidden, fc2_weight, preferred_element_type=jnp.float32)
    embed_total = sum_scatter_groups(second_partial.astype(jnp.bfloat16)).astype(jnp.float32)
    image_embeds = (embed_total + fc2_bias.astype(jnp.float32)).astype(jnp.bfloat16)
    hits = got_place.reshape(1, -1) == jnp.arange(seq_rows, dtype=jnp.int32)[:, None]
    placed = jnp.dot(
        hits.astype(jnp.bfloat16), image_embeds, preferred_element_type=jnp.float32
    ).astype(jnp.bfloat16)
    sequence_embeds = jnp.where(jnp.any(hits, axis=1)[:, None], placed, text_embeds)
    entering = jnp.where(lax.axis_index("section") == 0, sequence_embeds, incoming).astype(
        jnp.float32
    )
    row_total = total_mp(jnp.sum(entering * entering, axis=1))
    layer_inputs = (
        entering * lax.rsqrt(row_total / HID + llm_eps)[:, None] * llm_gain.astype(jnp.float32)
    ).astype(jnp.bfloat16)
    return (sequence_embeds, layer_inputs)


LAG = 3
FC2_COLS = 512
HALF_ROOT = 0.5**0.5


def remote(src, dst, send_sem, recv_sem, device):
    return pltpu.make_async_remote_copy(
        src_ref=src,
        dst_ref=dst,
        send_sem=send_sem,
        recv_sem=recv_sem,
        device_id=device,
        device_id_type=pl.DeviceIdType.MESH,
    )


def group_device(group):
    per_section = lax.axis_size("dp")
    return {"section": group // per_section, "dp": lax.rem(group, per_section)}


def tell(device):
    pl.semaphore_signal(
        pltpu.get_barrier_semaphore(),
        inc=1,
        device_id=device,
        device_id_type=pl.DeviceIdType.MESH,
    )


def merger_kernel(
    patches_hbm,
    counts_ref,
    dest_ref,
    qkv_hbm,
    wo_hbm,
    attn_gain_ref,
    merge_gain_ref,
    w1_hbm,
    b1_ref,
    w2_hbm,
    b2_ref,
    text_hbm,
    carry_hbm,
    img_ref,
    spot_ref,
    base_ref,
    total_ref,
    incoming_hbm,
    patches_ref,
    qkv_ref,
    wo_ref,
    text_ref,
    carry_ref,
    text_squares,
    carry_squares,
    carry_sem,
    carry_send,
    carry_recv,
    normed,
    place_ref,
    sums_ref,
    query,
    key,
    value_part,
    attended,
    ordered,
    arrived,
    wo_all,
    x_ref,
    w1_ref,
    w2_ref,
    weight_sem,
    wo_send,
    wo_recv,
    wo_out,
    wo_plane,
    wo_pair,
    a_send,
    a_recv,
    rows,
    part,
    before,
    after,
    right_out,
    left_out,
    hidden,
    give,
    take,
    keep,
    x_out,
    x_in,
    y_out,
    y_in,
    squares,
    spots,
    sums,
    base_out,
    base_in,
    totals,
    row_send,
    row_recv,
    pair_recv,
    right_send,
    right_recv,
    left_send,
    left_recv,
    give_send,
    give_recv,
    x_send,
    x_recv,
    y_send,
    y_recv,
    spot_send,
    spot_recv,
    sum_send,
    sum_recv,
    base_send,
    base_recv,
    total_send,
    total_recv,
):
    groups = lax.axis_size("section") * lax.axis_size("dp")
    sections = lax.axis_size("section")
    line = lax.axis_size("mp")
    me = lax.axis_index("mp")
    section = lax.axis_index("section")
    dp = lax.axis_index("dp")
    core = lax.rem(dp, 2)
    column = dp // 2
    wide = lax.axis_size("dp") // 2
    group = section * lax.axis_size("dp") + dp
    chips = groups // 2
    pair = {"dp": flip(dp, 1)}
    over_x = {"dp": flip(dp, 2)}
    over_y = {"section": flip(section, 1)}
    quarters = 4
    pieces = chips * quarters
    take_rows = rows.shape[2] // 2
    lag_right = me * LAG
    half_rows = part.shape[3]
    split_from = 2
    single = 6
    run = half_rows // 2
    lag_left = (line - 1 - me) * LAG
    lag_total = (line - 1) * LAG

    fetches = [
        pltpu.make_async_copy(source, target, weight_sem.at[at])
        for at, (source, target) in enumerate(
            (
                (wo_hbm, wo_ref),
                (patches_hbm, patches_ref),
                (qkv_hbm, qkv_ref),
                (w1_hbm, w1_ref),
                (w2_hbm, w2_ref),
            )
        )
    ]
    for fetch in fetches:
        fetch.start()
    for step in range(1, groups):
        tell(group_device(lax.rem(group + step, groups)))
    for step in range(1, line):
        tell({"mp": lax.rem(me + step, line)})
    pl.semaphore_wait(pltpu.get_barrier_semaphore(), groups + line - 2)

    def chip_of(quarter):
        there_x = lax.rem(quarter // 2 + column, 2)
        there_y = lax.rem(lax.rem(quarter, 2) + section, 2)
        return there_y * wide + there_x

    def group_of(quarter, at_core):
        return chip_of(quarter) * 2 + at_core

    def own_send(chunk, which):
        sem = (row_recv.at[chunk, 1], row_recv.at[chunk, 2], pair_recv.at[chunk, 0])[which]
        device = (over_y, over_x, pair)[which]
        return remote(x_ref.at[chunk], rows.at[group, chunk], row_send.at[chunk, which], sem, device)

    def forward_x(chunk):
        spot = rows.at[group_of(1, core), chunk]
        return remote(spot, spot, row_send.at[chunk, 3], row_recv.at[chunk, 3], over_x)

    def forward_pair(chunk, quarter):
        spot = rows.at[group_of(quarter, core), chunk]
        return remote(
            spot, spot, row_send.at[chunk, 3 + quarter], pair_recv.at[chunk, quarter], pair
        )

    leads = section < sections - 1
    bands = carry_send.shape[0]
    band_rows = carry_hbm.shape[0] // bands
    text_fetch = pltpu.make_async_copy(text_hbm, text_ref, carry_sem.at[0])
    carry_fetch = pltpu.make_async_copy(carry_hbm, carry_ref, carry_sem.at[1])

    @pl.when(leads)
    def _():
        text_fetch.start()
        carry_fetch.start()

    def send_band(at):
        cut = pl.ds(pl.multiple_of(at * band_rows, band_rows), band_rows)
        return remote(
            carry_hbm.at[cut], incoming_hbm.at[cut], carry_send.at[at], carry_recv.at[at], {"section": section + 1}
        )

    def send_bands(first, last):
        @pl.when(leads)
        def _():
            for at in range(first, last):
                send_band(at).start()

    early = bands // 10
    looped = bands - early - bands // 6

    def wo_slice(ref, holder):
        high = wo_ref.shape[0] // lax.axis_size("dp")
        broad = wo_ref.shape[1] // sections
        top = pl.multiple_of(lax.rem(holder, lax.axis_size("dp")) * high, high)
        left = pl.multiple_of(holder // lax.axis_size("dp") * broad, broad)
        return ref.at[pl.ds(top, high), pl.ds(left, broad)]

    def wo_line(step):
        return remote(
            wo_slice(wo_ref, group),
            wo_slice(wo_all.at[me], group),
            wo_send.at[step - 1],
            wo_recv.at[step - 1],
            {"mp": lax.rem(me + step, line)},
        )

    def wo_hop(step, quarter, at, sem, device):
        block = wo_slice(wo_all.at[lax.rem(me - step + line, line)], group_of(quarter, core))
        return remote(block, block, wo_out.at[step - 1, at], sem, device)

    def wo_starts(step):
        return (
            wo_hop(step, 0, 0, wo_plane.at[step - 1, 1], over_y),
            wo_hop(step, 0, 1, wo_plane.at[step - 1, 2], over_x),
            wo_hop(step, 0, 2, wo_pair.at[step - 1, 0], pair),
        )

    def wo_forward_x(step):
        return wo_hop(step, 1, 3, wo_plane.at[step - 1, 3], over_x)

    def wo_forward_pair(step, quarter):
        return wo_hop(step, quarter, 3 + quarter, wo_pair.at[step - 1, quarter], pair)

    def wo_landed(step, quarter):
        return wo_hop(step, quarter, 0, wo_plane.at[step - 1, quarter], over_x)

    def wo_paired(step, quarter):
        block = wo_slice(wo_all.at[lax.rem(me - step + line, line)], group_of(quarter, 1 - core))
        return remote(block, block, wo_out.at[step - 1, 0], wo_pair.at[step - 1, quarter], pair)

    steps = range(1, line)
    low_end, high_end = me == 0, me == line - 1
    at_end = jnp.logical_or(low_end, high_end)
    first_sent = jnp.where(high_end, 3, 1)
    second = jnp.where(at_end, 2, 3)
    last_sent = jnp.where(low_end, 3, jnp.where(high_end, 1, 2))
    first_here = jnp.where(low_end, 3, 1)
    last_here = jnp.where(low_end, 1, jnp.where(high_end, 3, 2))
    fetches[0].wait()
    for step in (first_sent, second, last_sent):
        wo_line(step).start()

    send_bands(0, early)
    slots = ordered.shape[1]
    dest = dest_ref[...].reshape(1, slots)
    slot = lax.broadcasted_iota(jnp.int32, (1, slots), 1)
    tiles = counts_ref.shape[0]
    slice_rows = carry_hbm.shape[0]
    target = dest // slice_rows
    slot_place = slot
    for stride in [1 << bit for bit in range(run.bit_length() - 1, slots.bit_length())][::-1]:
        slot_place = jnp.where(slot_place >= stride, slot_place - stride, slot_place)
    slot_target = target * run + slot_place
    filled = jnp.zeros((1, slots), jnp.int32)
    for tile in range(tiles):
        start = tile * (slots // tiles)
        within = jnp.logical_and(slot >= start, slot - start < slots // tiles)
        filled = jnp.where(jnp.logical_and(within, (slot - start) * 4 < counts_ref[tile]), 1, filled)
    spot = jnp.where(filled > 0, dest - target * slice_rows, slice_rows)
    high = (spot // 16).astype(jnp.float32)
    low = (spot - spot // 16 * 16).astype(jnp.float32)
    to_group = lax.broadcasted_iota(jnp.int32, (groups, slots), 0) == target
    at_source = lax.broadcasted_iota(jnp.int32, (slots, slots), 1)
    moved = (at_source == group * run + slot_place.reshape(slots, 1)).astype(jnp.float32).astype(jnp.bfloat16)

    def moved_to(value):
        picked = jnp.where(to_group, value, 0.0).astype(jnp.bfloat16)
        return jnp.dot(picked, moved, preferred_element_type=jnp.float32)

    place_rows = (moved_to(high) * 16.0 + moved_to(low)).astype(jnp.int32)
    place_ref[...] = place_rows.reshape(place_ref.shape)
    place_copies = []
    for step in range(1, groups):
        peer = lax.rem(group + step, groups)
        copy = remote(
            place_ref.at[peer], spots.at[step], spot_send.at[step - 1], spot_recv.at[step - 1], group_device(peer)
        )
        copy.start()
        place_copies.append(copy)
    spots[0] = place_ref[group]

    tall = min(patches_ref.shape[0], 128)
    fetches[1].wait()

    @pl.loop(0, patches_ref.shape[0] // tall)
    def _(at):
        cut = pl.ds(at * tall, tall)
        normed[cut] = layer_norm(
            patches_ref[cut], attn_gain_ref[...].reshape(1, -1)
        ).astype(normed.dtype)

    fetches[2].wait()
    for which, ref in enumerate((query, key, value_part)):
        ref[...] = lax.dot_general(
            normed[...], qkv_ref[which], (((1,), (1,)), ((), ())), preferred_element_type=jnp.float32
        ).astype(ref.dtype)

    def begin(step):
        wo_line(step).wait_recv()
        for copy in wo_starts(step):
            copy.start()

    def pass_y(step):
        wo_landed(step, 1).wait_recv()
        wo_forward_x(step).start()
        wo_forward_pair(step, 1).start()

    def pass_x(step, quarter):
        wo_landed(step, quarter).wait_recv()
        wo_forward_pair(step, quarter).start()

    begin(first_here)
    wo_all[me] = wo_ref[...]

    block = query.shape[0] // tiles
    lane = lax.broadcasted_iota(jnp.int32, (1, query.shape[1]), 1)
    at_key = lax.broadcasted_iota(jnp.int32, (block, block), 1)

    def attend(tile):
        cut = pl.ds(tile * block, block)
        tile_query, tile_key, tile_value = query[cut], key[cut], value_part[cut]
        live = at_key < counts_ref[tile]
        result = jnp.zeros((block, query.shape[1]), jnp.float32)
        for head in range(query.shape[1] // HEAD_DIM):
            own = jnp.logical_and(lane >= head * HEAD_DIM, lane < (head + 1) * HEAD_DIM)
            own = own.astype(jnp.float32).astype(jnp.bfloat16)
            scores = lax.dot_general(
                tile_query * own, tile_key, (((1,), (1,)), ((), ())), preferred_element_type=jnp.float32
            )
            scores = jnp.where(live, scores * HEAD_DIM**-0.5, -1e30)
            power = jnp.exp(scores - jnp.max(scores, axis=1, keepdims=True))
            weights = (power / jnp.sum(power, axis=1, keepdims=True)).astype(jnp.bfloat16)
            result = result + jnp.dot(weights, tile_value * own, preferred_element_type=jnp.float32)
        attended[cut] = result.astype(attended.dtype)

    for tile in range(tiles):
        attend(tile)
        if tile == 0:
            begin(second)
    pass_y(first_here)
    begin(last_here)
    send_bands(early, bands - looped)

    whole = attended.shape[0]
    at_row = lax.broadcasted_iota(jnp.int32, (slots, whole), 0)
    at_patch = lax.broadcasted_iota(jnp.int32, (slots, whole), 1)
    order = (
        lax.broadcasted_iota(jnp.int32, (slots, slots), 0) == slot_target
    ).astype(jnp.float32).astype(jnp.bfloat16)

    def picked(patch, source):
        pick = (at_patch == at_row * line + patch).astype(jnp.float32).astype(jnp.bfloat16)
        rows_of = jnp.dot(pick, source, preferred_element_type=jnp.float32).astype(jnp.bfloat16)
        return jnp.dot(order, rows_of, preferred_element_type=jnp.float32)

    for patch in range(line):
        ordered[patch] = picked(patch, attended[...]).astype(ordered.dtype)

    def exchange(step):
        peer = lax.rem(me + step, line)
        return remote(ordered.at[peer], arrived.at[me], a_send.at[step - 1], a_recv.at[step - 1], {"mp": peer})

    for step in steps:
        exchange(step).start()
    arrived[me] = ordered[me]
    block_out = picked(me, patches_ref[...])
    pass_y(second)
    pass_x(first_here, 2)
    pass_y(last_here)
    pass_x(second, 2)
    pass_x(first_here, 3)
    pass_x(last_here, 2)
    pass_x(second, 3)
    pass_x(last_here, 3)
    for step in steps:
        for quarter in range(quarters):
            wo_paired(step, quarter).wait_recv()
    for step in steps:
        exchange(step).wait_recv()
    for source in range(line):
        block_out = block_out + jnp.dot(
            arrived[source], wo_all[source], preferred_element_type=jnp.float32
        )
    block_out = block_out.astype(jnp.bfloat16)
    x_ref[...] = (
        layer_norm(block_out, merge_gain_ref[...].reshape(1, -1)).astype(x_ref.dtype).reshape(x_ref.shape)
    )
    for chunk in range(chips):
        own_send(chunk, 0).start()
    for which in (1, 2):
        own_send(0, which).start()
    rows[group] = x_ref[...]
    for fetch in fetches[3:]:
        fetch.wait()

    def send_right(piece):
        return remote(
            right_out.at[piece], before.at[piece], right_send.at[piece], right_recv.at[piece], {"mp": me + 1}
        )

    def send_left(piece):
        return remote(
            left_out.at[piece], after.at[piece], left_send.at[piece], left_recv.at[piece], {"mp": me - 1}
        )

    def send_give(chunk):
        return remote(give.at[chunk], take.at[chunk], give_send.at[chunk], give_recv.at[chunk], pair)

    parts = x_send.shape[1]
    span = keep.shape[1] // parts

    def send_x(chunk, at):
        cut = pl.ds(at * span, span)
        return remote(
            x_out.at[chunk, cut], x_in.at[chunk, cut], x_send.at[chunk, at], x_recv.at[chunk, at], over_x
        )

    def send_y(at):
        cut = pl.ds(at * span, span)
        return remote(y_out.at[cut], y_in.at[cut], y_send.at[at], y_recv.at[at], over_y)

    def settle(chunk):
        send_give(chunk).wait_recv()
        mine = lax.rem(chunk, wide) == column

        @pl.when(mine)
        def _():
            @pl.loop(0, parts)
            def _(at):
                cut = pl.ds(at * span, span)
                keep[chunk, cut] = keep[chunk, cut] + take[chunk, cut].astype(jnp.float32)

        @pl.when(jnp.logical_not(mine))
        def _():
            @pl.loop(0, parts)
            def _(at):
                cut = pl.ds(at * span, span)
                x_out[chunk, cut] = (
                    keep[chunk, cut] + take[chunk, cut].astype(jnp.float32)
                ).astype(x_out.dtype)
                send_x(chunk, at).start()

    sum_rows = base_out.shape[0]

    def folded(value):
        value = value.astype(jnp.float32)
        square = value * value
        width = squares.shape[1]
        total = square[:, :width]
        for at_col in range(1, square.shape[1] // width):
            total = total + square[:, at_col * width : (at_col + 1) * width]
        return total

    def exchange_sums(step):
        return remote(
            sums_ref, sums.at[step], sum_send.at[step - 1], sum_recv.at[step - 1], {"mp": lax.rem(me + step, line)}
        )

    send_base = remote(base_out, base_in, base_send, base_recv, {"section": section + 1})
    share = text_ref.shape[0] // pieces

    def stage(i, carry):
        for extra in range(2):
            band = bands - looped + (i - quarters) * 2 + extra

            @pl.when(jnp.logical_and(leads, jnp.logical_and(i >= quarters, band < bands)))
            def _():
                send_band(band).start()

        @pl.when(jnp.logical_and(leads, i < pieces))
        def _():
            @pl.when(i == 0)
            def _():
                text_fetch.wait()
                carry_fetch.wait()

            cut = pl.ds(pl.multiple_of(i * share, share), share)
            text_squares[cut] = folded(text_ref[cut])
            carry_squares[cut] = folded(carry_ref[cut])

        @pl.when(jnp.logical_and(leads, i == pieces))
        def _():
            for which, ref in enumerate((text_squares, carry_squares)):
                for at in range(sum_rows):
                    cut = pl.ds(at * 128, 128)
                    at_sum = which * sum_rows + at
                    sums_ref[at_sum : at_sum + 1] = jnp.sum(ref[cut].T, axis=0, keepdims=True)
            for step in steps:
                exchange_sums(step).start()

        @pl.when(jnp.logical_and(leads, i == pieces + 4))
        def _():
            both = sums_ref[...]
            for step in steps:
                exchange_sums(step).wait()
                both = both + sums[step]
            base_out[...] = both[sum_rows:]
            base_ref[...] = both[:sum_rows]
            send_base.start()

        def relay(piece):
            chunk = piece // quarters
            quarter = lax.rem(piece, quarters)

            @pl.when(quarter == 1)
            def _():
                remote(
                    x_ref.at[chunk], rows.at[group_of(1, core), chunk], row_send.at[chunk, 0], row_recv.at[chunk, 1], over_y
                ).wait_recv()
                forward_x(chunk).start()
                forward_pair(chunk, 1).start()

                @pl.when(chunk + 1 < chips)
                def _():
                    for which in (1, 2):
                        own_send(chunk + 1, which).start()

            @pl.when(quarter > 1)
            def _():
                remote(
                    x_ref.at[chunk], rows.at[group_of(quarter, core), chunk], row_send.at[chunk, 1], row_recv.at[chunk, quarter], over_x
                ).wait_recv()
                forward_pair(chunk, quarter).start()

        def multiply(piece):
            chunk = piece // quarters
            quarter = lax.rem(piece, quarters)
            spot = rows.at[group_of(quarter, 1 - core), chunk]
            remote(x_ref.at[chunk], spot, row_send.at[chunk, 2], pair_recv.at[chunk, quarter], pair).wait_recv()
            lhs = rows[pl.ds(chip_of(quarter) * 2, 2), chunk]
            result = jnp.dot(
                lhs.reshape(-1, lhs.shape[2]), w1_ref[...], preferred_element_type=jnp.float32
            ).reshape(2, 2, run, part.shape[4])
            for target in range(2):
                part[chunk, quarter, target] = result[:, target].reshape(part.shape[3:])

        def once_then_twice(turn, work):
            @pl.when(jnp.logical_and(turn >= 0, turn < single))
            def _():
                work(turn)

            @pl.when(jnp.logical_and(turn >= single, turn < (pieces + single) // 2))
            def _():
                work(turn * 2 - single)
                work(turn * 2 - single + 1)

        once_then_twice(i, relay)
        once_then_twice(i - 1, multiply)

        def halves(piece):
            chunk = piece // quarters
            turn = lax.rem(piece, quarters)
            first_quarter = jnp.where(chunk < split_from, turn, lax.rem(turn, 2) * 2)
            last_quarter = jnp.where(chunk < split_from, turn, lax.rem(turn, 2) * 2 + 1)
            first_target = jnp.where(chunk < split_from, 0, turn // 2)
            last_target = jnp.where(chunk < split_from, 1, turn // 2)
            low_half, high_half = pl.ds(0, half_rows), pl.ds(half_rows, half_rows)
            return (
                (low_half, (chunk, first_quarter, first_target)),
                (high_half, (chunk, last_quarter, last_target)),
            )

        at_right = i - 1 - lag_right

        @pl.when(jnp.logical_and(me < line - 1, jnp.logical_and(at_right >= 0, at_right < pieces)))
        def _():
            @pl.when(me == 0)
            def _():
                for cut, spot in halves(at_right):
                    right_out[at_right, cut] = part[spot].astype(right_out.dtype)

            @pl.when(me > 0)
            def _():
                send_right(at_right).wait_recv()
                for cut, spot in halves(at_right):
                    right_out[at_right, cut] = (
                        part[spot] + before[at_right, cut].astype(jnp.float32)
                    ).astype(right_out.dtype)

            send_right(at_right).start()

        at_left = i - 1 - lag_left

        @pl.when(jnp.logical_and(me > 0, jnp.logical_and(at_left >= 0, at_left < pieces)))
        def _():
            @pl.when(me == line - 1)
            def _():
                for cut, spot in halves(at_left):
                    left_out[at_left, cut] = part[spot].astype(left_out.dtype)

            @pl.when(me < line - 1)
            def _():
                send_left(at_left).wait_recv()
                for cut, spot in halves(at_left):
                    left_out[at_left, cut] = (
                        part[spot] + after[at_left, cut].astype(jnp.float32)
                    ).astype(left_out.dtype)

            send_left(at_left).start()

        at_total = i - 1 - lag_total

        @pl.when(at_total >= 0)
        def _():
            chunk = at_total // quarters
            turn = lax.rem(at_total, quarters)

            @pl.when(
                jnp.logical_and(
                    jnp.logical_and(turn == 0, chunk > 0), jnp.logical_or(chunk <= split_from, core == 1)
                )
            )
            def _():
                settle(chunk - 1)

            @pl.when(jnp.logical_and(jnp.logical_and(turn == 2, chunk >= split_from), core == 0))
            def _():
                settle(chunk)

            @pl.when(me == line - 1)
            def _():
                send_right(at_total).wait_recv()

            @pl.when(me == 0)
            def _():
                send_left(at_total).wait_recv()

            for cut, spot in halves(at_total):
                _, quarter, target = spot

                @pl.when(me > 0)
                def _():
                    part[spot] = part[spot] + before[at_total, cut].astype(jnp.float32)

                @pl.when(me < line - 1)
                def _():
                    part[spot] = part[spot] + after[at_total, cut].astype(jnp.float32)

                value = part[spot] + b1_ref[...].reshape(1, -1).astype(jnp.float32)
                value = 0.5 * value * (1.0 + lax.erf(value * HALF_ROOT))
                hidden[chunk, target, chip_of(quarter)] = value.astype(hidden.dtype)

            def project(target):
                lhs = hidden[chunk, target].reshape(-1, hidden.shape[4])

                @pl.loop(0, w2_ref.shape[1] // FC2_COLS)
                def _(at):
                    cols = pl.ds(pl.multiple_of(at * FC2_COLS, FC2_COLS), FC2_COLS)
                    result = jnp.dot(lhs, w2_ref[:, cols], preferred_element_type=jnp.float32)

                    @pl.when(core == target)
                    def _():
                        keep[chunk, :, cols] = result

                    @pl.when(core != target)
                    def _():
                        give[chunk, :, cols] = result.astype(give.dtype)

                @pl.when(core != target)
                def _():
                    send_give(chunk).start()

            @pl.when(jnp.logical_and(turn == 1, chunk >= split_from))
            def _():
                project(0)

            @pl.when(turn == quarters - 1)
            def _():
                @pl.when(chunk < split_from)
                def _():
                    project(0)

                project(1)

        return carry

    lax.fori_loop(0, pieces + 1 + lag_total, stage, 0)

    @pl.when(core == 1)
    def _():
        settle(chips - 1)

    spot_sum = spots[0]
    for copy in place_copies:
        copy.wait_recv()
    for step in range(1, groups):
        spot_sum = spot_sum + spots[step]
    spot_ref[...] = spot_sum

    @pl.when(section > 0)
    def _():
        send_base.wait_recv()
        base_ref[...] = base_in[...]

        @pl.loop(0, bands)
        def _(at):
            remote(
                carry_hbm.at[pl.ds(0, band_rows)], incoming_hbm.at[pl.ds(0, band_rows)], carry_send.at[at], carry_recv.at[at], over_y
            ).wait_recv()

    own_chunk = section * wide + column
    y_chunk = flip(section, 1) * wide + column

    @pl.loop(0, parts)
    def _(at):
        cut = pl.ds(at * span, span)
        send_x(y_chunk, at).wait_recv()
        y_out[cut] = (keep[y_chunk, cut] + x_in[y_chunk, cut].astype(jnp.float32)).astype(y_out.dtype)
        send_y(at).start()

    @pl.loop(0, parts)
    def _(at):
        cut = pl.ds(at * span, span)
        send_x(own_chunk, at).wait_recv()
        send_y(at).wait_recv()
        value = (
            keep[own_chunk, cut]
            + x_in[own_chunk, cut].astype(jnp.float32)
            + y_in[cut].astype(jnp.float32)
            + b2_ref[...].reshape(1, -1).astype(jnp.float32)
        ).astype(img_ref.dtype)
        img_ref[cut] = value
        squares[cut] = folded(value)

    totals[0] = jnp.sum(squares[...].T, axis=0, keepdims=True)
    total_copies = []
    for step in range(1, line):
        copy = remote(
            totals.at[0], totals.at[step], total_send.at[step - 1], total_recv.at[step - 1], {"mp": lax.rem(me + step, line)}
        )
        copy.start()
        total_copies.append(copy)

    for step in steps:
        wo_line(step).wait_send()
        for copy in wo_starts(step) + (wo_forward_x(step),):
            copy.wait_send()
        for quarter in range(1, quarters):
            wo_forward_pair(step, quarter).wait_send()
        exchange(step).wait_send()

    for chunk in range(chips):
        for which in range(3):
            own_send(chunk, which).wait_send()
        forward_x(chunk).wait_send()
        for quarter in range(1, quarters):
            forward_pair(chunk, quarter).wait_send()
        send_give(chunk).wait_send()

        @pl.when(chunk % wide != column)
        def _():
            for at in range(parts):
                send_x(chunk, at).wait_send()

    for at in range(parts):
        send_y(at).wait_send()

    @pl.when(me < line - 1)
    def _():
        @pl.loop(0, pieces)
        def _(piece):
            send_right(piece).wait_send()

    @pl.when(me > 0)
    def _():
        @pl.loop(0, pieces)
        def _(piece):
            send_left(piece).wait_send()

    for copy in place_copies:
        copy.wait_send()

    @pl.when(leads)
    def _():
        send_base.wait_send()

        @pl.loop(0, bands)
        def _(at):
            send_band(at).wait_send()

    row_total = totals[0]
    for step, copy in enumerate(total_copies):
        copy.wait()
        row_total = row_total + totals[step + 1]
    total_ref[...] = row_total


def merger(patches, counts, dest, qkv, wo, attn_gain, merge_gain, w1, b1, w2, b2, text, carry):
    groups = lax.axis_size("section") * lax.axis_size("dp")
    line = lax.axis_size("mp")
    chips = groups // 2
    patch_rows, width = patches.shape
    slot_rows = patch_rows // 4
    chunk_rows = slot_rows // chips
    run = chunk_rows // 2
    local_cols = qkv.shape[1]
    units = w1.shape[1]
    features = w2.shape[1]
    pieces = chips * 4
    piece_rows = 2 * chunk_rows
    target_rows = groups * run
    parts = 4
    low = jnp.bfloat16
    dma = pltpu.SemaphoreType.DMA
    sum_rows = text.shape[0] // 128
    bands = text.shape[0] // 16
    return pl.pallas_call(
        merger_kernel,
        out_shape=(
            jax.ShapeDtypeStruct((target_rows, features), low),
            jax.ShapeDtypeStruct((1, slot_rows), jnp.int32),
            jax.ShapeDtypeStruct((sum_rows, 128), jnp.float32),
            jax.ShapeDtypeStruct((1, target_rows), jnp.float32),
            jax.ShapeDtypeStruct(carry.shape, carry.dtype),
        ),
        in_specs=[
            pl.BlockSpec(memory_space={1: pltpu.SMEM, 2: pltpu.VMEM, 5: pltpu.VMEM, 6: pltpu.VMEM, 8: pltpu.VMEM, 10: pltpu.VMEM}.get(at, pl.ANY))
            for at in range(13)
        ],
        out_specs=[pl.BlockSpec(memory_space=pltpu.VMEM)] * 4 + [pl.BlockSpec(memory_space=pl.ANY)],
        scratch_shapes=[
            pltpu.VMEM(patches.shape, low),
            pltpu.VMEM(qkv.shape, low),
            pltpu.VMEM(wo.shape, low),
            pltpu.VMEM(text.shape, low),
            pltpu.VMEM(text.shape, low),
            pltpu.VMEM((text.shape[0], 128), jnp.float32),
            pltpu.VMEM((text.shape[0], 128), jnp.float32),
            dma((2,)),
            dma((bands,)),
            dma((bands,)),
            pltpu.VMEM(patches.shape, low),
            pltpu.VMEM((groups, 1, slot_rows), jnp.int32),
            pltpu.VMEM((2 * sum_rows, 128), jnp.float32),
            pltpu.VMEM((patch_rows, local_cols), low),
            pltpu.VMEM((patch_rows, local_cols), low),
            pltpu.VMEM((patch_rows, local_cols), low),
            pltpu.VMEM((patch_rows, local_cols), low),
            pltpu.VMEM((4, slot_rows, local_cols), low),
            pltpu.VMEM((line, slot_rows, local_cols), low),
            pltpu.VMEM((line,) + wo.shape, low),
            pltpu.VMEM((chips, chunk_rows, width), low),
            pltpu.VMEM(w1.shape, low),
            pltpu.VMEM(w2.shape, low),
            dma((5,)),
            dma((line - 1,)),
            dma((line - 1,)),
            dma((line - 1, 7)),
            dma((line - 1, 4)),
            dma((line - 1, 4)),
            dma((line - 1,)),
            dma((line - 1,)),
            pltpu.VMEM((groups, chips, chunk_rows, width), low),
            pltpu.VMEM((chips, 4, 2, chunk_rows, units), jnp.float32),
            pltpu.VMEM((pieces, piece_rows, units), low),
            pltpu.VMEM((pieces, piece_rows, units), low),
            pltpu.VMEM((pieces, piece_rows, units), low),
            pltpu.VMEM((pieces, piece_rows, units), low),
            pltpu.VMEM((chips, 2, chips, chunk_rows, units), low),
            pltpu.VMEM((chips, target_rows, features), low),
            pltpu.VMEM((chips, target_rows, features), low),
            pltpu.VMEM((chips, target_rows, features), jnp.float32),
            pltpu.VMEM((chips, target_rows, features), low),
            pltpu.VMEM((chips, target_rows, features), low),
            pltpu.VMEM((target_rows, features), low),
            pltpu.VMEM((target_rows, features), low),
            pltpu.VMEM((target_rows, 128), jnp.float32),
            pltpu.VMEM((groups, 1, slot_rows), jnp.int32),
            pltpu.VMEM((line, 2 * sum_rows, 128), jnp.float32),
            pltpu.VMEM((sum_rows, 128), jnp.float32),
            pltpu.VMEM((sum_rows, 128), jnp.float32),
            pltpu.VMEM((line, 1, target_rows), jnp.float32),
            dma((chips, 7)),
            dma((chips, 4)),
            dma((chips, 4)),
            dma((pieces,)),
            dma((pieces,)),
            dma((pieces,)),
            dma((pieces,)),
            dma((chips,)),
            dma((chips,)),
            dma((chips, parts)),
            dma((chips, parts)),
            dma((parts,)),
            dma((parts,)),
            dma((groups - 1,)),
            dma((groups - 1,)),
            dma((line - 1,)),
            dma((line - 1,)),
            dma,
            dma,
            dma((line - 1,)),
            dma((line - 1,)),
        ],
        cost_estimate=pl.CostEstimate(
            flops=10**11, bytes_accessed=10**7, transcendentals=0
        ),
        compiler_params=pltpu.CompilerParams(
            collective_id=6, has_side_effects=True, vmem_limit_bytes=VMEM_LIMIT
        ),
    )(patches, counts, dest, qkv, wo, attn_gain, merge_gain, w1, b1, w2, b2, text, carry)


def placing_kernel(
    text_hbm,
    incoming_hbm,
    img_ref,
    spot_ref,
    total_ref,
    base_ref,
    gain_ref,
    seq_hbm,
    layer_hbm,
    text,
    incoming,
    seq,
    layer,
    load_sem,
    store_sem,
):
    cuts = base_ref.shape[0]
    height = text.shape[0] // cuts
    first = lax.axis_index("section") == 0
    gain = gain_ref[...].reshape(1, -1).astype(jnp.float32)

    def move(which, at):
        cut = pl.ds(at * height, height)
        source, target, sem = (
            (text_hbm, text, load_sem.at[0, at]),
            (incoming_hbm, incoming, load_sem.at[1, at]),
            (seq, seq_hbm, store_sem.at[0, at]),
            (layer, layer_hbm, store_sem.at[1, at]),
        )[which]
        return pltpu.make_async_copy(source.at[cut], target.at[cut], sem)

    for at in range(cuts):
        move(0, at).start()

        @pl.when(jnp.logical_not(first))
        def _():
            move(1, at).start()

    width = base_ref.shape[1]
    diagonal = lax.broadcasted_iota(jnp.int32, (height, width), 0) == lax.broadcasted_iota(
        jnp.int32, (height, width), 1
    )
    for at in range(cuts):
        cut = pl.ds(at * height, height)
        at_row = at * height + lax.broadcasted_iota(jnp.int32, (height, spot_ref.shape[1]), 0)
        hits = spot_ref[...] == at_row
        hit = jnp.max(hits.astype(jnp.float32), axis=1, keepdims=True) > 0.0
        placed = jnp.dot(
            hits.astype(jnp.float32).astype(jnp.bfloat16), img_ref[...], preferred_element_type=jnp.float32
        ).astype(jnp.bfloat16)
        base = jnp.sum(jnp.where(diagonal, base_ref[at : at + 1], 0.0), axis=1, keepdims=True)
        move(0, at).wait()
        seq[cut] = jnp.where(hit, placed, text[cut])
        move(2, at).start()

        @pl.when(first)
        def _():
            total = jnp.sum(jnp.where(hits, total_ref[...], 0.0), axis=1, keepdims=True)
            total = jnp.where(hit, total, base)
            scale = lax.rsqrt(total / HID + llm_eps)
            layer[cut] = (seq[cut].astype(jnp.float32) * scale * gain).astype(layer.dtype)

        @pl.when(jnp.logical_not(first))
        def _():
            move(1, at).wait()
            scale = lax.rsqrt(base / HID + llm_eps)
            layer[cut] = (incoming[cut].astype(jnp.float32) * scale * gain).astype(layer.dtype)

        move(3, at).start()

    for at in range(cuts):
        move(2, at).wait()
        move(3, at).wait()


def placing(text, incoming, img, spot, total, base, gain):
    cuts = base.shape[0]
    return pl.pallas_call(
        placing_kernel,
        out_shape=(jax.ShapeDtypeStruct(text.shape, text.dtype),) * 2,
        in_specs=[pl.BlockSpec(memory_space=pl.ANY)] * 2 + [pl.BlockSpec(memory_space=pltpu.VMEM)] * 5,
        out_specs=[pl.BlockSpec(memory_space=pl.ANY)] * 2,
        scratch_shapes=[pltpu.VMEM(text.shape, text.dtype)] * 4
        + [pltpu.SemaphoreType.DMA((2, cuts)), pltpu.SemaphoreType.DMA((2, cuts))],
        cost_estimate=pl.CostEstimate(flops=10**9, bytes_accessed=10**7, transcendentals=0),
        compiler_params=pltpu.CompilerParams(vmem_limit_bytes=VMEM_LIMIT),
    )(text, incoming, img, spot, total, base, gain)


def per_device(*operands):
    (patches, patch_counts, dest_rows, qkv_weight, out_weight, attn_gain, merge_gain) = operands[:7]
    (fc1_weight, fc1_bias, fc2_weight, fc2_bias, text_embeds, section_hidden, llm_gain) = operands[7:]
    outer, _ = group_bits()
    group_count = lax.axis_size("section") * lax.axis_size("dp")
    merged_rows = patches.shape[0] // 4
    run_cap = merged_rows // group_count
    seq_rows = text_embeds.shape[0]
    held = group_count * merged_rows * patches.shape[1] * patches.dtype.itemsize
    if lax.axis_size("mp") != 4 or outer != [("dp", 2), ("section", 1)] or held > KERNEL_BYTES or run_cap % 16 or merged_rows % 128 or seq_rows % 128:
        return plain_per_device(*operands)
    img, spot, base, total, incoming = merger(
        patches,
        patch_counts,
        dest_rows,
        qkv_weight.transpose(1, 2, 0),
        out_weight,
        attn_gain,
        merge_gain,
        fc1_weight,
        fc1_bias,
        fc2_weight,
        fc2_bias,
        text_embeds,
        section_hidden,
    )
    return placing(text_embeds, incoming, img, spot, total, base, llm_gain)


def solution(mesh):
    in_specs = (
        P(("section", "dp"), None),
        P(("section", "dp")),
        P(("section", "dp")),
        P(None, None, "mp"),
        P("mp", None),
        P(),
        P(),
        P("mp", ("section", "dp")),
        P(("section", "dp")),
        P(("section", "dp"), "mp"),
        P("mp"),
        P(("section", "dp"), "mp"),
        P(("section", "dp"), "mp"),
        P("mp"),
    )
    out_specs = (P(("section", "dp"), "mp"), P(("section", "dp"), "mp"))
    return jax.shard_map(
        per_device, mesh=mesh, in_specs=in_specs, out_specs=out_specs, check_vma=False
    )
```

```python
import functools
import math

import jax
import jax.numpy as jnp
from jax import lax
from jax.experimental import pallas as pl
from jax.experimental.pallas import tpu as pltpu
from jax.sharding import PartitionSpec as P

HEAD_DIM = 80
HID = 8192


vit_eps = 1e-06
llm_eps = 1e-06


def from_behind(value, axis, steps):
    count = lax.axis_size(axis)
    first, last = (max(0, -steps), min(count, count - steps))
    return lax.ppermute(value, axis, [(source, source + steps) for source in range(first, last)])


def layer_norm(values, gain):
    centred = values.astype(jnp.float32)
    centred = centred - jnp.mean(centred, axis=-1, keepdims=True)
    variance = jnp.mean(centred * centred, axis=-1, keepdims=True)
    return centred * lax.rsqrt(variance + vit_eps) * gain.astype(jnp.float32)


VMEM_LIMIT = 60 * 1024 * 1024
KERNEL_BYTES = 8 * 1024 * 1024


def vmem_call(kernel, out, scratch, sent_bytes, ident, *operands):
    return pl.pallas_call(
        kernel,
        out_shape=out,
        in_specs=[pl.BlockSpec(memory_space=pltpu.VMEM)] * len(operands),
        out_specs=pl.BlockSpec(memory_space=pltpu.VMEM),
        scratch_shapes=scratch,
        cost_estimate=pl.CostEstimate(
            flops=sent_bytes * 20000, bytes_accessed=sent_bytes * 2, transcendentals=0
        ),
        compiler_params=pltpu.CompilerParams(
            collective_id=ident, has_side_effects=True, vmem_limit_bytes=VMEM_LIMIT
        ),
    )(*operands)


def exchange_kernel(count, spread, x_ref, o_ref, send_sem, recv_sem, own_sem):
    me = lax.axis_index("mp")
    barrier = pltpu.get_barrier_semaphore()
    for step in range(1, count):
        peer = lax.rem(me + step, count)
        pl.semaphore_signal(
            barrier, inc=1, device_id={"mp": peer}, device_id_type=pl.DeviceIdType.MESH
        )
    pl.semaphore_wait(barrier, count - 1)
    copies = []
    for step in sorted(range(1, count), key=lambda s: -min(s, count - s)):
        peer = lax.rem(me + step, count)
        copy = pltpu.make_async_remote_copy(
            src_ref=x_ref.at[peer] if spread else x_ref,
            dst_ref=o_ref.at[me],
            send_sem=send_sem.at[step - 1],
            recv_sem=recv_sem.at[step - 1],
            device_id={"mp": peer},
            device_id_type=pl.DeviceIdType.MESH,
        )
        copy.start()
        copies.append(copy)
    own = pltpu.make_async_copy(x_ref.at[me] if spread else x_ref, o_ref.at[me], own_sem)
    own.start()
    own.wait()
    for copy in copies:
        copy.wait()


def relay_kernel(count, x_ref, o_ref, send_sem, recv_sem, own_sem):
    me = lax.axis_index("mp")
    barrier = pltpu.get_barrier_semaphore()
    for step in range(1, count):
        peer = lax.rem(me + step, count)
        pl.semaphore_signal(
            barrier, inc=1, device_id={"mp": peer}, device_id_type=pl.DeviceIdType.MESH
        )
    pl.semaphore_wait(barrier, count - 1)
    own = pltpu.make_async_copy(x_ref, o_ref.at[me], own_sem)
    own.start()

    def hop(way, step):
        owner = lax.rem(me - way * step + count, count)
        return pltpu.make_async_remote_copy(
            src_ref=o_ref.at[owner] if step else x_ref,
            dst_ref=o_ref.at[owner],
            send_sem=send_sem.at[(way + 1) // 2, step],
            recv_sem=recv_sem.at[(way + 1) // 2, step],
            device_id={"mp": lax.rem(me + way + count, count)},
            device_id_type=pl.DeviceIdType.MESH,
        )

    def holds(way, step):
        return me >= step if way > 0 else me + step < count

    def sends(way):
        return me < count - 1 if way > 0 else me > 0

    for step in range(count):
        for way in (1, -1):
            if step:

                @pl.when(holds(way, step))
                def _():
                    owner = lax.rem(me - way * step + count, count)
                    pltpu.make_async_remote_copy(
                        src_ref=x_ref,
                        dst_ref=o_ref.at[owner],
                        send_sem=send_sem.at[(way + 1) // 2, step - 1],
                        recv_sem=recv_sem.at[(way + 1) // 2, step - 1],
                        device_id={"mp": lax.rem(me - way + count, count)},
                        device_id_type=pl.DeviceIdType.MESH,
                    ).wait_recv()

            if step < count - 1:

                @pl.when(jnp.logical_and(holds(way, step), sends(way)))
                def _():
                    hop(way, step).start()

    own.wait()
    for step in range(count - 1):
        for way in (1, -1):

            @pl.when(jnp.logical_and(holds(way, step), sends(way)))
            def _():
                hop(way, step).wait_send()


def relay_mp(value, ident):
    count = lax.axis_size("mp")
    return vmem_call(
        functools.partial(relay_kernel, count),
        jax.ShapeDtypeStruct((count,) + value.shape, value.dtype),
        [
            pltpu.SemaphoreType.DMA((2, count - 1)),
            pltpu.SemaphoreType.DMA((2, count - 1)),
            pltpu.SemaphoreType.DMA,
        ],
        count * value.size * value.dtype.itemsize,
        ident,
        value,
    )


def exchange_mp(value, spread, ident):
    count = lax.axis_size("mp")
    shape = value.shape if spread else (count,) + value.shape
    size = math.prod(shape) * value.dtype.itemsize
    return vmem_call(
        functools.partial(exchange_kernel, count, spread),
        jax.ShapeDtypeStruct(shape, value.dtype),
        [
            pltpu.SemaphoreType.DMA((count - 1,)),
            pltpu.SemaphoreType.DMA((count - 1,)),
            pltpu.SemaphoreType.DMA,
        ],
        size,
        ident,
        value,
    )


def sum_scatter_mp(blocks, ident):
    return jnp.sum(exchange_mp(blocks, True, ident).astype(jnp.float32), axis=0)


def gather_mp(value):
    got = relay_mp(value, 2)
    return got.reshape((-1,) + value.shape[1:])


def total_mp(value):
    return jnp.sum(exchange_mp(value.reshape(-1, 128), False, 3), axis=0).reshape(-1)


def flip(index, bit):
    return index + bit * (1 - 2 * (index // bit % 2))


def group_bits():
    outer = [("dp", 1 << k) for k in range(1, lax.axis_size("dp").bit_length() - 1)]
    outer += [("section", 1 << k) for k in range(lax.axis_size("section").bit_length() - 1)]
    return outer, ("dp", 1)


def meets(axis, bit):
    return {axis: flip(lax.axis_index(axis), bit)}


def group_at(mask):
    spots = {axis: lax.axis_index(axis) for axis in ("section", "dp")}
    for axis, bit in mask:
        spots[axis] = flip(spots[axis], bit)
    return spots["section"] * lax.axis_size("dp") + spots["dp"]


def greet(bits):
    barrier = pltpu.get_barrier_semaphore()
    for axis, bit in bits:
        pl.semaphore_signal(
            barrier, inc=1, device_id=meets(axis, bit), device_id_type=pl.DeviceIdType.MESH
        )
    pl.semaphore_wait(barrier, len(bits))


def gather_kernel(x_ref, o_ref, send_sem, recv_sem, own_sem):
    outer, last = group_bits()
    greet(outer + [last])
    half = x_ref.shape[1] // 2
    sent, waiting = [], []
    slots = iter(range(send_sem.shape[0]))

    def pass_on(mask, stage, part, order):
        cols = pl.ds(part * half, half)
        spot = group_at(mask)
        source = o_ref.at[spot, :, cols] if mask else x_ref.at[:, cols]
        for later in range(stage, len(order)):
            slot = next(slots)
            copy = pltpu.make_async_remote_copy(
                src_ref=source,
                dst_ref=o_ref.at[spot, :, cols],
                send_sem=send_sem.at[slot],
                recv_sem=recv_sem.at[slot],
                device_id=meets(*order[later]),
                device_id_type=pl.DeviceIdType.MESH,
            )
            copy.start()
            sent.append(copy)
            waiting.append((later, copy, mask + [order[later]], part, order))

    pass_on([], 0, 0, outer + [last])
    pass_on([], 0, 1, outer[::-1] + [last])
    own = pltpu.make_async_copy(x_ref, o_ref.at[group_at([])], own_sem)
    own.start()
    while waiting:
        first = min(range(len(waiting)), key=lambda at: waiting[at][0])
        stage, copy, mask, part, order = waiting.pop(first)
        copy.wait_recv()
        pass_on(mask, stage + 1, part, order)
    for copy in sent:
        copy.wait_send()
    own.wait()


def gather_groups(value):
    count = lax.axis_size("section") * lax.axis_size("dp")
    size = count * value.size * value.dtype.itemsize
    if size > KERNEL_BYTES:
        return lax.all_gather(value, ("section", "dp"), axis=0, tiled=True)
    slots = 2 * (count - 1)
    got = vmem_call(
        gather_kernel,
        jax.ShapeDtypeStruct((count,) + value.shape, value.dtype),
        [
            pltpu.SemaphoreType.DMA((slots,)),
            pltpu.SemaphoreType.DMA((slots,)),
            pltpu.SemaphoreType.DMA,
        ],
        size,
        4,
        value,
    )
    return got.reshape(-1, value.shape[1])


def scatter_kernel(x_ref, o_ref, held, taken, send_sem, recv_sem):
    outer, first = group_bits()
    greet(outer + [first])
    rows = x_ref.shape[1]
    half = x_ref.shape[2] // 2
    chunk = 32
    orders = ([first] + outer, [first] + outer[::-1])
    slots = iter(range(send_sem.shape[0]))
    masks = [[]]
    for bit in outer:
        masks = masks + [mask + [bit] for mask in masks]
    place_of = {frozenset(mask): at for at, mask in enumerate(masks)}
    base = len(masks)
    live = {}

    def send(part, stage):
        cols = pl.ds(part * half, half)
        bit = orders[part][stage]
        kept = orders[part][stage + 1 :]
        copies = []
        for mask in [m for m in masks if set(m) <= set(kept)]:
            if stage == 0:
                source = x_ref.at[group_at(mask + [bit]), :, cols]
            else:
                source = held.at[place_of[frozenset(mask + [bit])], :, cols]
            landing = 2 * base - 2 ** (len(kept) + 1) + [
                m for m in masks if set(m) <= set(kept)
            ].index(mask)
            slot = next(slots)
            copy = pltpu.make_async_remote_copy(
                src_ref=source,
                dst_ref=taken.at[landing, :, cols],
                send_sem=send_sem.at[slot],
                recv_sem=recv_sem.at[slot],
                device_id=meets(*bit),
                device_id_type=pl.DeviceIdType.MESH,
            )
            copy.start()
            copies.append((copy, mask, landing))
        live[part, stage] = copies

    def add(part, stage):
        cols = pl.ds(part * half, half)
        final = stage + 1 == len(orders[part])
        following = None if final else orders[part][stage + 1]
        copies = live[part, stage]
        for copy, mask, landing in sorted(copies, key=lambda c: following not in c[1]):
            copy.wait_recv()
            at = place_of[frozenset(mask)]
            spot = group_at(mask)

            @pl.loop(0, rows // chunk)
            def _(step):
                span = pl.ds(step * chunk, chunk)
                mine = x_ref[spot, span, cols] if stage == 0 else held[at, span, cols]
                total = mine.astype(jnp.float32) + taken[landing, span, cols].astype(jnp.float32)
                if final:
                    o_ref[span, cols] = total
                else:
                    held[at, span, cols] = total.astype(held.dtype)

    send(0, 0)
    send(1, 0)
    for stage in range(len(orders[0])):
        for part in (0, 1):
            add(part, stage)
            if stage + 1 < len(orders[0]):
                send(part, stage + 1)
    for copies in live.values():
        for copy, _, _ in copies:
            copy.wait_send()


def sum_scatter_groups(value):
    count = lax.axis_size("section") * lax.axis_size("dp")
    size = value.size * value.dtype.itemsize
    if size > KERNEL_BYTES:
        return lax.psum_scatter(value, ("section", "dp"), scatter_dimension=0, tiled=True)
    rows, cols = value.shape[0] // count, value.shape[1]
    slots = 2 * (count - 1)
    return vmem_call(
        scatter_kernel,
        jax.ShapeDtypeStruct((rows, cols), jnp.float32),
        [
            pltpu.VMEM((count // 2, rows, cols), value.dtype),
            pltpu.VMEM((count - 1, rows, cols), value.dtype),
            pltpu.SemaphoreType.DMA((slots,)),
            pltpu.SemaphoreType.DMA((slots,)),
        ],
        size,
        5,
        value.reshape(count, rows, cols),
    )


def plain_per_device(
    patches,
    patch_counts,
    dest_rows,
    qkv_weight,
    out_weight,
    attn_gain,
    merge_gain,
    fc1_weight,
    fc1_bias,
    fc2_weight,
    fc2_bias,
    text_embeds,
    section_hidden,
    llm_gain,
):
    width = patches.shape[1]
    tile_total = patch_counts.shape[0]
    block_rows = patches.shape[0] // tile_total
    merged_rows = patches.shape[0] // 4
    local_cols = qkv_weight.shape[2]
    local_heads = local_cols // HEAD_DIM
    feature_cols = text_embeds.shape[1]
    seq_rows = text_embeds.shape[0]
    section_count = lax.axis_size("section")
    group_count = section_count * lax.axis_size("dp")
    run_cap = max(2, merged_rows // group_count)
    run_total = merged_rows // run_cap
    run_target = dest_rows.reshape(run_total, run_cap)[:, 0] // seq_rows
    takes = jnp.arange(group_count, dtype=jnp.int32)[:, None] == run_target[None, :]
    slot_in_tile = jnp.arange(merged_rows, dtype=jnp.int32) % (block_rows // 4)
    tile_counts = jnp.repeat(patch_counts, block_rows // 4, total_repeat_length=merged_rows)
    live = slot_in_tile * 4 < tile_counts
    place = jnp.where(live, dest_rows % seq_rows - seq_rows, 0).reshape(run_total, run_cap)
    send_place = jnp.sum(jnp.where(takes[:, :, None], place[None], 0), axis=1) + seq_rows
    got_place = lax.all_to_all(send_place, ("section", "dp"), split_axis=0, concat_axis=0, tiled=True)
    incoming = from_behind(section_hidden, "section", 1)
    normed_in = layer_norm(patches, attn_gain).astype(jnp.bfloat16)
    projections = jnp.dot(
        normed_in, qkv_weight.reshape(width, 3 * local_cols), preferred_element_type=jnp.float32
    ).astype(jnp.bfloat16)
    projections = projections.reshape(tile_total, block_rows, 3, local_heads, HEAD_DIM)
    query_part = projections[:, :, 0]
    key_part = projections[:, :, 1]
    value_part = projections[:, :, 2]
    scores = jnp.einsum(
        "tqhd,tkhd->thqk", query_part, key_part, preferred_element_type=jnp.float32
    ) * HEAD_DIM ** (-0.5)
    key_live = (
        jnp.arange(block_rows, dtype=jnp.int32)[None, None, None, :]
        < patch_counts[:, None, None, None]
    )
    scores = jnp.where(key_live, scores, -1e30)
    weights = jax.nn.softmax(scores, axis=-1).astype(jnp.bfloat16)
    attended = jnp.einsum(
        "thqk,tkhd->tqhd", weights, value_part, preferred_element_type=jnp.float32
    ).astype(jnp.bfloat16)
    attended = attended.reshape(patches.shape[0], local_cols)
    lane_source = jnp.arange(run_total, dtype=jnp.int32)[None, :] * run_cap
    run_source = jnp.sum(jnp.where(takes, lane_source, 0), axis=1)
    row_source = (
        run_source[:, None] + jnp.arange(run_cap, dtype=jnp.int32)[None, :]
    ).reshape(-1) * 4
    slots_at = jnp.arange(patches.shape[0], dtype=jnp.int32)
    patch_at = jnp.arange(4, dtype=jnp.int32)
    order = (
        (row_source[None, :] + patch_at[:, None]).reshape(-1)[:, None] == slots_at[None, :]
    ).astype(jnp.bfloat16)
    own_order = (
        (row_source + lax.axis_index("mp"))[:, None] == slots_at[None, :]
    ).astype(jnp.bfloat16)
    ordered = jnp.dot(order, attended, preferred_element_type=jnp.float32).astype(jnp.bfloat16)
    own_patch = jnp.dot(own_order, patches, preferred_element_type=jnp.float32)
    partial_proj = jnp.dot(ordered, out_weight, preferred_element_type=jnp.float32)
    own_proj = sum_scatter_mp(
        partial_proj.astype(jnp.bfloat16).reshape(4, group_count * run_cap, width), 0
    )
    block_out = (own_patch + own_proj).astype(jnp.bfloat16)
    merge_part = layer_norm(block_out, merge_gain).astype(jnp.bfloat16)
    slot_rows = group_count * run_cap
    gathered = gather_groups(merge_part)
    gathered = (
        gathered.reshape(group_count, group_count, run_cap, width)
        .transpose(1, 0, 2, 3)
        .reshape(group_count * slot_rows, width)
    )
    first_partial = jnp.dot(gathered, fc1_weight, preferred_element_type=jnp.float32)
    mp_count = lax.axis_size("mp")
    first_total = sum_scatter_mp(
        first_partial.astype(jnp.bfloat16).reshape(mp_count, -1, fc1_weight.shape[1]),
        1,
    )
    hidden_part = jax.nn.gelu(
        first_total + fc1_bias.astype(jnp.float32), approximate=False
    ).astype(jnp.bfloat16)
    hidden = gather_mp(hidden_part)
    second_partial = jnp.dot(hidden, fc2_weight, preferred_element_type=jnp.float32)
    embed_total = sum_scatter_groups(second_partial.astype(jnp.bfloat16)).astype(jnp.float32)
    image_embeds = (embed_total + fc2_bias.astype(jnp.float32)).astype(jnp.bfloat16)
    hits = got_place.reshape(1, -1) == jnp.arange(seq_rows, dtype=jnp.int32)[:, None]
    placed = jnp.dot(
        hits.astype(jnp.bfloat16), image_embeds, preferred_element_type=jnp.float32
    ).astype(jnp.bfloat16)
    sequence_embeds = jnp.where(jnp.any(hits, axis=1)[:, None], placed, text_embeds)
    entering = jnp.where(lax.axis_index("section") == 0, sequence_embeds, incoming).astype(
        jnp.float32
    )
    row_total = total_mp(jnp.sum(entering * entering, axis=1))
    layer_inputs = (
        entering * lax.rsqrt(row_total / HID + llm_eps)[:, None] * llm_gain.astype(jnp.float32)
    ).astype(jnp.bfloat16)
    return (sequence_embeds, layer_inputs)


LAG = 2
FC2_COLS = 1024
HALF_ROOT = 0.5**0.5


def remote(src, dst, send_sem, recv_sem, device):
    return pltpu.make_async_remote_copy(
        src_ref=src,
        dst_ref=dst,
        send_sem=send_sem,
        recv_sem=recv_sem,
        device_id=device,
        device_id_type=pl.DeviceIdType.MESH,
    )


def group_device(group):
    per_section = lax.axis_size("dp")
    return {"section": group // per_section, "dp": lax.rem(group, per_section)}


def tell(device):
    pl.semaphore_signal(
        pltpu.get_barrier_semaphore(),
        inc=1,
        device_id=device,
        device_id_type=pl.DeviceIdType.MESH,
    )


def merger_kernel(
    patches_hbm,
    counts_ref,
    dest_ref,
    qkv_hbm,
    wo_hbm,
    attn_gain_ref,
    merge_gain_ref,
    w1_hbm,
    b1_ref,
    w2_hbm,
    b2_ref,
    text_hbm,
    carry_hbm,
    img_ref,
    spot_ref,
    base_ref,
    total_ref,
    incoming_hbm,
    patches_ref,
    qkv_ref,
    wo_ref,
    text_ref,
    carry_ref,
    text_squares,
    carry_squares,
    carry_sem,
    carry_send,
    carry_recv,
    normed,
    place_ref,
    sums_ref,
    query,
    key,
    value_part,
    attended,
    ordered,
    arrived,
    wo_all,
    x_ref,
    w1_ref,
    w2_ref,
    weight_sem,
    wo_send,
    wo_recv,
    wo_out,
    wo_plane,
    wo_pair,
    a_send,
    a_recv,
    rows,
    part,
    before,
    after,
    right_out,
    left_out,
    hidden,
    give,
    take,
    keep,
    x_out,
    x_in,
    y_out,
    y_in,
    squares,
    spots,
    sums,
    base_out,
    base_in,
    totals,
    row_send,
    row_recv,
    pair_recv,
    right_send,
    right_recv,
    left_send,
    left_recv,
    give_send,
    give_recv,
    x_send,
    x_recv,
    y_send,
    y_recv,
    spot_send,
    spot_recv,
    sum_send,
    sum_recv,
    base_send,
    base_recv,
    total_send,
    total_recv,
):
    groups = lax.axis_size("section") * lax.axis_size("dp")
    sections = lax.axis_size("section")
    line = lax.axis_size("mp")
    me = lax.axis_index("mp")
    section = lax.axis_index("section")
    dp = lax.axis_index("dp")
    core = lax.rem(dp, 2)
    column = dp // 2
    wide = lax.axis_size("dp") // 2
    group = section * lax.axis_size("dp") + dp
    chips = groups // 2
    pair = {"dp": flip(dp, 1)}
    over_x = {"dp": flip(dp, 2)}
    over_y = {"section": flip(section, 1)}
    quarters = 4
    pieces = chips * quarters
    take_rows = rows.shape[2] // 2
    lag_right = me * LAG
    half_rows = part.shape[3]
    split_from = 3
    single = 8
    run = half_rows // 2
    lag_left = (line - 1 - me) * LAG
    lag_total = (line - 1) * LAG

    fetches = [
        pltpu.make_async_copy(source, target, weight_sem.at[at])
        for at, (source, target) in enumerate(
            (
                (wo_hbm, wo_ref),
                (patches_hbm, patches_ref),
                (qkv_hbm, qkv_ref),
                (w1_hbm, w1_ref),
                (w2_hbm, w2_ref),
            )
        )
    ]
    for fetch in fetches:
        fetch.start()
    for step in range(1, groups):
        tell(group_device(lax.rem(group + step, groups)))
    for step in range(1, line):
        tell({"mp": lax.rem(me + step, line)})
    pl.semaphore_wait(pltpu.get_barrier_semaphore(), groups + line - 2)

    def chip_of(quarter):
        there_x = lax.rem(quarter // 2 + column, 2)
        there_y = lax.rem(lax.rem(quarter, 2) + section, 2)
        return there_y * wide + there_x

    def group_of(quarter, at_core):
        return chip_of(quarter) * 2 + at_core

    def own_send(chunk, which):
        sem = (row_recv.at[chunk, 1], row_recv.at[chunk, 2], pair_recv.at[chunk, 0])[which]
        device = (over_y, over_x, pair)[which]
        return remote(x_ref.at[chunk], rows.at[group, chunk], row_send.at[chunk, which], sem, device)

    def forward_x(chunk):
        spot = rows.at[group_of(1, core), chunk]
        return remote(spot, spot, row_send.at[chunk, 3], row_recv.at[chunk, 3], over_x)

    def forward_pair(chunk, quarter):
        spot = rows.at[group_of(quarter, core), chunk]
        return remote(
            spot, spot, row_send.at[chunk, 3 + quarter], pair_recv.at[chunk, quarter], pair
        )

    leads = section < sections - 1
    bands = carry_send.shape[0]
    band_rows = carry_hbm.shape[0] // bands
    text_fetch = pltpu.make_async_copy(text_hbm, text_ref, carry_sem.at[0])
    carry_fetch = pltpu.make_async_copy(carry_hbm, carry_ref, carry_sem.at[1])

    @pl.when(leads)
    def _():
        text_fetch.start()
        carry_fetch.start()

    def send_band(at):
        cut = pl.ds(pl.multiple_of(at * band_rows, band_rows), band_rows)
        return remote(
            carry_hbm.at[cut], incoming_hbm.at[cut], carry_send.at[at], carry_recv.at[at], {"section": section + 1}
        )

    def send_bands(first, last):
        @pl.when(leads)
        def _():
            for at in range(first, last):
                send_band(at).start()

    early = bands // 10
    looped = bands - early - bands // 6

    def wo_slice(ref, holder):
        high = wo_ref.shape[0] // lax.axis_size("dp")
        broad = wo_ref.shape[1] // sections
        top = pl.multiple_of(lax.rem(holder, lax.axis_size("dp")) * high, high)
        left = pl.multiple_of(holder // lax.axis_size("dp") * broad, broad)
        return ref.at[pl.ds(top, high), pl.ds(left, broad)]

    def wo_line(step):
        return remote(
            wo_slice(wo_ref, group),
            wo_slice(wo_all.at[me], group),
            wo_send.at[step - 1],
            wo_recv.at[step - 1],
            {"mp": lax.rem(me + step, line)},
        )

    def wo_hop(step, quarter, at, sem, device):
        block = wo_slice(wo_all.at[lax.rem(me - step + line, line)], group_of(quarter, core))
        return remote(block, block, wo_out.at[step - 1, at], sem, device)

    def wo_starts(step):
        return (
            wo_hop(step, 0, 0, wo_plane.at[step - 1, 1], over_y),
            wo_hop(step, 0, 1, wo_plane.at[step - 1, 2], over_x),
            wo_hop(step, 0, 2, wo_pair.at[step - 1, 0], pair),
        )

    def wo_forward_x(step):
        return wo_hop(step, 1, 3, wo_plane.at[step - 1, 3], over_x)

    def wo_forward_pair(step, quarter):
        return wo_hop(step, quarter, 3 + quarter, wo_pair.at[step - 1, quarter], pair)

    def wo_landed(step, quarter):
        return wo_hop(step, quarter, 0, wo_plane.at[step - 1, quarter], over_x)

    def wo_paired(step, quarter):
        block = wo_slice(wo_all.at[lax.rem(me - step + line, line)], group_of(quarter, 1 - core))
        return remote(block, block, wo_out.at[step - 1, 0], wo_pair.at[step - 1, quarter], pair)

    steps = range(1, line)
    low_end, high_end = me == 0, me == line - 1
    at_end = jnp.logical_or(low_end, high_end)
    first_sent = jnp.where(high_end, 3, 1)
    second = jnp.where(at_end, 2, 3)
    last_sent = jnp.where(low_end, 3, jnp.where(high_end, 1, 2))
    first_here = jnp.where(low_end, 3, 1)
    last_here = jnp.where(low_end, 1, jnp.where(high_end, 3, 2))
    fetches[0].wait()
    for step in (first_sent, second, last_sent):
        wo_line(step).start()

    send_bands(0, early)
    slots = ordered.shape[1]
    dest = dest_ref[...].reshape(1, slots)
    slot = lax.broadcasted_iota(jnp.int32, (1, slots), 1)
    tiles = counts_ref.shape[0]
    slice_rows = carry_hbm.shape[0]
    target = dest // slice_rows
    slot_place = slot
    for stride in [1 << bit for bit in range(run.bit_length() - 1, slots.bit_length())][::-1]:
        slot_place = jnp.where(slot_place >= stride, slot_place - stride, slot_place)
    slot_target = target * run + slot_place
    filled = jnp.zeros((1, slots), jnp.int32)
    for tile in range(tiles):
        start = tile * (slots // tiles)
        within = jnp.logical_and(slot >= start, slot - start < slots // tiles)
        filled = jnp.where(jnp.logical_and(within, (slot - start) * 4 < counts_ref[tile]), 1, filled)
    spot = jnp.where(filled > 0, dest - target * slice_rows, slice_rows)
    high = (spot // 16).astype(jnp.float32)
    low = (spot - spot // 16 * 16).astype(jnp.float32)
    to_group = lax.broadcasted_iota(jnp.int32, (groups, slots), 0) == target
    at_source = lax.broadcasted_iota(jnp.int32, (slots, slots), 1)
    moved = (at_source == group * run + slot_place.reshape(slots, 1)).astype(jnp.float32).astype(jnp.bfloat16)

    def moved_to(value):
        picked = jnp.where(to_group, value, 0.0).astype(jnp.bfloat16)
        return jnp.dot(picked, moved, preferred_element_type=jnp.float32)

    place_rows = (moved_to(high) * 16.0 + moved_to(low)).astype(jnp.int32)
    place_ref[...] = place_rows.reshape(place_ref.shape)
    place_copies = []
    for step in range(1, groups):
        peer = lax.rem(group + step, groups)
        copy = remote(
            place_ref.at[peer], spots.at[step], spot_send.at[step - 1], spot_recv.at[step - 1], group_device(peer)
        )
        copy.start()
        place_copies.append(copy)
    spots[0] = place_ref[group]

    tall = min(patches_ref.shape[0], 128)
    fetches[1].wait()

    @pl.loop(0, patches_ref.shape[0] // tall)
    def _(at):
        cut = pl.ds(at * tall, tall)
        normed[cut] = layer_norm(
            patches_ref[cut], attn_gain_ref[...].reshape(1, -1)
        ).astype(normed.dtype)

    fetches[2].wait()
    for which, ref in enumerate((query, key, value_part)):
        ref[...] = lax.dot_general(
            normed[...], qkv_ref[which], (((1,), (1,)), ((), ())), preferred_element_type=jnp.float32
        ).astype(ref.dtype)

    def begin(step):
        wo_line(step).wait_recv()
        for copy in wo_starts(step):
            copy.start()

    def pass_y(step):
        wo_landed(step, 1).wait_recv()
        wo_forward_x(step).start()
        wo_forward_pair(step, 1).start()

    def pass_x(step, quarter):
        wo_landed(step, quarter).wait_recv()
        wo_forward_pair(step, quarter).start()

    begin(first_here)
    wo_all[me] = wo_ref[...]

    block = query.shape[0] // tiles
    lane = lax.broadcasted_iota(jnp.int32, (1, query.shape[1]), 1)
    at_key = lax.broadcasted_iota(jnp.int32, (block, block), 1)

    def attend(tile):
        cut = pl.ds(tile * block, block)
        tile_query, tile_key, tile_value = query[cut], key[cut], value_part[cut]
        live = at_key < counts_ref[tile]
        result = jnp.zeros((block, query.shape[1]), jnp.float32)
        for head in range(query.shape[1] // HEAD_DIM):
            own = jnp.logical_and(lane >= head * HEAD_DIM, lane < (head + 1) * HEAD_DIM)
            own = own.astype(jnp.float32).astype(jnp.bfloat16)
            scores = lax.dot_general(
                tile_query * own, tile_key, (((1,), (1,)), ((), ())), preferred_element_type=jnp.float32
            )
            scores = jnp.where(live, scores * HEAD_DIM**-0.5, -1e30)
            power = jnp.exp(scores - jnp.max(scores, axis=1, keepdims=True))
            weights = (power / jnp.sum(power, axis=1, keepdims=True)).astype(jnp.bfloat16)
            result = result + jnp.dot(weights, tile_value * own, preferred_element_type=jnp.float32)
        attended[cut] = result.astype(attended.dtype)

    tile_slots = slots // tiles

    def pick(height, width, patch):
        at_row = lax.broadcasted_iota(jnp.int32, (height, width), 0)
        at_patch = lax.broadcasted_iota(jnp.int32, (height, width), 1)
        return (at_patch == at_row * line + patch).astype(jnp.float32).astype(jnp.bfloat16)

    def exchange(step, tile):
        peer = lax.rem(me + step, line)
        cut = pl.ds(tile * tile_slots, tile_slots)
        return remote(
            ordered.at[peer, cut], arrived.at[me, cut], a_send.at[step - 1, tile], a_recv.at[step - 1, tile], {"mp": peer}
        )

    def spread(tile):
        source = attended[pl.ds(tile * block, block)]
        for patch in range(line):
            ordered[patch, pl.ds(tile * tile_slots, tile_slots)] = jnp.dot(
                pick(tile_slots, block, patch), source, preferred_element_type=jnp.float32
            ).astype(ordered.dtype)
        for step in (first_sent, second, last_sent):
            exchange(step, tile).start()

    for tile in range(tiles):
        attend(tile)
        spread(tile)
        if tile == 0:
            begin(second)
    begin(last_here)
    pass_y(first_here)
    send_bands(early, bands - looped)
    arrived[me] = ordered[me]
    order = (
        lax.broadcasted_iota(jnp.int32, (slots, slots), 0) == slot_target
    ).astype(jnp.float32).astype(jnp.bfloat16)
    block_out = jnp.dot(
        pick(slots, patches_ref.shape[0], me), patches_ref[...], preferred_element_type=jnp.float32
    )
    pass_y(second)
    pass_x(first_here, 2)
    pass_y(last_here)
    pass_x(second, 2)
    pass_x(first_here, 3)
    pass_x(last_here, 2)
    pass_x(second, 3)
    pass_x(last_here, 3)
    for step in steps:
        for quarter in range(quarters):
            wo_paired(step, quarter).wait_recv()
    for step in steps:
        for tile in range(tiles):
            exchange(step, tile).wait_recv()
    for source in range(line):
        block_out = block_out + jnp.dot(
            arrived[source], wo_all[source], preferred_element_type=jnp.float32
        )
    block_out = block_out.astype(jnp.bfloat16)
    merged = layer_norm(block_out, merge_gain_ref[...].reshape(1, -1)).astype(x_ref.dtype)
    x_ref[...] = (
        jnp.dot(order, merged, preferred_element_type=jnp.float32).astype(x_ref.dtype).reshape(x_ref.shape)
    )
    for chunk in range(chips):
        own_send(chunk, 0).start()
    for which in (1, 2):
        own_send(0, which).start()
    rows[group] = x_ref[...]
    for fetch in fetches[3:]:
        fetch.wait()

    def send_right(piece):
        return remote(
            right_out.at[piece], before.at[piece], right_send.at[piece], right_recv.at[piece], {"mp": me + 1}
        )

    def send_left(piece):
        return remote(
            left_out.at[piece], after.at[piece], left_send.at[piece], left_recv.at[piece], {"mp": me - 1}
        )

    def send_give(chunk):
        return remote(give.at[chunk], take.at[chunk], give_send.at[chunk], give_recv.at[chunk], pair)

    parts = x_send.shape[1]
    span = keep.shape[1] // parts

    def send_x(chunk, at):
        cut = pl.ds(at * span, span)
        return remote(
            x_out.at[chunk, cut], x_in.at[chunk, cut], x_send.at[chunk, at], x_recv.at[chunk, at], over_x
        )

    def send_y(at):
        cut = pl.ds(at * span, span)
        return remote(y_out.at[cut], y_in.at[cut], y_send.at[at], y_recv.at[at], over_y)

    def settle(chunk):
        send_give(chunk).wait_recv()
        mine = lax.rem(chunk, wide) == column

        @pl.when(mine)
        def _():
            @pl.loop(0, parts)
            def _(at):
                cut = pl.ds(at * span, span)
                keep[chunk, cut] = keep[chunk, cut] + take[chunk, cut].astype(jnp.float32)

        @pl.when(jnp.logical_not(mine))
        def _():
            @pl.loop(0, parts)
            def _(at):
                cut = pl.ds(at * span, span)
                x_out[chunk, cut] = (
                    keep[chunk, cut] + take[chunk, cut].astype(jnp.float32)
                ).astype(x_out.dtype)
                send_x(chunk, at).start()

    sum_rows = base_out.shape[0]

    def folded(value):
        value = value.astype(jnp.float32)
        square = value * value
        width = squares.shape[1]
        total = square[:, :width]
        for at_col in range(1, square.shape[1] // width):
            total = total + square[:, at_col * width : (at_col + 1) * width]
        return total

    def exchange_sums(step):
        return remote(
            sums_ref, sums.at[step], sum_send.at[step - 1], sum_recv.at[step - 1], {"mp": lax.rem(me + step, line)}
        )

    send_base = remote(base_out, base_in, base_send, base_recv, {"section": section + 1})
    share = text_ref.shape[0] // pieces

    def stage(i, carry):
        for extra in range(2):
            band = bands - looped + (i - quarters) * 2 + extra

            @pl.when(jnp.logical_and(leads, jnp.logical_and(i >= quarters, band < bands)))
            def _():
                send_band(band).start()

        @pl.when(jnp.logical_and(leads, i < pieces))
        def _():
            @pl.when(i == 0)
            def _():
                text_fetch.wait()
                carry_fetch.wait()

            cut = pl.ds(pl.multiple_of(i * share, share), share)
            text_squares[cut] = folded(text_ref[cut])
            carry_squares[cut] = folded(carry_ref[cut])

        @pl.when(jnp.logical_and(leads, i == pieces))
        def _():
            for which, ref in enumerate((text_squares, carry_squares)):
                for at in range(sum_rows):
                    cut = pl.ds(at * 128, 128)
                    at_sum = which * sum_rows + at
                    sums_ref[at_sum : at_sum + 1] = jnp.sum(ref[cut].T, axis=0, keepdims=True)
            for step in steps:
                exchange_sums(step).start()

        @pl.when(jnp.logical_and(leads, i == pieces + 4))
        def _():
            both = sums_ref[...]
            for step in steps:
                exchange_sums(step).wait()
                both = both + sums[step]
            base_out[...] = both[sum_rows:]
            base_ref[...] = both[:sum_rows]
            send_base.start()

        def relay(piece):
            chunk = piece // quarters
            quarter = lax.rem(piece, quarters)

            @pl.when(quarter == 1)
            def _():
                remote(
                    x_ref.at[chunk], rows.at[group_of(1, core), chunk], row_send.at[chunk, 0], row_recv.at[chunk, 1], over_y
                ).wait_recv()
                forward_x(chunk).start()
                forward_pair(chunk, 1).start()

                @pl.when(chunk + 1 < chips)
                def _():
                    for which in (1, 2):
                        own_send(chunk + 1, which).start()

            @pl.when(quarter > 1)
            def _():
                remote(
                    x_ref.at[chunk], rows.at[group_of(quarter, core), chunk], row_send.at[chunk, 1], row_recv.at[chunk, quarter], over_x
                ).wait_recv()
                forward_pair(chunk, quarter).start()

        def multiply(piece):
            chunk = piece // quarters
            quarter = lax.rem(piece, quarters)
            spot = rows.at[group_of(quarter, 1 - core), chunk]
            remote(x_ref.at[chunk], spot, row_send.at[chunk, 2], pair_recv.at[chunk, quarter], pair).wait_recv()
            lhs = rows[pl.ds(chip_of(quarter) * 2, 2), chunk]
            result = jnp.dot(
                lhs.reshape(-1, lhs.shape[2]), w1_ref[...], preferred_element_type=jnp.float32
            ).reshape(2, 2, run, part.shape[4])
            for target in range(2):
                part[chunk, quarter, target] = result[:, target].reshape(part.shape[3:])

        def once_then_twice(turn, work):
            @pl.when(jnp.logical_and(turn >= 0, turn < single))
            def _():
                work(turn)

            @pl.when(jnp.logical_and(turn >= single, turn < (pieces + single) // 2))
            def _():
                work(turn * 2 - single)
                work(turn * 2 - single + 1)

        once_then_twice(i, relay)
        once_then_twice(i - 1, multiply)

        def halves(piece):
            chunk = piece // quarters
            turn = lax.rem(piece, quarters)
            first_quarter = jnp.where(chunk < split_from, turn, lax.rem(turn, 2) * 2)
            last_quarter = jnp.where(chunk < split_from, turn, lax.rem(turn, 2) * 2 + 1)
            first_target = jnp.where(chunk < split_from, 0, turn // 2)
            last_target = jnp.where(chunk < split_from, 1, turn // 2)
            low_half, high_half = pl.ds(0, half_rows), pl.ds(half_rows, half_rows)
            return (
                (low_half, (chunk, first_quarter, first_target)),
                (high_half, (chunk, last_quarter, last_target)),
            )

        at_right = i - 1 - lag_right

        @pl.when(jnp.logical_and(me < line - 1, jnp.logical_and(at_right >= 0, at_right < pieces)))
        def _():
            @pl.when(me == 0)
            def _():
                for cut, spot in halves(at_right):
                    right_out[at_right, cut] = part[spot].astype(right_out.dtype)

            @pl.when(me > 0)
            def _():
                send_right(at_right).wait_recv()
                for cut, spot in halves(at_right):
                    right_out[at_right, cut] = (
                        part[spot] + before[at_right, cut].astype(jnp.float32)
                    ).astype(right_out.dtype)

            send_right(at_right).start()

        at_left = i - 1 - lag_left

        @pl.when(jnp.logical_and(me > 0, jnp.logical_and(at_left >= 0, at_left < pieces)))
        def _():
            @pl.when(me == line - 1)
            def _():
                for cut, spot in halves(at_left):
                    left_out[at_left, cut] = part[spot].astype(left_out.dtype)

            @pl.when(me < line - 1)
            def _():
                send_left(at_left).wait_recv()
                for cut, spot in halves(at_left):
                    left_out[at_left, cut] = (
                        part[spot] + after[at_left, cut].astype(jnp.float32)
                    ).astype(left_out.dtype)

            send_left(at_left).start()

        at_total = i - 1 - lag_total

        @pl.when(at_total >= 0)
        def _():
            chunk = at_total // quarters
            turn = lax.rem(at_total, quarters)

            @pl.when(
                jnp.logical_and(
                    jnp.logical_and(turn == 0, chunk > 0), jnp.logical_or(chunk <= split_from, core == 1)
                )
            )
            def _():
                settle(chunk - 1)

            @pl.when(jnp.logical_and(jnp.logical_and(turn == 2, chunk >= split_from), core == 0))
            def _():
                settle(chunk)

            @pl.when(me == line - 1)
            def _():
                send_right(at_total).wait_recv()

            @pl.when(me == 0)
            def _():
                send_left(at_total).wait_recv()

            for cut, spot in halves(at_total):
                _, quarter, target = spot

                @pl.when(me > 0)
                def _():
                    part[spot] = part[spot] + before[at_total, cut].astype(jnp.float32)

                @pl.when(me < line - 1)
                def _():
                    part[spot] = part[spot] + after[at_total, cut].astype(jnp.float32)

                value = part[spot] + b1_ref[...].reshape(1, -1).astype(jnp.float32)
                value = 0.5 * value * (1.0 + lax.erf(value * HALF_ROOT))
                hidden[chunk, target, chip_of(quarter)] = value.astype(hidden.dtype)

            def project(target):
                lhs = hidden[chunk, target].reshape(-1, hidden.shape[4])

                @pl.loop(0, w2_ref.shape[1] // FC2_COLS)
                def _(at):
                    cols = pl.ds(pl.multiple_of(at * FC2_COLS, FC2_COLS), FC2_COLS)
                    result = jnp.dot(lhs, w2_ref[:, cols], preferred_element_type=jnp.float32)

                    @pl.when(core == target)
                    def _():
                        keep[chunk, :, cols] = result

                    @pl.when(core != target)
                    def _():
                        give[chunk, :, cols] = result.astype(give.dtype)

                @pl.when(core != target)
                def _():
                    send_give(chunk).start()

            @pl.when(jnp.logical_and(turn == 1, chunk >= split_from))
            def _():
                project(0)

            @pl.when(turn == quarters - 1)
            def _():
                @pl.when(chunk < split_from)
                def _():
                    project(0)

                project(1)

        return carry

    lax.fori_loop(0, pieces + 1 + lag_total, stage, 0)

    @pl.when(core == 1)
    def _():
        settle(chips - 1)

    spot_sum = spots[0]
    for copy in place_copies:
        copy.wait_recv()
    for step in range(1, groups):
        spot_sum = spot_sum + spots[step]
    spot_ref[...] = spot_sum

    @pl.when(section > 0)
    def _():
        send_base.wait_recv()
        base_ref[...] = base_in[...]

        @pl.loop(0, bands)
        def _(at):
            remote(
                carry_hbm.at[pl.ds(0, band_rows)], incoming_hbm.at[pl.ds(0, band_rows)], carry_send.at[at], carry_recv.at[at], over_y
            ).wait_recv()

    own_chunk = section * wide + column
    y_chunk = flip(section, 1) * wide + column

    @pl.loop(0, parts)
    def _(at):
        cut = pl.ds(at * span, span)
        send_x(y_chunk, at).wait_recv()
        y_out[cut] = (keep[y_chunk, cut] + x_in[y_chunk, cut].astype(jnp.float32)).astype(y_out.dtype)
        send_y(at).start()

    @pl.loop(0, parts)
    def _(at):
        cut = pl.ds(at * span, span)
        send_x(own_chunk, at).wait_recv()
        send_y(at).wait_recv()
        value = (
            keep[own_chunk, cut]
            + x_in[own_chunk, cut].astype(jnp.float32)
            + y_in[cut].astype(jnp.float32)
            + b2_ref[...].reshape(1, -1).astype(jnp.float32)
        ).astype(img_ref.dtype)
        img_ref[cut] = value
        squares[cut] = folded(value)

    totals[0] = jnp.sum(squares[...].T, axis=0, keepdims=True)
    total_copies = []
    for step in range(1, line):
        copy = remote(
            totals.at[0], totals.at[step], total_send.at[step - 1], total_recv.at[step - 1], {"mp": lax.rem(me + step, line)}
        )
        copy.start()
        total_copies.append(copy)

    for step in steps:
        wo_line(step).wait_send()
        for copy in wo_starts(step) + (wo_forward_x(step),):
            copy.wait_send()
        for quarter in range(1, quarters):
            wo_forward_pair(step, quarter).wait_send()
        for tile in range(tiles):
            exchange(step, tile).wait_send()

    for chunk in range(chips):
        for which in range(3):
            own_send(chunk, which).wait_send()
        forward_x(chunk).wait_send()
        for quarter in range(1, quarters):
            forward_pair(chunk, quarter).wait_send()
        send_give(chunk).wait_send()

        @pl.when(chunk % wide != column)
        def _():
            for at in range(parts):
                send_x(chunk, at).wait_send()

    for at in range(parts):
        send_y(at).wait_send()

    @pl.when(me < line - 1)
    def _():
        @pl.loop(0, pieces)
        def _(piece):
            send_right(piece).wait_send()

    @pl.when(me > 0)
    def _():
        @pl.loop(0, pieces)
        def _(piece):
            send_left(piece).wait_send()

    for copy in place_copies:
        copy.wait_send()

    @pl.when(leads)
    def _():
        send_base.wait_send()

        @pl.loop(0, bands)
        def _(at):
            send_band(at).wait_send()

    row_total = totals[0]
    for step, copy in enumerate(total_copies):
        copy.wait()
        row_total = row_total + totals[step + 1]
    total_ref[...] = row_total


def merger(patches, counts, dest, qkv, wo, attn_gain, merge_gain, w1, b1, w2, b2, text, carry):
    groups = lax.axis_size("section") * lax.axis_size("dp")
    line = lax.axis_size("mp")
    chips = groups // 2
    patch_rows, width = patches.shape
    slot_rows = patch_rows // 4
    chunk_rows = slot_rows // chips
    run = chunk_rows // 2
    local_cols = qkv.shape[1]
    units = w1.shape[1]
    features = w2.shape[1]
    pieces = chips * 4
    piece_rows = 2 * chunk_rows
    target_rows = groups * run
    parts = 8
    low = jnp.bfloat16
    dma = pltpu.SemaphoreType.DMA
    sum_rows = text.shape[0] // 128
    bands = text.shape[0] // 16
    return pl.pallas_call(
        merger_kernel,
        out_shape=(
            jax.ShapeDtypeStruct((target_rows, features), low),
            jax.ShapeDtypeStruct((1, slot_rows), jnp.int32),
            jax.ShapeDtypeStruct((sum_rows, 128), jnp.float32),
            jax.ShapeDtypeStruct((1, target_rows), jnp.float32),
            jax.ShapeDtypeStruct(carry.shape, carry.dtype),
        ),
        in_specs=[
            pl.BlockSpec(memory_space={1: pltpu.SMEM, 2: pltpu.VMEM, 5: pltpu.VMEM, 6: pltpu.VMEM, 8: pltpu.VMEM, 10: pltpu.VMEM}.get(at, pl.ANY))
            for at in range(13)
        ],
        out_specs=[pl.BlockSpec(memory_space=pltpu.VMEM)] * 4 + [pl.BlockSpec(memory_space=pl.ANY)],
        scratch_shapes=[
            pltpu.VMEM(patches.shape, low),
            pltpu.VMEM(qkv.shape, low),
            pltpu.VMEM(wo.shape, low),
            pltpu.VMEM(text.shape, low),
            pltpu.VMEM(text.shape, low),
            pltpu.VMEM((text.shape[0], 128), jnp.float32),
            pltpu.VMEM((text.shape[0], 128), jnp.float32),
            dma((2,)),
            dma((bands,)),
            dma((bands,)),
            pltpu.VMEM(patches.shape, low),
            pltpu.VMEM((groups, 1, slot_rows), jnp.int32),
            pltpu.VMEM((2 * sum_rows, 128), jnp.float32),
            pltpu.VMEM((patch_rows, local_cols), low),
            pltpu.VMEM((patch_rows, local_cols), low),
            pltpu.VMEM((patch_rows, local_cols), low),
            pltpu.VMEM((patch_rows, local_cols), low),
            pltpu.VMEM((4, slot_rows, local_cols), low),
            pltpu.VMEM((line, slot_rows, local_cols), low),
            pltpu.VMEM((line,) + wo.shape, low),
            pltpu.VMEM((chips, chunk_rows, width), low),
            pltpu.VMEM(w1.shape, low),
            pltpu.VMEM(w2.shape, low),
            dma((5,)),
            dma((line - 1,)),
            dma((line - 1,)),
            dma((line - 1, 7)),
            dma((line - 1, 4)),
            dma((line - 1, 4)),
            dma((line - 1, counts.shape[0])),
            dma((line - 1, counts.shape[0])),
            pltpu.VMEM((groups, chips, chunk_rows, width), low),
            pltpu.VMEM((chips, 4, 2, chunk_rows, units), jnp.float32),
            pltpu.VMEM((pieces, piece_rows, units), low),
            pltpu.VMEM((pieces, piece_rows, units), low),
            pltpu.VMEM((pieces, piece_rows, units), low),
            pltpu.VMEM((pieces, piece_rows, units), low),
            pltpu.VMEM((chips, 2, chips, chunk_rows, units), low),
            pltpu.VMEM((chips, target_rows, features), low),
            pltpu.VMEM((chips, target_rows, features), low),
            pltpu.VMEM((chips, target_rows, features), jnp.float32),
            pltpu.VMEM((chips, target_rows, features), low),
            pltpu.VMEM((chips, target_rows, features), low),
            pltpu.VMEM((target_rows, features), low),
            pltpu.VMEM((target_rows, features), low),
            pltpu.VMEM((target_rows, 128), jnp.float32),
            pltpu.VMEM((groups, 1, slot_rows), jnp.int32),
            pltpu.VMEM((line, 2 * sum_rows, 128), jnp.float32),
            pltpu.VMEM((sum_rows, 128), jnp.float32),
            pltpu.VMEM((sum_rows, 128), jnp.float32),
            pltpu.VMEM((line, 1, target_rows), jnp.float32),
            dma((chips, 7)),
            dma((chips, 4)),
            dma((chips, 4)),
            dma((pieces,)),
            dma((pieces,)),
            dma((pieces,)),
            dma((pieces,)),
            dma((chips,)),
            dma((chips,)),
            dma((chips, parts)),
            dma((chips, parts)),
            dma((parts,)),
            dma((parts,)),
            dma((groups - 1,)),
            dma((groups - 1,)),
            dma((line - 1,)),
            dma((line - 1,)),
            dma,
            dma,
            dma((line - 1,)),
            dma((line - 1,)),
        ],
        cost_estimate=pl.CostEstimate(
            flops=10**11, bytes_accessed=10**7, transcendentals=0
        ),
        compiler_params=pltpu.CompilerParams(
            collective_id=6, has_side_effects=True, vmem_limit_bytes=VMEM_LIMIT
        ),
    )(patches, counts, dest, qkv, wo, attn_gain, merge_gain, w1, b1, w2, b2, text, carry)


def placing_kernel(
    text_hbm,
    incoming_hbm,
    img_ref,
    spot_ref,
    total_ref,
    base_ref,
    gain_ref,
    seq_hbm,
    layer_hbm,
    text,
    incoming,
    seq,
    layer,
    load_sem,
    store_sem,
):
    cuts = load_sem.shape[1]
    height = text.shape[0] // cuts
    per = base_ref.shape[1] // height
    first = lax.axis_index("section") == 0
    gain = gain_ref[...].reshape(1, -1).astype(jnp.float32)

    def move(which, at):
        cut = pl.ds(at * height, height)
        source, target, sem = (
            (text_hbm, text, load_sem.at[0, at]),
            (incoming_hbm, incoming, load_sem.at[1, at]),
            (seq, seq_hbm, store_sem.at[0, at]),
            (layer, layer_hbm, store_sem.at[1, at]),
        )[which]
        return pltpu.make_async_copy(source.at[cut], target.at[cut], sem)

    for at in range(cuts):
        move(0, at).start()

        @pl.when(jnp.logical_not(first))
        def _():
            move(1, at).start()

    width = base_ref.shape[1]
    lane = lax.broadcasted_iota(jnp.int32, (height, width), 1)
    low_row = lax.broadcasted_iota(jnp.int32, (height, width), 0)
    for at in range(cuts):
        cut = pl.ds(at * height, height)
        at_row = at * height + lax.broadcasted_iota(jnp.int32, (height, spot_ref.shape[1]), 0)
        hits = spot_ref[...] == at_row
        hit = jnp.max(hits.astype(jnp.float32), axis=1, keepdims=True) > 0.0
        placed = jnp.dot(
            hits.astype(jnp.float32).astype(jnp.bfloat16), img_ref[...], preferred_element_type=jnp.float32
        ).astype(jnp.bfloat16)
        diagonal = lane == low_row + at % per * height
        base = jnp.sum(
            jnp.where(diagonal, base_ref[at // per : at // per + 1], 0.0), axis=1, keepdims=True
        )
        move(0, at).wait()
        seq[cut] = jnp.where(hit, placed, text[cut])
        move(2, at).start()

        @pl.when(first)
        def _():
            total = jnp.sum(jnp.where(hits, total_ref[...], 0.0), axis=1, keepdims=True)
            total = jnp.where(hit, total, base)
            scale = lax.rsqrt(total / HID + llm_eps)
            layer[cut] = (seq[cut].astype(jnp.float32) * scale * gain).astype(layer.dtype)

        @pl.when(jnp.logical_not(first))
        def _():
            move(1, at).wait()
            scale = lax.rsqrt(base / HID + llm_eps)
            layer[cut] = (incoming[cut].astype(jnp.float32) * scale * gain).astype(layer.dtype)

        move(3, at).start()

    for at in range(cuts):
        move(2, at).wait()
        move(3, at).wait()


def placing(text, incoming, img, spot, total, base, gain):
    cuts = base.shape[0]
    return pl.pallas_call(
        placing_kernel,
        out_shape=(jax.ShapeDtypeStruct(text.shape, text.dtype),) * 2,
        in_specs=[pl.BlockSpec(memory_space=pl.ANY)] * 2 + [pl.BlockSpec(memory_space=pltpu.VMEM)] * 5,
        out_specs=[pl.BlockSpec(memory_space=pl.ANY)] * 2,
        scratch_shapes=[pltpu.VMEM(text.shape, text.dtype)] * 4
        + [pltpu.SemaphoreType.DMA((2, cuts)), pltpu.SemaphoreType.DMA((2, cuts))],
        cost_estimate=pl.CostEstimate(flops=10**9, bytes_accessed=10**7, transcendentals=0),
        compiler_params=pltpu.CompilerParams(vmem_limit_bytes=VMEM_LIMIT),
    )(text, incoming, img, spot, total, base, gain)


def per_device(*operands):
    (patches, patch_counts, dest_rows, qkv_weight, out_weight, attn_gain, merge_gain) = operands[:7]
    (fc1_weight, fc1_bias, fc2_weight, fc2_bias, text_embeds, section_hidden, llm_gain) = operands[7:]
    outer, _ = group_bits()
    group_count = lax.axis_size("section") * lax.axis_size("dp")
    merged_rows = patches.shape[0] // 4
    run_cap = merged_rows // group_count
    seq_rows = text_embeds.shape[0]
    held = group_count * merged_rows * patches.shape[1] * patches.dtype.itemsize
    if lax.axis_size("mp") != 4 or outer != [("dp", 2), ("section", 1)] or held > KERNEL_BYTES or run_cap % 16 or merged_rows % 128 or seq_rows % 128:
        return plain_per_device(*operands)
    img, spot, base, total, incoming = merger(
        patches,
        patch_counts,
        dest_rows,
        qkv_weight.transpose(1, 2, 0),
        out_weight,
        attn_gain,
        merge_gain,
        fc1_weight,
        fc1_bias,
        fc2_weight,
        fc2_bias,
        text_embeds,
        section_hidden,
    )
    return placing(text_embeds, incoming, img, spot, total, base, llm_gain)


def solution(mesh):
    in_specs = (
        P(("section", "dp"), None),
        P(("section", "dp")),
        P(("section", "dp")),
        P(None, None, "mp"),
        P("mp", None),
        P(),
        P(),
        P("mp", ("section", "dp")),
        P(("section", "dp")),
        P(("section", "dp"), "mp"),
        P("mp"),
        P(("section", "dp"), "mp"),
        P(("section", "dp"), "mp"),
        P("mp"),
    )
    out_specs = (P(("section", "dp"), "mp"), P(("section", "dp"), "mp"))
    return jax.shard_map(
        per_device, mesh=mesh, in_specs=in_specs, out_specs=out_specs, check_vma=False
    )
```

```python
import functools
import math

import jax
import jax.numpy as jnp
from jax import lax
from jax.experimental import pallas as pl
from jax.experimental.pallas import tpu as pltpu
from jax.sharding import PartitionSpec as P

HEAD_DIM = 80
HID = 8192


vit_eps = 1e-06
llm_eps = 1e-06


def from_behind(value, axis, steps):
    count = lax.axis_size(axis)
    first, last = (max(0, -steps), min(count, count - steps))
    return lax.ppermute(value, axis, [(source, source + steps) for source in range(first, last)])


def layer_norm(values, gain):
    centred = values.astype(jnp.float32)
    centred = centred - jnp.mean(centred, axis=-1, keepdims=True)
    variance = jnp.mean(centred * centred, axis=-1, keepdims=True)
    return centred * lax.rsqrt(variance + vit_eps) * gain.astype(jnp.float32)


VMEM_LIMIT = 60 * 1024 * 1024
KERNEL_BYTES = 8 * 1024 * 1024


def vmem_call(kernel, out, scratch, sent_bytes, ident, *operands):
    return pl.pallas_call(
        kernel,
        out_shape=out,
        in_specs=[pl.BlockSpec(memory_space=pltpu.VMEM)] * len(operands),
        out_specs=pl.BlockSpec(memory_space=pltpu.VMEM),
        scratch_shapes=scratch,
        cost_estimate=pl.CostEstimate(
            flops=sent_bytes * 20000, bytes_accessed=sent_bytes * 2, transcendentals=0
        ),
        compiler_params=pltpu.CompilerParams(
            collective_id=ident, has_side_effects=True, vmem_limit_bytes=VMEM_LIMIT
        ),
    )(*operands)


def exchange_kernel(count, spread, x_ref, o_ref, send_sem, recv_sem, own_sem):
    me = lax.axis_index("mp")
    barrier = pltpu.get_barrier_semaphore()
    for step in range(1, count):
        peer = lax.rem(me + step, count)
        pl.semaphore_signal(
            barrier, inc=1, device_id={"mp": peer}, device_id_type=pl.DeviceIdType.MESH
        )
    pl.semaphore_wait(barrier, count - 1)
    copies = []
    for step in sorted(range(1, count), key=lambda s: -min(s, count - s)):
        peer = lax.rem(me + step, count)
        copy = pltpu.make_async_remote_copy(
            src_ref=x_ref.at[peer] if spread else x_ref,
            dst_ref=o_ref.at[me],
            send_sem=send_sem.at[step - 1],
            recv_sem=recv_sem.at[step - 1],
            device_id={"mp": peer},
            device_id_type=pl.DeviceIdType.MESH,
        )
        copy.start()
        copies.append(copy)
    own = pltpu.make_async_copy(x_ref.at[me] if spread else x_ref, o_ref.at[me], own_sem)
    own.start()
    own.wait()
    for copy in copies:
        copy.wait()


def relay_kernel(count, x_ref, o_ref, send_sem, recv_sem, own_sem):
    me = lax.axis_index("mp")
    barrier = pltpu.get_barrier_semaphore()
    for step in range(1, count):
        peer = lax.rem(me + step, count)
        pl.semaphore_signal(
            barrier, inc=1, device_id={"mp": peer}, device_id_type=pl.DeviceIdType.MESH
        )
    pl.semaphore_wait(barrier, count - 1)
    own = pltpu.make_async_copy(x_ref, o_ref.at[me], own_sem)
    own.start()

    def hop(way, step):
        owner = lax.rem(me - way * step + count, count)
        return pltpu.make_async_remote_copy(
            src_ref=o_ref.at[owner] if step else x_ref,
            dst_ref=o_ref.at[owner],
            send_sem=send_sem.at[(way + 1) // 2, step],
            recv_sem=recv_sem.at[(way + 1) // 2, step],
            device_id={"mp": lax.rem(me + way + count, count)},
            device_id_type=pl.DeviceIdType.MESH,
        )

    def holds(way, step):
        return me >= step if way > 0 else me + step < count

    def sends(way):
        return me < count - 1 if way > 0 else me > 0

    for step in range(count):
        for way in (1, -1):
            if step:

                @pl.when(holds(way, step))
                def _():
                    owner = lax.rem(me - way * step + count, count)
                    pltpu.make_async_remote_copy(
                        src_ref=x_ref,
                        dst_ref=o_ref.at[owner],
                        send_sem=send_sem.at[(way + 1) // 2, step - 1],
                        recv_sem=recv_sem.at[(way + 1) // 2, step - 1],
                        device_id={"mp": lax.rem(me - way + count, count)},
                        device_id_type=pl.DeviceIdType.MESH,
                    ).wait_recv()

            if step < count - 1:

                @pl.when(jnp.logical_and(holds(way, step), sends(way)))
                def _():
                    hop(way, step).start()

    own.wait()
    for step in range(count - 1):
        for way in (1, -1):

            @pl.when(jnp.logical_and(holds(way, step), sends(way)))
            def _():
                hop(way, step).wait_send()


def relay_mp(value, ident):
    count = lax.axis_size("mp")
    return vmem_call(
        functools.partial(relay_kernel, count),
        jax.ShapeDtypeStruct((count,) + value.shape, value.dtype),
        [
            pltpu.SemaphoreType.DMA((2, count - 1)),
            pltpu.SemaphoreType.DMA((2, count - 1)),
            pltpu.SemaphoreType.DMA,
        ],
        count * value.size * value.dtype.itemsize,
        ident,
        value,
    )


def exchange_mp(value, spread, ident):
    count = lax.axis_size("mp")
    shape = value.shape if spread else (count,) + value.shape
    size = math.prod(shape) * value.dtype.itemsize
    return vmem_call(
        functools.partial(exchange_kernel, count, spread),
        jax.ShapeDtypeStruct(shape, value.dtype),
        [
            pltpu.SemaphoreType.DMA((count - 1,)),
            pltpu.SemaphoreType.DMA((count - 1,)),
            pltpu.SemaphoreType.DMA,
        ],
        size,
        ident,
        value,
    )


def sum_scatter_mp(blocks, ident):
    return jnp.sum(exchange_mp(blocks, True, ident).astype(jnp.float32), axis=0)


def gather_mp(value):
    got = relay_mp(value, 2)
    return got.reshape((-1,) + value.shape[1:])


def total_mp(value):
    return jnp.sum(exchange_mp(value.reshape(-1, 128), False, 3), axis=0).reshape(-1)


def flip(index, bit):
    return index + bit * (1 - 2 * (index // bit % 2))


def group_bits():
    outer = [("dp", 1 << k) for k in range(1, lax.axis_size("dp").bit_length() - 1)]
    outer += [("section", 1 << k) for k in range(lax.axis_size("section").bit_length() - 1)]
    return outer, ("dp", 1)


def meets(axis, bit):
    return {axis: flip(lax.axis_index(axis), bit)}


def group_at(mask):
    spots = {axis: lax.axis_index(axis) for axis in ("section", "dp")}
    for axis, bit in mask:
        spots[axis] = flip(spots[axis], bit)
    return spots["section"] * lax.axis_size("dp") + spots["dp"]


def greet(bits):
    barrier = pltpu.get_barrier_semaphore()
    for axis, bit in bits:
        pl.semaphore_signal(
            barrier, inc=1, device_id=meets(axis, bit), device_id_type=pl.DeviceIdType.MESH
        )
    pl.semaphore_wait(barrier, len(bits))


def gather_kernel(x_ref, o_ref, send_sem, recv_sem, own_sem):
    outer, last = group_bits()
    greet(outer + [last])
    half = x_ref.shape[1] // 2
    sent, waiting = [], []
    slots = iter(range(send_sem.shape[0]))

    def pass_on(mask, stage, part, order):
        cols = pl.ds(part * half, half)
        spot = group_at(mask)
        source = o_ref.at[spot, :, cols] if mask else x_ref.at[:, cols]
        for later in range(stage, len(order)):
            slot = next(slots)
            copy = pltpu.make_async_remote_copy(
                src_ref=source,
                dst_ref=o_ref.at[spot, :, cols],
                send_sem=send_sem.at[slot],
                recv_sem=recv_sem.at[slot],
                device_id=meets(*order[later]),
                device_id_type=pl.DeviceIdType.MESH,
            )
            copy.start()
            sent.append(copy)
            waiting.append((later, copy, mask + [order[later]], part, order))

    pass_on([], 0, 0, outer + [last])
    pass_on([], 0, 1, outer[::-1] + [last])
    own = pltpu.make_async_copy(x_ref, o_ref.at[group_at([])], own_sem)
    own.start()
    while waiting:
        first = min(range(len(waiting)), key=lambda at: waiting[at][0])
        stage, copy, mask, part, order = waiting.pop(first)
        copy.wait_recv()
        pass_on(mask, stage + 1, part, order)
    for copy in sent:
        copy.wait_send()
    own.wait()


def gather_groups(value):
    count = lax.axis_size("section") * lax.axis_size("dp")
    size = count * value.size * value.dtype.itemsize
    if size > KERNEL_BYTES:
        return lax.all_gather(value, ("section", "dp"), axis=0, tiled=True)
    slots = 2 * (count - 1)
    got = vmem_call(
        gather_kernel,
        jax.ShapeDtypeStruct((count,) + value.shape, value.dtype),
        [
            pltpu.SemaphoreType.DMA((slots,)),
            pltpu.SemaphoreType.DMA((slots,)),
            pltpu.SemaphoreType.DMA,
        ],
        size,
        4,
        value,
    )
    return got.reshape(-1, value.shape[1])


def scatter_kernel(x_ref, o_ref, held, taken, send_sem, recv_sem):
    outer, first = group_bits()
    greet(outer + [first])
    rows = x_ref.shape[1]
    half = x_ref.shape[2] // 2
    chunk = 32
    orders = ([first] + outer, [first] + outer[::-1])
    slots = iter(range(send_sem.shape[0]))
    masks = [[]]
    for bit in outer:
        masks = masks + [mask + [bit] for mask in masks]
    place_of = {frozenset(mask): at for at, mask in enumerate(masks)}
    base = len(masks)
    live = {}

    def send(part, stage):
        cols = pl.ds(part * half, half)
        bit = orders[part][stage]
        kept = orders[part][stage + 1 :]
        copies = []
        for mask in [m for m in masks if set(m) <= set(kept)]:
            if stage == 0:
                source = x_ref.at[group_at(mask + [bit]), :, cols]
            else:
                source = held.at[place_of[frozenset(mask + [bit])], :, cols]
            landing = 2 * base - 2 ** (len(kept) + 1) + [
                m for m in masks if set(m) <= set(kept)
            ].index(mask)
            slot = next(slots)
            copy = pltpu.make_async_remote_copy(
                src_ref=source,
                dst_ref=taken.at[landing, :, cols],
                send_sem=send_sem.at[slot],
                recv_sem=recv_sem.at[slot],
                device_id=meets(*bit),
                device_id_type=pl.DeviceIdType.MESH,
            )
            copy.start()
            copies.append((copy, mask, landing))
        live[part, stage] = copies

    def add(part, stage):
        cols = pl.ds(part * half, half)
        final = stage + 1 == len(orders[part])
        following = None if final else orders[part][stage + 1]
        copies = live[part, stage]
        for copy, mask, landing in sorted(copies, key=lambda c: following not in c[1]):
            copy.wait_recv()
            at = place_of[frozenset(mask)]
            spot = group_at(mask)

            @pl.loop(0, rows // chunk)
            def _(step):
                span = pl.ds(step * chunk, chunk)
                mine = x_ref[spot, span, cols] if stage == 0 else held[at, span, cols]
                total = mine.astype(jnp.float32) + taken[landing, span, cols].astype(jnp.float32)
                if final:
                    o_ref[span, cols] = total
                else:
                    held[at, span, cols] = total.astype(held.dtype)

    send(0, 0)
    send(1, 0)
    for stage in range(len(orders[0])):
        for part in (0, 1):
            add(part, stage)
            if stage + 1 < len(orders[0]):
                send(part, stage + 1)
    for copies in live.values():
        for copy, _, _ in copies:
            copy.wait_send()


def sum_scatter_groups(value):
    count = lax.axis_size("section") * lax.axis_size("dp")
    size = value.size * value.dtype.itemsize
    if size > KERNEL_BYTES:
        return lax.psum_scatter(value, ("section", "dp"), scatter_dimension=0, tiled=True)
    rows, cols = value.shape[0] // count, value.shape[1]
    slots = 2 * (count - 1)
    return vmem_call(
        scatter_kernel,
        jax.ShapeDtypeStruct((rows, cols), jnp.float32),
        [
            pltpu.VMEM((count // 2, rows, cols), value.dtype),
            pltpu.VMEM((count - 1, rows, cols), value.dtype),
            pltpu.SemaphoreType.DMA((slots,)),
            pltpu.SemaphoreType.DMA((slots,)),
        ],
        size,
        5,
        value.reshape(count, rows, cols),
    )


def plain_per_device(
    patches,
    patch_counts,
    dest_rows,
    qkv_weight,
    out_weight,
    attn_gain,
    merge_gain,
    fc1_weight,
    fc1_bias,
    fc2_weight,
    fc2_bias,
    text_embeds,
    section_hidden,
    llm_gain,
):
    width = patches.shape[1]
    tile_total = patch_counts.shape[0]
    block_rows = patches.shape[0] // tile_total
    merged_rows = patches.shape[0] // 4
    local_cols = qkv_weight.shape[2]
    local_heads = local_cols // HEAD_DIM
    feature_cols = text_embeds.shape[1]
    seq_rows = text_embeds.shape[0]
    section_count = lax.axis_size("section")
    group_count = section_count * lax.axis_size("dp")
    run_cap = max(2, merged_rows // group_count)
    run_total = merged_rows // run_cap
    run_target = dest_rows.reshape(run_total, run_cap)[:, 0] // seq_rows
    takes = jnp.arange(group_count, dtype=jnp.int32)[:, None] == run_target[None, :]
    slot_in_tile = jnp.arange(merged_rows, dtype=jnp.int32) % (block_rows // 4)
    tile_counts = jnp.repeat(patch_counts, block_rows // 4, total_repeat_length=merged_rows)
    live = slot_in_tile * 4 < tile_counts
    place = jnp.where(live, dest_rows % seq_rows - seq_rows, 0).reshape(run_total, run_cap)
    send_place = jnp.sum(jnp.where(takes[:, :, None], place[None], 0), axis=1) + seq_rows
    got_place = lax.all_to_all(send_place, ("section", "dp"), split_axis=0, concat_axis=0, tiled=True)
    incoming = from_behind(section_hidden, "section", 1)
    normed_in = layer_norm(patches, attn_gain).astype(jnp.bfloat16)
    projections = jnp.dot(
        normed_in, qkv_weight.reshape(width, 3 * local_cols), preferred_element_type=jnp.float32
    ).astype(jnp.bfloat16)
    projections = projections.reshape(tile_total, block_rows, 3, local_heads, HEAD_DIM)
    query_part = projections[:, :, 0]
    key_part = projections[:, :, 1]
    value_part = projections[:, :, 2]
    scores = jnp.einsum(
        "tqhd,tkhd->thqk", query_part, key_part, preferred_element_type=jnp.float32
    ) * HEAD_DIM ** (-0.5)
    key_live = (
        jnp.arange(block_rows, dtype=jnp.int32)[None, None, None, :]
        < patch_counts[:, None, None, None]
    )
    scores = jnp.where(key_live, scores, -1e30)
    weights = jax.nn.softmax(scores, axis=-1).astype(jnp.bfloat16)
    attended = jnp.einsum(
        "thqk,tkhd->tqhd", weights, value_part, preferred_element_type=jnp.float32
    ).astype(jnp.bfloat16)
    attended = attended.reshape(patches.shape[0], local_cols)
    lane_source = jnp.arange(run_total, dtype=jnp.int32)[None, :] * run_cap
    run_source = jnp.sum(jnp.where(takes, lane_source, 0), axis=1)
    row_source = (
        run_source[:, None] + jnp.arange(run_cap, dtype=jnp.int32)[None, :]
    ).reshape(-1) * 4
    slots_at = jnp.arange(patches.shape[0], dtype=jnp.int32)
    patch_at = jnp.arange(4, dtype=jnp.int32)
    order = (
        (row_source[None, :] + patch_at[:, None]).reshape(-1)[:, None] == slots_at[None, :]
    ).astype(jnp.bfloat16)
    own_order = (
        (row_source + lax.axis_index("mp"))[:, None] == slots_at[None, :]
    ).astype(jnp.bfloat16)
    ordered = jnp.dot(order, attended, preferred_element_type=jnp.float32).astype(jnp.bfloat16)
    own_patch = jnp.dot(own_order, patches, preferred_element_type=jnp.float32)
    partial_proj = jnp.dot(ordered, out_weight, preferred_element_type=jnp.float32)
    own_proj = sum_scatter_mp(
        partial_proj.astype(jnp.bfloat16).reshape(4, group_count * run_cap, width), 0
    )
    block_out = (own_patch + own_proj).astype(jnp.bfloat16)
    merge_part = layer_norm(block_out, merge_gain).astype(jnp.bfloat16)
    slot_rows = group_count * run_cap
    gathered = gather_groups(merge_part)
    gathered = (
        gathered.reshape(group_count, group_count, run_cap, width)
        .transpose(1, 0, 2, 3)
        .reshape(group_count * slot_rows, width)
    )
    first_partial = jnp.dot(gathered, fc1_weight, preferred_element_type=jnp.float32)
    mp_count = lax.axis_size("mp")
    first_total = sum_scatter_mp(
        first_partial.astype(jnp.bfloat16).reshape(mp_count, -1, fc1_weight.shape[1]),
        1,
    )
    hidden_part = jax.nn.gelu(
        first_total + fc1_bias.astype(jnp.float32), approximate=False
    ).astype(jnp.bfloat16)
    hidden = gather_mp(hidden_part)
    second_partial = jnp.dot(hidden, fc2_weight, preferred_element_type=jnp.float32)
    embed_total = sum_scatter_groups(second_partial.astype(jnp.bfloat16)).astype(jnp.float32)
    image_embeds = (embed_total + fc2_bias.astype(jnp.float32)).astype(jnp.bfloat16)
    hits = got_place.reshape(1, -1) == jnp.arange(seq_rows, dtype=jnp.int32)[:, None]
    placed = jnp.dot(
        hits.astype(jnp.bfloat16), image_embeds, preferred_element_type=jnp.float32
    ).astype(jnp.bfloat16)
    sequence_embeds = jnp.where(jnp.any(hits, axis=1)[:, None], placed, text_embeds)
    entering = jnp.where(lax.axis_index("section") == 0, sequence_embeds, incoming).astype(
        jnp.float32
    )
    row_total = total_mp(jnp.sum(entering * entering, axis=1))
    layer_inputs = (
        entering * lax.rsqrt(row_total / HID + llm_eps)[:, None] * llm_gain.astype(jnp.float32)
    ).astype(jnp.bfloat16)
    return (sequence_embeds, layer_inputs)


LAG = 2
FC2_COLS = 1024
HALF_ROOT = 0.5**0.5


def remote(src, dst, send_sem, recv_sem, device):
    return pltpu.make_async_remote_copy(
        src_ref=src,
        dst_ref=dst,
        send_sem=send_sem,
        recv_sem=recv_sem,
        device_id=device,
        device_id_type=pl.DeviceIdType.MESH,
    )


def group_device(group):
    per_section = lax.axis_size("dp")
    return {"section": group // per_section, "dp": lax.rem(group, per_section)}


def tell(device):
    pl.semaphore_signal(
        pltpu.get_barrier_semaphore(),
        inc=1,
        device_id=device,
        device_id_type=pl.DeviceIdType.MESH,
    )


def merger_kernel(
    patches_hbm,
    counts_ref,
    dest_ref,
    qkv_hbm,
    wo_hbm,
    attn_gain_ref,
    merge_gain_ref,
    w1_hbm,
    b1_ref,
    w2_hbm,
    b2_ref,
    text_hbm,
    carry_hbm,
    img_ref,
    spot_ref,
    base_ref,
    total_ref,
    incoming_hbm,
    patches_ref,
    qkv_ref,
    wo_ref,
    text_ref,
    carry_ref,
    text_squares,
    carry_squares,
    carry_sem,
    carry_send,
    carry_recv,
    normed,
    place_ref,
    sums_ref,
    query,
    key,
    value_part,
    attended,
    ordered,
    arrived,
    wo_all,
    x_ref,
    w1_ref,
    w2_ref,
    weight_sem,
    wo_send,
    wo_recv,
    wo_out,
    wo_plane,
    wo_pair,
    a_send,
    a_recv,
    rows,
    part,
    before,
    after,
    right_out,
    left_out,
    hidden,
    give,
    take,
    keep,
    x_out,
    x_in,
    y_out,
    y_in,
    squares,
    spots,
    sums,
    base_out,
    base_in,
    totals,
    row_send,
    row_recv,
    pair_recv,
    right_send,
    right_recv,
    left_send,
    left_recv,
    give_send,
    give_recv,
    x_send,
    x_recv,
    y_send,
    y_recv,
    spot_send,
    spot_recv,
    sum_send,
    sum_recv,
    base_send,
    base_recv,
    total_send,
    total_recv,
):
    groups = lax.axis_size("section") * lax.axis_size("dp")
    sections = lax.axis_size("section")
    line = lax.axis_size("mp")
    me = lax.axis_index("mp")
    section = lax.axis_index("section")
    dp = lax.axis_index("dp")
    core = lax.rem(dp, 2)
    column = dp // 2
    wide = lax.axis_size("dp") // 2
    group = section * lax.axis_size("dp") + dp
    chips = groups // 2
    pair = {"dp": flip(dp, 1)}
    over_x = {"dp": flip(dp, 2)}
    over_y = {"section": flip(section, 1)}
    quarters = 4
    pieces = chips * quarters
    take_rows = rows.shape[2] // 2
    lag_right = me * LAG
    half_rows = part.shape[3]
    split_from = 3
    single = 12
    run = half_rows // 2
    lag_left = (line - 1 - me) * LAG
    lag_total = (line - 1) * LAG

    fetches = [
        pltpu.make_async_copy(source, target, weight_sem.at[at])
        for at, (source, target) in enumerate(
            (
                (wo_hbm, wo_ref),
                (patches_hbm, patches_ref),
                (qkv_hbm, qkv_ref),
                (w1_hbm, w1_ref),
                (w2_hbm, w2_ref),
            )
        )
    ]
    for fetch in fetches:
        fetch.start()
    for step in range(1, groups):
        tell(group_device(lax.rem(group + step, groups)))
    for step in range(1, line):
        tell({"mp": lax.rem(me + step, line)})
    pl.semaphore_wait(pltpu.get_barrier_semaphore(), groups + line - 2)

    def chip_of(quarter):
        there_x = lax.rem(quarter // 2 + column, 2)
        there_y = lax.rem(lax.rem(quarter, 2) + section, 2)
        return there_y * wide + there_x

    def group_of(quarter, at_core):
        return chip_of(quarter) * 2 + at_core

    def own_send(chunk, which):
        sem = (row_recv.at[chunk, 1], row_recv.at[chunk, 2], pair_recv.at[chunk, 0])[which]
        device = (over_y, over_x, pair)[which]
        return remote(x_ref.at[chunk], rows.at[group, chunk], row_send.at[chunk, which], sem, device)

    def forward_x(chunk):
        spot = rows.at[group_of(1, core), chunk]
        return remote(spot, spot, row_send.at[chunk, 3], row_recv.at[chunk, 3], over_x)

    def forward_pair(chunk, quarter):
        spot = rows.at[group_of(quarter, core), chunk]
        return remote(
            spot, spot, row_send.at[chunk, 3 + quarter], pair_recv.at[chunk, quarter], pair
        )

    leads = section < sections - 1
    bands = carry_send.shape[0]
    band_rows = carry_hbm.shape[0] // bands
    text_fetch = pltpu.make_async_copy(text_hbm, text_ref, carry_sem.at[0])
    carry_fetch = pltpu.make_async_copy(carry_hbm, carry_ref, carry_sem.at[1])

    @pl.when(leads)
    def _():
        text_fetch.start()
        carry_fetch.start()

    def send_band(at):
        cut = pl.ds(pl.multiple_of(at * band_rows, band_rows), band_rows)
        return remote(
            carry_hbm.at[cut], incoming_hbm.at[cut], carry_send.at[at], carry_recv.at[at], {"section": section + 1}
        )

    def send_bands(first, last):
        @pl.when(leads)
        def _():
            for at in range(first, last):
                send_band(at).start()

    early = bands // 10
    looped = bands - early - bands // 6

    def wo_slice(ref, holder):
        high = wo_ref.shape[0] // lax.axis_size("dp")
        broad = wo_ref.shape[1] // sections
        top = pl.multiple_of(lax.rem(holder, lax.axis_size("dp")) * high, high)
        left = pl.multiple_of(holder // lax.axis_size("dp") * broad, broad)
        return ref.at[pl.ds(top, high), pl.ds(left, broad)]

    def wo_line(step):
        return remote(
            wo_slice(wo_ref, group),
            wo_slice(wo_all.at[me], group),
            wo_send.at[step - 1],
            wo_recv.at[step - 1],
            {"mp": lax.rem(me + step, line)},
        )

    def wo_hop(step, quarter, at, sem, device):
        block = wo_slice(wo_all.at[lax.rem(me - step + line, line)], group_of(quarter, core))
        return remote(block, block, wo_out.at[step - 1, at], sem, device)

    def wo_starts(step):
        return (
            wo_hop(step, 0, 0, wo_plane.at[step - 1, 1], over_y),
            wo_hop(step, 0, 1, wo_plane.at[step - 1, 2], over_x),
            wo_hop(step, 0, 2, wo_pair.at[step - 1, 0], pair),
        )

    def wo_forward_x(step):
        return wo_hop(step, 1, 3, wo_plane.at[step - 1, 3], over_x)

    def wo_forward_pair(step, quarter):
        return wo_hop(step, quarter, 3 + quarter, wo_pair.at[step - 1, quarter], pair)

    def wo_landed(step, quarter):
        return wo_hop(step, quarter, 0, wo_plane.at[step - 1, quarter], over_x)

    def wo_paired(step, quarter):
        block = wo_slice(wo_all.at[lax.rem(me - step + line, line)], group_of(quarter, 1 - core))
        return remote(block, block, wo_out.at[step - 1, 0], wo_pair.at[step - 1, quarter], pair)

    steps = range(1, line)
    low_end, high_end = me == 0, me == line - 1
    at_end = jnp.logical_or(low_end, high_end)
    first_sent = jnp.where(high_end, 3, 1)
    second = jnp.where(at_end, 2, 3)
    last_sent = jnp.where(low_end, 3, jnp.where(high_end, 1, 2))
    first_here = jnp.where(low_end, 3, 1)
    last_here = jnp.where(low_end, 1, jnp.where(high_end, 3, 2))
    fetches[0].wait()
    for step in (first_sent, second, last_sent):
        wo_line(step).start()

    send_bands(0, early)
    slots = ordered.shape[1]
    dest = dest_ref[...].reshape(1, slots)
    slot = lax.broadcasted_iota(jnp.int32, (1, slots), 1)
    tiles = counts_ref.shape[0]
    slice_rows = carry_hbm.shape[0]
    target = dest // slice_rows
    slot_place = slot
    for stride in [1 << bit for bit in range(run.bit_length() - 1, slots.bit_length())][::-1]:
        slot_place = jnp.where(slot_place >= stride, slot_place - stride, slot_place)
    slot_target = target * run + slot_place
    filled = jnp.zeros((1, slots), jnp.int32)
    for tile in range(tiles):
        start = tile * (slots // tiles)
        within = jnp.logical_and(slot >= start, slot - start < slots // tiles)
        filled = jnp.where(jnp.logical_and(within, (slot - start) * 4 < counts_ref[tile]), 1, filled)
    spot = jnp.where(filled > 0, dest - target * slice_rows, slice_rows)
    high = (spot // 16).astype(jnp.float32)
    low = (spot - spot // 16 * 16).astype(jnp.float32)
    to_group = lax.broadcasted_iota(jnp.int32, (groups, slots), 0) == target
    at_source = lax.broadcasted_iota(jnp.int32, (slots, slots), 1)
    moved = (at_source == group * run + slot_place.reshape(slots, 1)).astype(jnp.float32).astype(jnp.bfloat16)

    def moved_to(value):
        picked = jnp.where(to_group, value, 0.0).astype(jnp.bfloat16)
        return jnp.dot(picked, moved, preferred_element_type=jnp.float32)

    place_rows = (moved_to(high) * 16.0 + moved_to(low)).astype(jnp.int32)
    place_ref[...] = place_rows.reshape(place_ref.shape)
    place_copies = []
    for step in range(1, groups):
        peer = lax.rem(group + step, groups)
        copy = remote(
            place_ref.at[peer], spots.at[step], spot_send.at[step - 1], spot_recv.at[step - 1], group_device(peer)
        )
        copy.start()
        place_copies.append(copy)
    spots[0] = place_ref[group]

    tall = min(patches_ref.shape[0], 128)
    fetches[1].wait()

    @pl.loop(0, patches_ref.shape[0] // tall)
    def _(at):
        cut = pl.ds(at * tall, tall)
        normed[cut] = layer_norm(
            patches_ref[cut], attn_gain_ref[...].reshape(1, -1)
        ).astype(normed.dtype)

    fetches[2].wait()
    for which, ref in enumerate((query, key, value_part)):
        ref[...] = lax.dot_general(
            normed[...], qkv_ref[which], (((1,), (1,)), ((), ())), preferred_element_type=jnp.float32
        ).astype(ref.dtype)

    def begin(step):
        wo_line(step).wait_recv()
        for copy in wo_starts(step):
            copy.start()

    def pass_y(step):
        wo_landed(step, 1).wait_recv()
        wo_forward_x(step).start()
        wo_forward_pair(step, 1).start()

    def pass_x(step, quarter):
        wo_landed(step, quarter).wait_recv()
        wo_forward_pair(step, quarter).start()

    begin(first_here)
    wo_all[me] = wo_ref[...]

    block = query.shape[0] // tiles
    lane = lax.broadcasted_iota(jnp.int32, (1, query.shape[1]), 1)
    at_key = lax.broadcasted_iota(jnp.int32, (block, block), 1)

    def attend(tile):
        cut = pl.ds(tile * block, block)
        tile_query, tile_key, tile_value = query[cut], key[cut], value_part[cut]
        live = at_key < counts_ref[tile]
        result = jnp.zeros((block, query.shape[1]), jnp.float32)
        for head in range(query.shape[1] // HEAD_DIM):
            own = jnp.logical_and(lane >= head * HEAD_DIM, lane < (head + 1) * HEAD_DIM)
            own = own.astype(jnp.float32).astype(jnp.bfloat16)
            scores = lax.dot_general(
                tile_query * own, tile_key, (((1,), (1,)), ((), ())), preferred_element_type=jnp.float32
            )
            scores = jnp.where(live, scores * HEAD_DIM**-0.5, -1e30)
            power = jnp.exp(scores - jnp.max(scores, axis=1, keepdims=True))
            weights = (power / jnp.sum(power, axis=1, keepdims=True)).astype(jnp.bfloat16)
            result = result + jnp.dot(weights, tile_value * own, preferred_element_type=jnp.float32)
        attended[cut] = result.astype(attended.dtype)

    tile_slots = slots // tiles

    def pick(height, width, patch):
        at_row = lax.broadcasted_iota(jnp.int32, (height, width), 0)
        at_patch = lax.broadcasted_iota(jnp.int32, (height, width), 1)
        return (at_patch == at_row * line + patch).astype(jnp.float32).astype(jnp.bfloat16)

    def exchange(step, tile):
        peer = lax.rem(me + step, line)
        cut = pl.ds(tile * tile_slots, tile_slots)
        return remote(
            ordered.at[peer, cut], arrived.at[me, cut], a_send.at[step - 1, tile], a_recv.at[step - 1, tile], {"mp": peer}
        )

    def spread(tile):
        source = attended[pl.ds(tile * block, block)]
        for patch in range(line):
            ordered[patch, pl.ds(tile * tile_slots, tile_slots)] = jnp.dot(
                pick(tile_slots, block, patch), source, preferred_element_type=jnp.float32
            ).astype(ordered.dtype)
        for step in (first_sent, second, last_sent):
            exchange(step, tile).start()

    for tile in range(tiles):
        attend(tile)
        spread(tile)
        if tile == 0:
            begin(second)
    begin(last_here)
    pass_y(first_here)
    send_bands(early, bands - looped)
    arrived[me] = ordered[me]
    order = (
        lax.broadcasted_iota(jnp.int32, (slots, slots), 0) == slot_target
    ).astype(jnp.float32).astype(jnp.bfloat16)
    block_out = jnp.dot(
        pick(slots, patches_ref.shape[0], me), patches_ref[...], preferred_element_type=jnp.float32
    )
    pass_y(second)
    pass_x(first_here, 2)
    pass_y(last_here)
    pass_x(second, 2)
    pass_x(first_here, 3)
    pass_x(last_here, 2)
    pass_x(second, 3)
    pass_x(last_here, 3)
    for step in steps:
        for quarter in range(quarters):
            wo_paired(step, quarter).wait_recv()
    for step in steps:
        for tile in range(tiles):
            exchange(step, tile).wait_recv()
    for source in range(line):
        block_out = block_out + jnp.dot(
            arrived[source], wo_all[source], preferred_element_type=jnp.float32
        )
    block_out = block_out.astype(jnp.bfloat16)
    merged = layer_norm(block_out, merge_gain_ref[...].reshape(1, -1)).astype(x_ref.dtype)
    x_ref[...] = (
        jnp.dot(order, merged, preferred_element_type=jnp.float32).astype(x_ref.dtype).reshape(x_ref.shape)
    )
    for chunk in range(chips):
        own_send(chunk, 0).start()
    for which in (1, 2):
        own_send(0, which).start()
    rows[group] = x_ref[...]
    for fetch in fetches[3:]:
        fetch.wait()

    def send_right(piece):
        return remote(
            right_out.at[piece], before.at[piece], right_send.at[piece], right_recv.at[piece], {"mp": me + 1}
        )

    def send_left(piece):
        return remote(
            left_out.at[piece], after.at[piece], left_send.at[piece], left_recv.at[piece], {"mp": me - 1}
        )

    def send_give(chunk):
        return remote(give.at[chunk], take.at[chunk], give_send.at[chunk], give_recv.at[chunk], pair)

    parts = x_send.shape[1]
    span = keep.shape[1] // parts

    def send_x(chunk, at):
        cut = pl.ds(at * span, span)
        return remote(
            x_out.at[chunk, cut], x_in.at[chunk, cut], x_send.at[chunk, at], x_recv.at[chunk, at], over_x
        )

    def send_y(at):
        cut = pl.ds(at * span, span)
        return remote(y_out.at[cut], y_in.at[cut], y_send.at[at], y_recv.at[at], over_y)

    def settle(chunk):
        send_give(chunk).wait_recv()
        mine = lax.rem(chunk, wide) == column

        @pl.when(mine)
        def _():
            @pl.loop(0, parts)
            def _(at):
                cut = pl.ds(at * span, span)
                keep[chunk, cut] = keep[chunk, cut] + take[chunk, cut].astype(jnp.float32)

        @pl.when(jnp.logical_not(mine))
        def _():
            @pl.loop(0, parts)
            def _(at):
                cut = pl.ds(at * span, span)
                x_out[chunk, cut] = (
                    keep[chunk, cut] + take[chunk, cut].astype(jnp.float32)
                ).astype(x_out.dtype)
                send_x(chunk, at).start()

    sum_rows = base_out.shape[0]

    def folded(value):
        value = value.astype(jnp.float32)
        square = value * value
        width = squares.shape[1]
        total = square[:, :width]
        for at_col in range(1, square.shape[1] // width):
            total = total + square[:, at_col * width : (at_col + 1) * width]
        return total

    def exchange_sums(step):
        return remote(
            sums_ref, sums.at[step], sum_send.at[step - 1], sum_recv.at[step - 1], {"mp": lax.rem(me + step, line)}
        )

    send_base = remote(base_out, base_in, base_send, base_recv, {"section": section + 1})
    share = text_ref.shape[0] // pieces

    def stage(i, carry):
        for extra in range(2):
            band = bands - looped + (i - quarters) * 2 + extra

            @pl.when(jnp.logical_and(leads, jnp.logical_and(i >= quarters, band < bands)))
            def _():
                send_band(band).start()

        @pl.when(jnp.logical_and(leads, i < pieces))
        def _():
            @pl.when(i == 0)
            def _():
                text_fetch.wait()
                carry_fetch.wait()

            cut = pl.ds(pl.multiple_of(i * share, share), share)
            text_squares[cut] = folded(text_ref[cut])
            carry_squares[cut] = folded(carry_ref[cut])

        @pl.when(jnp.logical_and(leads, i == pieces))
        def _():
            for which, ref in enumerate((text_squares, carry_squares)):
                for at in range(sum_rows):
                    cut = pl.ds(at * 128, 128)
                    at_sum = which * sum_rows + at
                    sums_ref[at_sum : at_sum + 1] = jnp.sum(ref[cut].T, axis=0, keepdims=True)
            for step in steps:
                exchange_sums(step).start()

        @pl.when(jnp.logical_and(leads, i == pieces + 4))
        def _():
            both = sums_ref[...]
            for step in steps:
                exchange_sums(step).wait()
                both = both + sums[step]
            base_out[...] = both[sum_rows:]
            base_ref[...] = both[:sum_rows]
            send_base.start()

        def relay(piece):
            chunk = piece // quarters
            quarter = lax.rem(piece, quarters)

            @pl.when(quarter == 1)
            def _():
                remote(
                    x_ref.at[chunk], rows.at[group_of(1, core), chunk], row_send.at[chunk, 0], row_recv.at[chunk, 1], over_y
                ).wait_recv()
                forward_x(chunk).start()
                forward_pair(chunk, 1).start()

                @pl.when(chunk + 1 < chips)
                def _():
                    for which in (1, 2):
                        own_send(chunk + 1, which).start()

            @pl.when(quarter > 1)
            def _():
                remote(
                    x_ref.at[chunk], rows.at[group_of(quarter, core), chunk], row_send.at[chunk, 1], row_recv.at[chunk, quarter], over_x
                ).wait_recv()
                forward_pair(chunk, quarter).start()

        def multiply(piece):
            chunk = piece // quarters
            quarter = lax.rem(piece, quarters)
            spot = rows.at[group_of(quarter, 1 - core), chunk]
            remote(x_ref.at[chunk], spot, row_send.at[chunk, 2], pair_recv.at[chunk, quarter], pair).wait_recv()
            lhs = rows[pl.ds(chip_of(quarter) * 2, 2), chunk]
            result = jnp.dot(
                lhs.reshape(-1, lhs.shape[2]), w1_ref[...], preferred_element_type=jnp.float32
            ).reshape(2, 2, run, part.shape[4])
            for target in range(2):
                part[chunk, quarter, target] = result[:, target].reshape(part.shape[3:])

        def once_then_twice(turn, work):
            @pl.when(jnp.logical_and(turn >= 0, turn < single))
            def _():
                work(turn)

            @pl.when(jnp.logical_and(turn >= single, turn < (pieces + single) // 2))
            def _():
                work(turn * 2 - single)
                work(turn * 2 - single + 1)

        once_then_twice(i, relay)
        once_then_twice(i - 1, multiply)

        def halves(piece):
            chunk = piece // quarters
            turn = lax.rem(piece, quarters)
            first_quarter = jnp.where(chunk < split_from, turn, lax.rem(turn, 2) * 2)
            last_quarter = jnp.where(chunk < split_from, turn, lax.rem(turn, 2) * 2 + 1)
            first_target = jnp.where(chunk < split_from, 0, turn // 2)
            last_target = jnp.where(chunk < split_from, 1, turn // 2)
            low_half, high_half = pl.ds(0, half_rows), pl.ds(half_rows, half_rows)
            return (
                (low_half, (chunk, first_quarter, first_target)),
                (high_half, (chunk, last_quarter, last_target)),
            )

        at_right = i - 1 - lag_right

        @pl.when(jnp.logical_and(me < line - 1, jnp.logical_and(at_right >= 0, at_right < pieces)))
        def _():
            @pl.when(me == 0)
            def _():
                for cut, spot in halves(at_right):
                    right_out[at_right, cut] = part[spot].astype(right_out.dtype)

            @pl.when(me > 0)
            def _():
                send_right(at_right).wait_recv()
                for cut, spot in halves(at_right):
                    right_out[at_right, cut] = (
                        part[spot] + before[at_right, cut].astype(jnp.float32)
                    ).astype(right_out.dtype)

            send_right(at_right).start()

        at_left = i - 1 - lag_left

        @pl.when(jnp.logical_and(me > 0, jnp.logical_and(at_left >= 0, at_left < pieces)))
        def _():
            @pl.when(me == line - 1)
            def _():
                for cut, spot in halves(at_left):
                    left_out[at_left, cut] = part[spot].astype(left_out.dtype)

            @pl.when(me < line - 1)
            def _():
                send_left(at_left).wait_recv()
                for cut, spot in halves(at_left):
                    left_out[at_left, cut] = (
                        part[spot] + after[at_left, cut].astype(jnp.float32)
                    ).astype(left_out.dtype)

            send_left(at_left).start()

        at_total = i - 1 - lag_total

        @pl.when(at_total >= 0)
        def _():
            chunk = at_total // quarters
            turn = lax.rem(at_total, quarters)

            @pl.when(
                jnp.logical_and(
                    jnp.logical_and(turn == 0, chunk > 0), jnp.logical_or(chunk <= split_from, core == 1)
                )
            )
            def _():
                settle(chunk - 1)

            @pl.when(jnp.logical_and(jnp.logical_and(turn == 2, chunk >= split_from), core == 0))
            def _():
                settle(chunk)

            @pl.when(me == line - 1)
            def _():
                send_right(at_total).wait_recv()

            @pl.when(me == 0)
            def _():
                send_left(at_total).wait_recv()

            for cut, spot in halves(at_total):
                _, quarter, target = spot

                @pl.when(me > 0)
                def _():
                    part[spot] = part[spot] + before[at_total, cut].astype(jnp.float32)

                @pl.when(me < line - 1)
                def _():
                    part[spot] = part[spot] + after[at_total, cut].astype(jnp.float32)

                value = part[spot] + b1_ref[...].reshape(1, -1).astype(jnp.float32)
                value = 0.5 * value * (1.0 + lax.erf(value * HALF_ROOT))
                hidden[chunk, target, chip_of(quarter)] = value.astype(hidden.dtype)

            def project(target):
                lhs = hidden[chunk, target].reshape(-1, hidden.shape[4])

                @pl.loop(0, w2_ref.shape[1] // FC2_COLS)
                def _(at):
                    cols = pl.ds(pl.multiple_of(at * FC2_COLS, FC2_COLS), FC2_COLS)
                    result = jnp.dot(lhs, w2_ref[:, cols], preferred_element_type=jnp.float32)

                    @pl.when(core == target)
                    def _():
                        keep[chunk, :, cols] = result

                    @pl.when(core != target)
                    def _():
                        give[chunk, :, cols] = result.astype(give.dtype)

                @pl.when(core != target)
                def _():
                    send_give(chunk).start()

            @pl.when(jnp.logical_and(turn == 1, chunk >= split_from))
            def _():
                project(0)

            @pl.when(turn == quarters - 1)
            def _():
                @pl.when(chunk < split_from)
                def _():
                    project(0)

                project(1)

        return carry

    lax.fori_loop(0, pieces + 1 + lag_total, stage, 0)

    @pl.when(core == 1)
    def _():
        settle(chips - 1)

    spot_sum = spots[0]
    for copy in place_copies:
        copy.wait_recv()
    for step in range(1, groups):
        spot_sum = spot_sum + spots[step]
    spot_ref[...] = spot_sum

    @pl.when(section > 0)
    def _():
        send_base.wait_recv()
        base_ref[...] = base_in[...]

        @pl.loop(0, bands)
        def _(at):
            remote(
                carry_hbm.at[pl.ds(0, band_rows)], incoming_hbm.at[pl.ds(0, band_rows)], carry_send.at[at], carry_recv.at[at], over_y
            ).wait_recv()

    own_chunk = section * wide + column
    y_chunk = flip(section, 1) * wide + column

    @pl.loop(0, parts)
    def _(at):
        cut = pl.ds(at * span, span)
        send_x(y_chunk, at).wait_recv()
        y_out[cut] = (keep[y_chunk, cut] + x_in[y_chunk, cut].astype(jnp.float32)).astype(y_out.dtype)
        send_y(at).start()

    @pl.loop(0, parts)
    def _(at):
        cut = pl.ds(at * span, span)
        send_x(own_chunk, at).wait_recv()
        send_y(at).wait_recv()
        value = (
            keep[own_chunk, cut]
            + x_in[own_chunk, cut].astype(jnp.float32)
            + y_in[cut].astype(jnp.float32)
            + b2_ref[...].reshape(1, -1).astype(jnp.float32)
        ).astype(img_ref.dtype)
        img_ref[cut] = value
        squares[cut] = folded(value)

    totals[0] = jnp.sum(squares[...].T, axis=0, keepdims=True)
    total_copies = []
    for step in range(1, line):
        copy = remote(
            totals.at[0], totals.at[step], total_send.at[step - 1], total_recv.at[step - 1], {"mp": lax.rem(me + step, line)}
        )
        copy.start()
        total_copies.append(copy)

    for step in steps:
        wo_line(step).wait_send()
        for copy in wo_starts(step) + (wo_forward_x(step),):
            copy.wait_send()
        for quarter in range(1, quarters):
            wo_forward_pair(step, quarter).wait_send()
        for tile in range(tiles):
            exchange(step, tile).wait_send()

    for chunk in range(chips):
        for which in range(3):
            own_send(chunk, which).wait_send()
        forward_x(chunk).wait_send()
        for quarter in range(1, quarters):
            forward_pair(chunk, quarter).wait_send()
        send_give(chunk).wait_send()

        @pl.when(chunk % wide != column)
        def _():
            for at in range(parts):
                send_x(chunk, at).wait_send()

    for at in range(parts):
        send_y(at).wait_send()

    @pl.when(me < line - 1)
    def _():
        @pl.loop(0, pieces)
        def _(piece):
            send_right(piece).wait_send()

    @pl.when(me > 0)
    def _():
        @pl.loop(0, pieces)
        def _(piece):
            send_left(piece).wait_send()

    for copy in place_copies:
        copy.wait_send()

    @pl.when(leads)
    def _():
        send_base.wait_send()

        @pl.loop(0, bands)
        def _(at):
            send_band(at).wait_send()

    row_total = totals[0]
    for step, copy in enumerate(total_copies):
        copy.wait()
        row_total = row_total + totals[step + 1]
    total_ref[...] = row_total


def merger(patches, counts, dest, qkv, wo, attn_gain, merge_gain, w1, b1, w2, b2, text, carry):
    groups = lax.axis_size("section") * lax.axis_size("dp")
    line = lax.axis_size("mp")
    chips = groups // 2
    patch_rows, width = patches.shape
    slot_rows = patch_rows // 4
    chunk_rows = slot_rows // chips
    run = chunk_rows // 2
    local_cols = qkv.shape[1]
    units = w1.shape[1]
    features = w2.shape[1]
    pieces = chips * 4
    piece_rows = 2 * chunk_rows
    target_rows = groups * run
    parts = 8
    low = jnp.bfloat16
    dma = pltpu.SemaphoreType.DMA
    sum_rows = text.shape[0] // 128
    bands = text.shape[0] // 16
    return pl.pallas_call(
        merger_kernel,
        out_shape=(
            jax.ShapeDtypeStruct((target_rows, features), low),
            jax.ShapeDtypeStruct((1, slot_rows), jnp.int32),
            jax.ShapeDtypeStruct((sum_rows, 128), jnp.float32),
            jax.ShapeDtypeStruct((1, target_rows), jnp.float32),
            jax.ShapeDtypeStruct(carry.shape, carry.dtype),
        ),
        in_specs=[
            pl.BlockSpec(memory_space={1: pltpu.SMEM, 2: pltpu.VMEM, 5: pltpu.VMEM, 6: pltpu.VMEM, 8: pltpu.VMEM, 10: pltpu.VMEM}.get(at, pl.ANY))
            for at in range(13)
        ],
        out_specs=[pl.BlockSpec(memory_space=pltpu.VMEM)] * 4 + [pl.BlockSpec(memory_space=pl.ANY)],
        scratch_shapes=[
            pltpu.VMEM(patches.shape, low),
            pltpu.VMEM(qkv.shape, low),
            pltpu.VMEM(wo.shape, low),
            pltpu.VMEM(text.shape, low),
            pltpu.VMEM(text.shape, low),
            pltpu.VMEM((text.shape[0], 128), jnp.float32),
            pltpu.VMEM((text.shape[0], 128), jnp.float32),
            dma((2,)),
            dma((bands,)),
            dma((bands,)),
            pltpu.VMEM(patches.shape, low),
            pltpu.VMEM((groups, 1, slot_rows), jnp.int32),
            pltpu.VMEM((2 * sum_rows, 128), jnp.float32),
            pltpu.VMEM((patch_rows, local_cols), low),
            pltpu.VMEM((patch_rows, local_cols), low),
            pltpu.VMEM((patch_rows, local_cols), low),
            pltpu.VMEM((patch_rows, local_cols), low),
            pltpu.VMEM((4, slot_rows, local_cols), low),
            pltpu.VMEM((line, slot_rows, local_cols), low),
            pltpu.VMEM((line,) + wo.shape, low),
            pltpu.VMEM((chips, chunk_rows, width), low),
            pltpu.VMEM(w1.shape, low),
            pltpu.VMEM(w2.shape, low),
            dma((5,)),
            dma((line - 1,)),
            dma((line - 1,)),
            dma((line - 1, 7)),
            dma((line - 1, 4)),
            dma((line - 1, 4)),
            dma((line - 1, counts.shape[0])),
            dma((line - 1, counts.shape[0])),
            pltpu.VMEM((groups, chips, chunk_rows, width), low),
            pltpu.VMEM((chips, 4, 2, chunk_rows, units), jnp.float32),
            pltpu.VMEM((pieces, piece_rows, units), low),
            pltpu.VMEM((pieces, piece_rows, units), low),
            pltpu.VMEM((pieces, piece_rows, units), low),
            pltpu.VMEM((pieces, piece_rows, units), low),
            pltpu.VMEM((chips, 2, chips, chunk_rows, units), low),
            pltpu.VMEM((chips, target_rows, features), low),
            pltpu.VMEM((chips, target_rows, features), low),
            pltpu.VMEM((chips, target_rows, features), jnp.float32),
            pltpu.VMEM((chips, target_rows, features), low),
            pltpu.VMEM((chips, target_rows, features), low),
            pltpu.VMEM((target_rows, features), low),
            pltpu.VMEM((target_rows, features), low),
            pltpu.VMEM((target_rows, 128), jnp.float32),
            pltpu.VMEM((groups, 1, slot_rows), jnp.int32),
            pltpu.VMEM((line, 2 * sum_rows, 128), jnp.float32),
            pltpu.VMEM((sum_rows, 128), jnp.float32),
            pltpu.VMEM((sum_rows, 128), jnp.float32),
            pltpu.VMEM((line, 1, target_rows), jnp.float32),
            dma((chips, 7)),
            dma((chips, 4)),
            dma((chips, 4)),
            dma((pieces,)),
            dma((pieces,)),
            dma((pieces,)),
            dma((pieces,)),
            dma((chips,)),
            dma((chips,)),
            dma((chips, parts)),
            dma((chips, parts)),
            dma((parts,)),
            dma((parts,)),
            dma((groups - 1,)),
            dma((groups - 1,)),
            dma((line - 1,)),
            dma((line - 1,)),
            dma,
            dma,
            dma((line - 1,)),
            dma((line - 1,)),
        ],
        cost_estimate=pl.CostEstimate(
            flops=10**11, bytes_accessed=10**7, transcendentals=0
        ),
        compiler_params=pltpu.CompilerParams(
            collective_id=6, has_side_effects=True, vmem_limit_bytes=VMEM_LIMIT
        ),
    )(patches, counts, dest, qkv, wo, attn_gain, merge_gain, w1, b1, w2, b2, text, carry)


def placing_kernel(
    text_hbm,
    incoming_hbm,
    img_ref,
    spot_ref,
    total_ref,
    base_ref,
    gain_ref,
    seq_hbm,
    layer_hbm,
    text,
    incoming,
    seq,
    layer,
    load_sem,
    store_sem,
):
    cuts = load_sem.shape[1]
    height = text.shape[0] // cuts
    per = base_ref.shape[1] // height
    first = lax.axis_index("section") == 0
    gain = gain_ref[...].reshape(1, -1).astype(jnp.float32)

    def move(which, at):
        cut = pl.ds(at * height, height)
        source, target, sem = (
            (text_hbm, text, load_sem.at[0, at]),
            (incoming_hbm, incoming, load_sem.at[1, at]),
            (seq, seq_hbm, store_sem.at[0, at]),
            (layer, layer_hbm, store_sem.at[1, at]),
        )[which]
        return pltpu.make_async_copy(source.at[cut], target.at[cut], sem)

    for at in range(cuts):
        move(0, at).start()

        @pl.when(jnp.logical_not(first))
        def _():
            move(1, at).start()

    width = base_ref.shape[1]
    lane = lax.broadcasted_iota(jnp.int32, (height, width), 1)
    low_row = lax.broadcasted_iota(jnp.int32, (height, width), 0)
    for at in range(cuts):
        cut = pl.ds(at * height, height)
        at_row = at * height + lax.broadcasted_iota(jnp.int32, (height, spot_ref.shape[1]), 0)
        hits = spot_ref[...] == at_row
        hit = jnp.max(hits.astype(jnp.float32), axis=1, keepdims=True) > 0.0
        placed = jnp.dot(
            hits.astype(jnp.float32).astype(jnp.bfloat16), img_ref[...], preferred_element_type=jnp.float32
        ).astype(jnp.bfloat16)
        diagonal = lane == low_row + at % per * height
        base = jnp.sum(
            jnp.where(diagonal, base_ref[at // per : at // per + 1], 0.0), axis=1, keepdims=True
        )
        move(0, at).wait()
        seq[cut] = jnp.where(hit, placed, text[cut])
        move(2, at).start()

        @pl.when(first)
        def _():
            total = jnp.sum(jnp.where(hits, total_ref[...], 0.0), axis=1, keepdims=True)
            total = jnp.where(hit, total, base)
            scale = lax.rsqrt(total / HID + llm_eps)
            layer[cut] = (seq[cut].astype(jnp.float32) * scale * gain).astype(layer.dtype)

        @pl.when(jnp.logical_not(first))
        def _():
            move(1, at).wait()
            scale = lax.rsqrt(base / HID + llm_eps)
            layer[cut] = (incoming[cut].astype(jnp.float32) * scale * gain).astype(layer.dtype)

        move(3, at).start()

    for at in range(cuts):
        move(2, at).wait()
        move(3, at).wait()


def placing(text, incoming, img, spot, total, base, gain):
    cuts = base.shape[0]
    return pl.pallas_call(
        placing_kernel,
        out_shape=(jax.ShapeDtypeStruct(text.shape, text.dtype),) * 2,
        in_specs=[pl.BlockSpec(memory_space=pl.ANY)] * 2 + [pl.BlockSpec(memory_space=pltpu.VMEM)] * 5,
        out_specs=[pl.BlockSpec(memory_space=pl.ANY)] * 2,
        scratch_shapes=[pltpu.VMEM(text.shape, text.dtype)] * 4
        + [pltpu.SemaphoreType.DMA((2, cuts)), pltpu.SemaphoreType.DMA((2, cuts))],
        cost_estimate=pl.CostEstimate(flops=10**9, bytes_accessed=10**7, transcendentals=0),
        compiler_params=pltpu.CompilerParams(vmem_limit_bytes=VMEM_LIMIT),
    )(text, incoming, img, spot, total, base, gain)


def per_device(*operands):
    (patches, patch_counts, dest_rows, qkv_weight, out_weight, attn_gain, merge_gain) = operands[:7]
    (fc1_weight, fc1_bias, fc2_weight, fc2_bias, text_embeds, section_hidden, llm_gain) = operands[7:]
    outer, _ = group_bits()
    group_count = lax.axis_size("section") * lax.axis_size("dp")
    merged_rows = patches.shape[0] // 4
    run_cap = merged_rows // group_count
    seq_rows = text_embeds.shape[0]
    held = group_count * merged_rows * patches.shape[1] * patches.dtype.itemsize
    if lax.axis_size("mp") != 4 or outer != [("dp", 2), ("section", 1)] or held > KERNEL_BYTES or run_cap % 16 or merged_rows % 128 or seq_rows % 128:
        return plain_per_device(*operands)
    img, spot, base, total, incoming = merger(
        patches,
        patch_counts,
        dest_rows,
        qkv_weight.transpose(1, 2, 0),
        out_weight,
        attn_gain,
        merge_gain,
        fc1_weight,
        fc1_bias,
        fc2_weight,
        fc2_bias,
        text_embeds,
        section_hidden,
    )
    return placing(text_embeds, incoming, img, spot, total, base, llm_gain)


def solution(mesh):
    in_specs = (
        P(("section", "dp"), None),
        P(("section", "dp")),
        P(("section", "dp")),
        P(None, None, "mp"),
        P("mp", None),
        P(),
        P(),
        P("mp", ("section", "dp")),
        P(("section", "dp")),
        P(("section", "dp"), "mp"),
        P("mp"),
        P(("section", "dp"), "mp"),
        P(("section", "dp"), "mp"),
        P("mp"),
    )
    out_specs = (P(("section", "dp"), "mp"), P(("section", "dp"), "mp"))
    return jax.shard_map(
        per_device, mesh=mesh, in_specs=in_specs, out_specs=out_specs, check_vma=False
    )
```
